32 devices in a mesh: dp: 2 (over x), tp: 4 (over z), cp: 4 (over y, core).
Axes of the slice: x: 2, y: 2, z: 4, core: 2. Of those that a mesh axis runs over, the one named last changes fastest.
Arguments:
- hidden: bfloat16 [4096, 2048], P(('dp', 'cp')), parts along dimension 0
- seg_ids: int32 [4096], P(('dp', 'cp')), parts along dimension 0
- w_q: bfloat16 [2048, 2048], P(None, 'tp')
- b_q: bfloat16 [2048], P('tp')
- w_kv: bfloat16 [2048, 256], replicated
- b_kv: bfloat16 [256], replicated
- w_o: bfloat16 [2048, 2048], P('tp')
- b_o: bfloat16 [2048], replicated
- ln_gain: bfloat16 [2048], replicated
- ln_bias: bfloat16 [2048], replicated
Outputs:
- output 1: bfloat16 [4096, 2048], P(('dp', 'cp')), parts along dimension 0
- output 2: bfloat16 [4096, 128], P(('dp', 'cp')), parts along dimension 0
- output 3: bfloat16 [4096, 128], P(('dp', 'cp')), parts along dimension 0
There are 2 independent parts. The reference program is written for one: setup_inputs(seed, part) draws one part's arguments, and reference() takes and returns one part's arrays. A program takes and returns all parts, laid end to end along the dimension named above; an argument that names none is the same for every part.
All inputs are finite; a program needn't handle non-finite values.
Results may differ from the reference program's by a relative error of at most 0.0128857.
Values are sent between devices in bfloat16 or wider.
A program may use at most 1 GiB of HBM per device.

```python
import jax
import jax.numpy as jnp
from jax import lax

D_MODEL = 2048
N_HEADS = 16
HEAD_DIM = 128
TOKENS = 2048
HEAD_GROUPS = 4

LN_EPS = 1e-5
ATTN_SCALE = HEAD_DIM ** -0.5
QUERY_ROWS = min(TOKENS, 64)


def draw_segments(seg_key):
    len_low = TOKENS // 27 + 1
    len_high = (TOKENS * 5) // 8
    max_prompts = TOKENS // len_low + 1
    lengths = jax.random.randint(seg_key, (max_prompts,), len_low, len_high + 1, dtype=jnp.int32)
    prompt_ends = jnp.cumsum(lengths)
    positions = jnp.arange(TOKENS, dtype=jnp.int32)
    return jnp.sum((positions[:, None] >= prompt_ends[None, :]).astype(jnp.int32), axis=1)


def setup_inputs(seed: int = 0, part: int = 0) -> dict:
    part_key = jax.random.fold_in(jax.random.key(seed), part)
    key_hidden, key_seg = jax.random.split(part_key)
    shared = jax.random.split(jax.random.key(seed + 1), 8)
    q_width = N_HEADS * HEAD_DIM
    hidden = (0.5 * jax.random.normal(key_hidden, (TOKENS, D_MODEL), jnp.float32)).astype(jnp.bfloat16)
    seg_ids = draw_segments(key_seg)
    w_q = (1.6 * D_MODEL ** -0.5 * jax.random.normal(shared[0], (D_MODEL, q_width), jnp.float32)).astype(jnp.bfloat16)
    b_q = (0.3 * jax.random.normal(shared[1], (q_width,), jnp.float32)).astype(jnp.bfloat16)
    w_kv = (1.6 * D_MODEL ** -0.5 * jax.random.normal(shared[2], (D_MODEL, 2 * HEAD_DIM), jnp.float32)).astype(jnp.bfloat16)
    b_kv = (0.2 * jax.random.normal(shared[3], (2 * HEAD_DIM,), jnp.float32)).astype(jnp.bfloat16)
    w_o = (q_width ** -0.5 * jax.random.normal(shared[4], (q_width, D_MODEL), jnp.float32)).astype(jnp.bfloat16)
    b_o = (0.3 * jax.random.normal(shared[5], (D_MODEL,), jnp.float32)).astype(jnp.bfloat16)
    ln_gain = (1.0 + 0.3 * jax.random.normal(shared[6], (D_MODEL,), jnp.float32)).astype(jnp.bfloat16)
    ln_bias = (0.3 * jax.random.normal(shared[7], (D_MODEL,), jnp.float32)).astype(jnp.bfloat16)
    return dict(hidden=hidden, seg_ids=seg_ids, w_q=w_q, b_q=b_q, w_kv=w_kv, b_kv=b_kv, w_o=w_o, b_o=b_o, ln_gain=ln_gain, ln_bias=ln_bias)


def reference(hidden, seg_ids, w_q, b_q, w_kv, b_kv, w_o, b_o, ln_gain, ln_bias):
    x_float = hidden.astype(jnp.float32)
    centered = x_float - jnp.mean(x_float, axis=-1, keepdims=True)
    variance = jnp.mean(centered * centered, axis=-1, keepdims=True)
    normed = (centered * lax.rsqrt(variance + LN_EPS) * ln_gain.astype(jnp.float32) + ln_bias.astype(jnp.float32)).astype(jnp.bfloat16)
    q_all = (jnp.dot(normed, w_q, preferred_element_type=jnp.float32) + b_q.astype(jnp.float32)).astype(jnp.bfloat16)
    kv_all = (jnp.dot(normed, w_kv, preferred_element_type=jnp.float32) + b_kv.astype(jnp.float32)).astype(jnp.bfloat16)
    k_cache = kv_all[:, :HEAD_DIM]
    v_cache = kv_all[:, HEAD_DIM:]
    k_float = k_cache.astype(jnp.float32)
    v_float = v_cache.astype(jnp.float32)
    positions = jnp.arange(TOKENS, dtype=jnp.int32)
    n_blocks = TOKENS // QUERY_ROWS
    q_blocks = q_all.reshape(n_blocks, QUERY_ROWS, N_HEADS, HEAD_DIM)
    seg_blocks = seg_ids.reshape(n_blocks, QUERY_ROWS)
    pos_blocks = positions.reshape(n_blocks, QUERY_ROWS)

    def attend(block_in):
        q_blk, seg_q, pos_q = block_in
        scores = jnp.einsum('bhd,kd->bhk', q_blk.astype(jnp.float32), k_float) * ATTN_SCALE
        visible = (seg_ids[None, :] == seg_q[:, None]) & (positions[None, :] <= pos_q[:, None])
        scores = jnp.where(visible[:, None, :], scores, -jnp.inf)
        p_weights = jax.nn.softmax(scores, axis=-1)
        return jnp.einsum('bhk,kd->bhd', p_weights, v_float).astype(jnp.bfloat16)

    attn_out = lax.map(attend, (q_blocks, seg_blocks, pos_blocks))
    group_width = N_HEADS * HEAD_DIM // HEAD_GROUPS
    attn_groups = attn_out.reshape(TOKENS, HEAD_GROUPS, group_width).transpose(1, 0, 2)
    wo_groups = w_o.reshape(HEAD_GROUPS, group_width, D_MODEL)

    def add_group(run_total, group_pair):
        attn_g, wo_g = group_pair
        partial = jnp.dot(attn_g, wo_g, preferred_element_type=jnp.float32).astype(jnp.bfloat16)
        return run_total + partial.astype(jnp.float32), None

    proj_sum, scan_tail = lax.scan(add_group, jnp.zeros((TOKENS, D_MODEL), jnp.float32), (attn_groups, wo_groups))
    y_out = (x_float + proj_sum + b_o.astype(jnp.float32)).astype(jnp.bfloat16)
    return (y_out, k_cache, v_cache)
```

```python
import functools
import jax
import jax.numpy as jnp
from jax import lax
from jax.experimental import pallas as pl
from jax.experimental.pallas import tpu as pltpu
from jax.sharding import PartitionSpec as P

HEAD_DIM = 128
LN_EPS = 1e-5
SCORE_SCALE = HEAD_DIM ** -0.5 * 1.4426950408889634
MESH = pl.DeviceIdType.MESH
BF16 = jnp.bfloat16
F32 = jnp.float32


class Sends:
    def __init__(self, sems):
        self.sems, self.made = sems, []

    def go(self, src, dst, recv, to, cond=None):
        slot = len(self.made)
        make = lambda: pltpu.make_async_remote_copy(src_ref=src(), dst_ref=dst(), send_sem=self.sems.at[slot], recv_sem=recv(),
                                                    device_id=to, device_id_type=MESH)
        self.made.append((make, cond))
        if cond is None:
            make().start()
        else:
            pl.when(cond())(lambda: make().start())

    def finish(self):
        for make, cond in self.made:
            if cond is None:
                make().wait_send()
            else:
                pl.when(cond())(lambda: make().wait_send())


def arrived(dst, recv):
    pltpu.make_async_copy(dst, dst, recv).wait()


N_SENDS = 64


def kernel(hid_hbm, seg_hbm, wq_hbm, bq_hbm, wkv_hbm, bkv_ref, wo_hbm, bo_ref, gain_ref, lnb_ref,
           y_ref, k_ref, v_ref,
           hid, normed, wkv, wq, wo, bq, seg, segcol, kv, q_s, o_all, part, m_s, l_s, acc_s,
           load_sem, send_sem, o_send, bq_recv, seg_recv, kv_recv, wq_recv, wo_recv, o_recv):
    tok, d_model = hid.shape
    width = wq.shape[2]
    heads = width // HEAD_DIM
    tile = tok // 4
    q_rows, o_rows = d_model // 8, width // 8
    dp, z, cp = lax.axis_index('dp'), lax.axis_index('tp'), lax.axis_index('cp')
    y, c = cp // 2, cp % 2
    pair = z + 1 - 2 * (z % 2)
    below, above = {'tp': z - 1}, {'tp': z + 1}
    to_x, to_y, to_core = {'dp': 1 - dp}, {'cp': cp + 2 - 4 * y}, {'cp': cp + 1 - 2 * c}
    pos = lambda px, py, pc: px * 4 + py * 2 + pc
    p_me, p_x, p_y, p_d = pos(dp, y, c), pos(1 - dp, y, c), pos(dp, 1 - y, c), pos(1 - dp, 1 - y, c)
    g_a = 1 + z % 2
    g_c = 3 - 3 * (z // 2)
    g_b = 6 - z - g_a - g_c
    sends = Sends(send_sem)

    loads = [pltpu.make_async_copy(hid_hbm, hid, load_sem.at[0]),
             pltpu.make_async_copy(wkv_hbm, wkv, load_sem.at[1]),
             pltpu.make_async_copy(wq_hbm, wq.at[0], load_sem.at[2]),
             pltpu.make_async_copy(bq_hbm, bq.at[0], load_sem.at[3]),
             pltpu.make_async_copy(seg_hbm, seg.at[cp], load_sem.at[4]),
             pltpu.make_async_copy(wo_hbm, wo.at[pl.ds(z * width, width), :], load_sem.at[5])]
    for load in loads:
        load.start()

    barrier = pltpu.get_barrier_semaphore()
    for step in (1, 2, 3):
        pl.semaphore_signal(barrier, inc=1, device_id={'cp': (cp + step) % 4}, device_id_type=MESH)
    pl.semaphore_signal(barrier, inc=1, device_id=to_x, device_id_type=MESH)

    @pl.when(z > 0)
    def _():
        pl.semaphore_signal(barrier, inc=1, device_id={'tp': z - 1}, device_id_type=MESH)

    @pl.when(z < 3)
    def _():
        pl.semaphore_signal(barrier, inc=1, device_id={'tp': z + 1}, device_id_type=MESH)

    pl.semaphore_wait(barrier, 5 + (z + 1) // 2 - 2 * (z // 3))

    wq_piece = lambda p: wq.at[1, pl.ds(p * q_rows, q_rows), :]
    wo_piece = lambda g, p: wo.at[pl.ds(g * width + p * o_rows, o_rows), :]

    own_q, own_o = lambda: wq_hbm.at[pl.ds(p_me * q_rows, q_rows), :], lambda: wo_hbm.at[pl.ds(p_me * o_rows, o_rows), :]
    sends.go(lambda: bq_hbm, lambda: bq.at[1], lambda: bq_recv, {'tp': pair})
    sends.go(own_q, lambda: wq_piece(p_me), lambda: wq_recv.at[p_me], {'tp': pair})
    sends.go(own_o, lambda: wo_piece(z, p_me), lambda: wo_recv.at[z, p_me], {'tp': z - 1}, lambda: z > 0)
    sends.go(own_o, lambda: wo_piece(z, p_me), lambda: wo_recv.at[z, p_me], {'tp': z + 1}, lambda: z < 3)
    for step in (1, 2, 3):
        sends.go(lambda: seg_hbm, lambda: seg.at[cp], lambda: seg_recv.at[cp], {'cp': cp + step}, lambda step=step: cp + step < 4)

    def pass_on(piece, recv, source, g=None):
        p = {'z': p_me, 'x': p_x, 'y': p_y, 'd': p_d}[source]
        src, sem = lambda: piece(p), lambda: recv(p)
        arrived(src(), sem())
        if source == 'z':
            if g is not None:
                sends.go(src, src, sem, below, lambda: (g > z) & (z > 0))
                sends.go(src, src, sem, above, lambda: (g < z) & (z < 3))
            sends.go(src, src, sem, to_x)
            sends.go(src, src, sem, to_y)
        elif source == 'x':
            sends.go(src, src, sem, to_y, lambda: c == 1)
        elif source == 'y':
            sends.go(src, src, sem, to_x, lambda: c == 0)
        sends.go(src, src, sem, to_core)

    def from_core(piece, recv):
        for px in (0, 1):
            for py in (0, 1):
                p = pos(px, py, 1 - c)
                arrived(piece(p), recv(p))

    def q_event(*sources):
        for source in sources:
            pass_on(wq_piece, lambda p: wq_recv.at[p], source)

    def o_event(g, *sources):
        for source in sources:
            pass_on(functools.partial(wo_piece, g), lambda p: wo_recv.at[g, p], source, g)

    loads[0].wait()
    gain = gain_ref[...].astype(F32)
    lnb = lnb_ref[...].astype(F32)
    ln_rows = min(64, tok)

    def ln_step(i, carry):
        rows = pl.ds(pl.multiple_of(i * ln_rows, ln_rows), ln_rows)
        x = hid[rows, :].astype(F32)
        cen = x - jnp.mean(x, axis=-1, keepdims=True)
        var = jnp.mean(cen * cen, axis=-1, keepdims=True)
        normed[rows, :] = (cen * lax.rsqrt(var + LN_EPS) * gain + lnb).astype(BF16)
        return carry

    lax.fori_loop(0, tok // ln_rows, ln_step, 0)

    loads[1].wait()
    kv_new = (jnp.dot(normed[...], wkv[...], preferred_element_type=F32) + bkv_ref[...].astype(F32)).astype(BF16)
    kv[cp, 0] = kv_new[:, :HEAD_DIM]
    kv[cp, 1] = kv_new[:, HEAD_DIM:]
    k_ref[...] = kv_new[:, :HEAD_DIM]
    v_ref[...] = kv_new[:, HEAD_DIM:]

    def project_q(which):
        qf = jnp.dot(normed[...], wq[which], preferred_element_type=F32) + bq[which].astype(F32)
        for r in range(4):
            for h in range(heads):
                q_s[which * 4 + r, h * tile:(h + 1) * tile, :] = qf[r * tile:(r + 1) * tile, h * HEAD_DIM:(h + 1) * HEAD_DIM].astype(BF16)

    loads[2].wait()
    loads[3].wait()
    sends.go(lambda: kv.at[cp], lambda: kv.at[cp], lambda: kv_recv.at[cp], to_core, lambda: c == 0)
    sends.go(lambda: kv.at[cp], lambda: kv.at[cp], lambda: kv_recv.at[cp], to_y, lambda: y == 0)
    project_q(0)
    loads[4].wait()
    for r in range(4):
        row = jnp.broadcast_to(seg[cp, :, r * tile:(r + 1) * tile], (tile, tile))
        segcol[r] = row.T

    @pl.when(y == 1)
    def _():
        arrived(kv.at[c], kv_recv.at[c])

    sends.go(lambda: kv.at[c], lambda: kv.at[c], lambda: kv_recv.at[c], to_core, lambda: y == 1)
    q_event('z')

    def scores(q, k_blk, mask):
        s = lax.dot_general(q, k_blk, (((1,), (1,)), ((), ())), preferred_element_type=F32) * SCORE_SCALE
        keys = k_blk.shape[0]
        return jnp.where(mask[None], s.reshape(heads, tile, keys), -jnp.inf).reshape(heads * tile, keys)

    def attend(t, carry):
        r = t % 4
        g = jnp.where(t < 4, z, pair)

        @pl.when(t == 4)
        def _():
            from_core(wq_piece, lambda p: wq_recv.at[p])
            arrived(bq.at[1], bq_recv)
            project_q(1)

        q = q_s[t]
        seg_q = segcol[r][:, :1]
        k_pos = lax.broadcasted_iota(jnp.int32, (tile, tok), 1)
        q_pos = lax.broadcasted_iota(jnp.int32, (tile, tok), 0) + r * tile
        s = scores(q, kv[cp, 0], (seg[cp] == seg_q) & (k_pos <= q_pos))
        m_new = jnp.max(s, axis=-1, keepdims=True)
        p = jnp.exp2(s - m_new)
        m_s[...] = jnp.broadcast_to(m_new, m_s.shape)
        l_s[...] = jnp.broadcast_to(jnp.sum(p, axis=-1, keepdims=True), l_s.shape)
        acc_s[...] = jnp.dot(p.astype(BF16), kv[cp, 1], preferred_element_type=F32)

        @pl.when(t == 0)
        def _():
            for j in range(3):
                pl.when(j < cp)(functools.partial(arrived, seg.at[j], seg_recv.at[j]))
            pl.when(y == 1)(functools.partial(arrived, kv.at[1 - c], kv_recv.at[1 - c]))
            pl.when(c == 1)(functools.partial(arrived, kv.at[cp - 1], kv_recv.at[cp - 1]))

        def earlier(j, inner):
            s = scores(q, kv[j, 0], seg[j] == seg_q)
            m_prev = m_s[...]
            m_new = jnp.maximum(m_prev, jnp.max(s, axis=-1, keepdims=True))
            p = jnp.exp2(s - m_new[:, :1])
            alpha = jnp.exp2(m_prev - m_new)
            m_s[...] = m_new
            l_s[...] = l_s[...] * alpha + jnp.sum(p, axis=-1, keepdims=True)
            acc_s[...] = acc_s[...] * alpha + jnp.dot(p.astype(BF16), kv[j, 1], preferred_element_type=F32)
            return inner

        lax.fori_loop(0, cp, earlier, 0)
        rows = pl.ds(pl.multiple_of(r * tile, tile), tile)
        for h in range(heads):
            part_o = acc_s[h * tile:(h + 1) * tile, :] / l_s[h * tile:(h + 1) * tile, :]
            o_all[g, rows, h * HEAD_DIM:(h + 1) * HEAD_DIM] = part_o.astype(BF16)

        events = {0: [(o_event, g_a, 'z')], 1: [(q_event, 'x', 'y')], 2: [(o_event, g_b, 'z')], 3: [(q_event, 'd')],
                  4: [(o_event, g_a, 'x', 'y')], 5: [(o_event, g_c, 'z'), (o_event, g_a, 'd')], 6: [(o_event, g_b, 'x', 'y')],
                  7: [(o_event, g_b, 'd')]}
        for when, todo in events.items():
            @pl.when(t == when)
            def _():
                for what, *about in todo:
                    what(*about)

        o_tile = o_all.at[g, rows, :]
        copy = pltpu.make_async_remote_copy(src_ref=o_tile, dst_ref=o_tile, send_sem=o_send.at[t], recv_sem=o_recv.at[t],
                                            device_id={'tp': 3 - z}, device_id_type=MESH)
        pl.when((z > 0) & (z < 3))(lambda: copy.start())
        return carry

    lax.fori_loop(0, 8, attend, 0)

    n_col = min(512, d_model)

    def project_o(g, rows, n_rows):
        def cols(n, carry):
            at = pl.ds(pl.multiple_of(n * n_col, n_col), n_col)
            part[g, rows, at] = jnp.dot(o_all[g, rows, :], wo[pl.ds(pl.multiple_of(g * width, width), width), at],
                                        preferred_element_type=F32).astype(BF16)
            return carry

        lax.fori_loop(0, d_model // n_col, cols, 0)

    loads[5].wait()
    every = pl.ds(0, tok)
    project_o(z, every, tok)
    from_core(functools.partial(wo_piece, g_a), lambda p: wo_recv.at[g_a, p])
    from_core(functools.partial(wo_piece, g_b), lambda p: wo_recv.at[g_b, p])
    project_o(pair, every, tok)

    def other(u, carry):
        r = u % 4
        g_1, g_2 = 2 - z // 2, 3 - 3 * (z // 2)
        g = jnp.where(u < 4, g_1, g_2)
        rows = pl.ds(pl.multiple_of(r * tile, tile), tile)
        o_tile = o_all.at[g, rows, :]
        arrived(o_tile, o_recv.at[u])
        for edge, cond in ((0, z == 1), (3, z == 2)):
            copy = pltpu.make_async_remote_copy(src_ref=o_tile, dst_ref=o_tile, send_sem=o_send.at[8 + u], recv_sem=o_recv.at[u],
                                                device_id={'tp': edge}, device_id_type=MESH)
            pl.when(cond)(lambda copy=copy: copy.start())

        @pl.when(u == 2)
        def _():
            o_event(g_c, 'x', 'y')

        @pl.when(u == 3)
        def _():
            o_event(g_c, 'd')
            from_core(functools.partial(wo_piece, g_c), lambda p: wo_recv.at[g_c, p])

        project_o(g, rows, tile)

        @pl.when(u >= 4)
        def _():
            def finish(i, inner):
                f_rows = tile // 4
                at = pl.ds(pl.multiple_of(r * tile + i * f_rows, f_rows), f_rows)
                total = part[0, at, :].astype(F32)
                for gg in (1, 2, 3):
                    total = total + part[gg, at, :].astype(F32)
                y_ref[at, :] = (hid[at, :].astype(F32) + total + bo_ref[...].astype(F32)).astype(BF16)
                return inner

            lax.fori_loop(0, 4, finish, 0)

        return carry

    lax.fori_loop(0, 8, other, 0)

    sends.finish()

    @pl.when((z > 0) & (z < 3))
    def _():
        def sent(u, carry):
            g = jnp.where(u < 4, z, pair)
            g_1, g_2 = 2 - z // 2, 3 - 3 * (z // 2)
            rows = pl.ds(pl.multiple_of((u % 4) * tile, tile), tile)
            for which, gg in ((u, g), (u + 8, jnp.where(u < 4, g_1, g_2))):
                o_tile = o_all.at[gg, rows, :]
                pltpu.make_async_copy(o_tile, o_tile, o_send.at[which]).wait()
            return carry

        lax.fori_loop(0, 8, sent, 0)


def solution(mesh):
    def local_block(hidden, seg_ids, w_q, b_q, w_kv, b_kv, w_o, b_o, ln_gain, ln_bias):
        tok, d_model = hidden.shape
        width = w_q.shape[1]
        heads = width // HEAD_DIM
        tile = tok // 4
        hbm = pl.BlockSpec(memory_space=pl.ANY)
        vmem = pl.BlockSpec(memory_space=pltpu.VMEM)
        row = lambda a: a.reshape(1, -1)
        dma = pltpu.SemaphoreType.DMA
        return pl.pallas_call(
            kernel,
            out_shape=(jax.ShapeDtypeStruct((tok, d_model), BF16), jax.ShapeDtypeStruct((tok, HEAD_DIM), BF16),
                       jax.ShapeDtypeStruct((tok, HEAD_DIM), BF16)),
            in_specs=[hbm, hbm, hbm, hbm, hbm, vmem, hbm, vmem, vmem, vmem],
            out_specs=(vmem, vmem, vmem),
            scratch_shapes=[
                pltpu.VMEM((tok, d_model), BF16),
                pltpu.VMEM((tok, d_model), BF16),
                pltpu.VMEM((d_model, 2 * HEAD_DIM), BF16),
                pltpu.VMEM((2, d_model, width), BF16),
                pltpu.VMEM((4 * width, d_model), BF16),
                pltpu.VMEM((2, 1, width), BF16),
                pltpu.VMEM((4, 1, tok), jnp.int32),
                pltpu.VMEM((4, tile, tile), jnp.int32),
                pltpu.VMEM((4, 2, tok, HEAD_DIM), BF16),
                pltpu.VMEM((8, heads * tile, HEAD_DIM), BF16),
                pltpu.VMEM((4, tok, width), BF16),
                pltpu.VMEM((4, tok, d_model), BF16),
                pltpu.VMEM((heads * tile, HEAD_DIM), F32),
                pltpu.VMEM((heads * tile, HEAD_DIM), F32),
                pltpu.VMEM((heads * tile, HEAD_DIM), F32),
                dma((6,)), dma((N_SENDS,)), dma((16,)), dma(()), dma((4,)), dma((4,)), dma((8,)), dma((4, 8)), dma((8,)),
            ],
            compiler_params=pltpu.CompilerParams(collective_id=0, has_side_effects=True, vmem_limit_bytes=60 * 2 ** 20),
            name='block',
        )(hidden, row(seg_ids), w_q, row(b_q), w_kv, row(b_kv), w_o, row(b_o), row(ln_gain), row(ln_bias))

    row_spec = P(('dp', 'cp'), None)
    tok_spec = P(('dp', 'cp'))
    return jax.shard_map(local_block, mesh=mesh,
                         in_specs=(row_spec, tok_spec, P(None, 'tp'), P('tp'), P(None, None), P(None), P('tp', None), P(None), P(None), P(None)),
                         out_specs=(row_spec, row_spec, row_spec), check_vma=False)
```

```python
import functools
import jax
import jax.numpy as jnp
from jax import lax
from jax.experimental import pallas as pl
from jax.experimental.pallas import tpu as pltpu
from jax.sharding import PartitionSpec as P

HEAD_DIM = 128
LN_EPS = 1e-5
SCORE_SCALE = HEAD_DIM ** -0.5 * 1.4426950408889634
MESH = pl.DeviceIdType.MESH
BF16 = jnp.bfloat16
F32 = jnp.float32


class Sends:
    def __init__(self, sems):
        self.sems, self.made = sems, []

    def go(self, src, dst, recv, to, cond=None):
        slot = len(self.made)
        make = lambda: pltpu.make_async_remote_copy(src_ref=src(), dst_ref=dst(), send_sem=self.sems.at[slot], recv_sem=recv(),
                                                    device_id=to, device_id_type=MESH)
        self.made.append((make, cond))
        if cond is None:
            make().start()
        else:
            pl.when(cond())(lambda: make().start())

    def finish(self):
        for make, cond in self.made:
            if cond is None:
                make().wait_send()
            else:
                pl.when(cond())(lambda: make().wait_send())


def arrived(dst, recv):
    pltpu.make_async_copy(dst, dst, recv).wait()


N_SENDS = 64


def kernel(hid_hbm, seg_hbm, wq_hbm, bq_hbm, wkv_hbm, bkv_hbm, wo_hbm, bo_hbm, gain_hbm, lnb_hbm,
           y_ref, k_ref, v_ref,
           hid, normed, wkv, wq, wo, bq_own, bq_pair, bkv_ref, bo_ref, gain_ref, lnb_ref, seg, segcol, kv, q_s, o_all, part, m_s, l_s, acc_s,
           load_sem, send_sem, o_send, bq_recv, seg_recv, kv_recv, wq_recv, wo_recv, o_recv):
    tok, d_model = hid.shape
    width = wq.shape[2]
    heads = width // HEAD_DIM
    tile = tok // 4
    q_rows, o_rows = d_model // 8, width // 8
    dp, z, cp = lax.axis_index('dp'), lax.axis_index('tp'), lax.axis_index('cp')
    y, c = cp // 2, cp % 2
    pair = z + 1 - 2 * (z % 2)
    below, above = {'tp': z - 1}, {'tp': z + 1}
    to_x, to_y, to_core = {'dp': 1 - dp}, {'cp': cp + 2 - 4 * y}, {'cp': cp + 1 - 2 * c}
    pos = lambda px, py, pc: px * 4 + py * 2 + pc
    p_me, p_x, p_y, p_d = pos(dp, y, c), pos(1 - dp, y, c), pos(dp, 1 - y, c), pos(1 - dp, 1 - y, c)
    g_a = 1 + z % 2
    g_c = 3 - 3 * (z // 2)
    g_b = 6 - z - g_a - g_c
    sends = Sends(send_sem)

    loads = [pltpu.make_async_copy(hid_hbm, hid, load_sem.at[0]),
             pltpu.make_async_copy(wkv_hbm, wkv, load_sem.at[1]),
             pltpu.make_async_copy(wq_hbm, wq.at[0], load_sem.at[2]),
             pltpu.make_async_copy(bq_hbm, bq_own, load_sem.at[3]),
             pltpu.make_async_copy(seg_hbm, seg.at[cp], load_sem.at[4]),
             pltpu.make_async_copy(wo_hbm, wo.at[pl.ds(z * width, width), :], load_sem.at[5]),
             pltpu.make_async_copy(gain_hbm, gain_ref, load_sem.at[6]),
             pltpu.make_async_copy(lnb_hbm, lnb_ref, load_sem.at[7]),
             pltpu.make_async_copy(bkv_hbm, bkv_ref, load_sem.at[8]),
             pltpu.make_async_copy(bo_hbm, bo_ref, load_sem.at[9])]
    for load in loads:
        load.start()

    barrier = pltpu.get_barrier_semaphore()
    for step in (1, 2, 3):
        pl.semaphore_signal(barrier, inc=1, device_id={'cp': (cp + step) % 4}, device_id_type=MESH)
    pl.semaphore_signal(barrier, inc=1, device_id=to_x, device_id_type=MESH)

    @pl.when(z > 0)
    def _():
        pl.semaphore_signal(barrier, inc=1, device_id={'tp': z - 1}, device_id_type=MESH)

    @pl.when(z < 3)
    def _():
        pl.semaphore_signal(barrier, inc=1, device_id={'tp': z + 1}, device_id_type=MESH)

    pl.semaphore_wait(barrier, 5 + (z + 1) // 2 - 2 * (z // 3))

    wq_piece = lambda p: wq.at[1, pl.ds(p * q_rows, q_rows), :]
    wo_piece = lambda g, p: wo.at[pl.ds(g * width + p * o_rows, o_rows), :]

    own_q, own_o = lambda: wq_hbm.at[pl.ds(p_me * q_rows, q_rows), :], lambda: wo_hbm.at[pl.ds(p_me * o_rows, o_rows), :]
    sends.go(lambda: bq_hbm, lambda: bq_pair, lambda: bq_recv, {'tp': pair})
    sends.go(own_q, lambda: wq_piece(p_me), lambda: wq_recv.at[p_me], {'tp': pair})
    sends.go(own_o, lambda: wo_piece(z, p_me), lambda: wo_recv.at[z, p_me], {'tp': z - 1}, lambda: z > 0)
    sends.go(own_o, lambda: wo_piece(z, p_me), lambda: wo_recv.at[z, p_me], {'tp': z + 1}, lambda: z < 3)
    for step in (1, 2, 3):
        sends.go(lambda: seg_hbm, lambda: seg.at[cp], lambda: seg_recv.at[cp], {'cp': cp + step}, lambda step=step: cp + step < 4)

    def pass_on(piece, recv, source, g=None):
        p = {'z': p_me, 'x': p_x, 'y': p_y, 'd': p_d}[source]
        src, sem = lambda: piece(p), lambda: recv(p)
        arrived(src(), sem())
        if source == 'z':
            if g is not None:
                sends.go(src, src, sem, below, lambda: (g > z) & (z > 0))
                sends.go(src, src, sem, above, lambda: (g < z) & (z < 3))
            sends.go(src, src, sem, to_x)
            sends.go(src, src, sem, to_y)
        elif source == 'x':
            sends.go(src, src, sem, to_y, lambda: c == 1)
        elif source == 'y':
            sends.go(src, src, sem, to_x, lambda: c == 0)
        sends.go(src, src, sem, to_core)

    def from_core(piece, recv):
        for px in (0, 1):
            for py in (0, 1):
                p = pos(px, py, 1 - c)
                arrived(piece(p), recv(p))

    def q_event(*sources):
        for source in sources:
            pass_on(wq_piece, lambda p: wq_recv.at[p], source)

    def o_event(g, *sources):
        for source in sources:
            pass_on(functools.partial(wo_piece, g), lambda p: wo_recv.at[g, p], source, g)

    for i in (0, 6, 7):
        loads[i].wait()
    gain = gain_ref[...].astype(F32)
    lnb = lnb_ref[...].astype(F32)
    ln_rows = min(64, tok)

    def ln_step(i, carry):
        rows = pl.ds(pl.multiple_of(i * ln_rows, ln_rows), ln_rows)
        x = hid[rows, :].astype(F32)
        cen = x - jnp.mean(x, axis=-1, keepdims=True)
        var = jnp.mean(cen * cen, axis=-1, keepdims=True)
        normed[rows, :] = (cen * lax.rsqrt(var + LN_EPS) * gain + lnb).astype(BF16)
        return carry

    lax.fori_loop(0, tok // ln_rows, ln_step, 0)

    loads[1].wait()
    loads[8].wait()
    kv_new = (jnp.dot(normed[...], wkv[...], preferred_element_type=F32) + bkv_ref[...].astype(F32)).astype(BF16)
    kv[cp, 0] = kv_new[:, :HEAD_DIM]
    kv[cp, 1] = kv_new[:, HEAD_DIM:]
    k_ref[...] = kv_new[:, :HEAD_DIM]
    v_ref[...] = kv_new[:, HEAD_DIM:]

    def project_q(which, bias):
        qf = jnp.dot(normed[...], wq[which], preferred_element_type=F32) + bias[...].astype(F32)
        for r in range(4):
            for h in range(heads):
                q_s[which * 4 + r, h * tile:(h + 1) * tile, :] = qf[r * tile:(r + 1) * tile, h * HEAD_DIM:(h + 1) * HEAD_DIM].astype(BF16)

    loads[2].wait()
    loads[3].wait()
    sends.go(lambda: kv.at[cp], lambda: kv.at[cp], lambda: kv_recv.at[cp], to_core, lambda: c == 0)
    sends.go(lambda: kv.at[cp], lambda: kv.at[cp], lambda: kv_recv.at[cp], to_y, lambda: y == 0)
    project_q(0, bq_own)
    loads[4].wait()
    for r in range(4):
        row = jnp.broadcast_to(seg[cp, :, r * tile:(r + 1) * tile], (tile, tile))
        segcol[r] = row.T

    @pl.when(y == 1)
    def _():
        arrived(kv.at[c], kv_recv.at[c])

    sends.go(lambda: kv.at[c], lambda: kv.at[c], lambda: kv_recv.at[c], to_core, lambda: y == 1)
    q_event('z')

    def scores(q, k_blk, mask):
        s = lax.dot_general(q, k_blk, (((1,), (1,)), ((), ())), preferred_element_type=F32) * SCORE_SCALE
        keys = k_blk.shape[0]
        return jnp.where(mask[None], s.reshape(heads, tile, keys), -jnp.inf).reshape(heads * tile, keys)

    def attend(t, carry):
        r = t % 4
        g = jnp.where(t < 4, z, pair)

        @pl.when(t == 4)
        def _():
            from_core(wq_piece, lambda p: wq_recv.at[p])
            arrived(bq_pair, bq_recv)
            project_q(1, bq_pair)

        q = q_s[t]
        seg_q = segcol[r][:, :1]
        k_pos = lax.broadcasted_iota(jnp.int32, (tile, tok), 1)
        q_pos = lax.broadcasted_iota(jnp.int32, (tile, tok), 0) + r * tile
        s = scores(q, kv[cp, 0], (seg[cp] == seg_q) & (k_pos <= q_pos))
        m_new = jnp.max(s, axis=-1, keepdims=True)
        p = jnp.exp2(s - m_new)
        m_s[...] = jnp.broadcast_to(m_new, m_s.shape)
        l_s[...] = jnp.broadcast_to(jnp.sum(p, axis=-1, keepdims=True), l_s.shape)
        acc_s[...] = jnp.dot(p.astype(BF16), kv[cp, 1], preferred_element_type=F32)

        @pl.when(t == 0)
        def _():
            for j in range(3):
                pl.when(j < cp)(functools.partial(arrived, seg.at[j], seg_recv.at[j]))
            pl.when(y == 1)(functools.partial(arrived, kv.at[1 - c], kv_recv.at[1 - c]))
            pl.when(c == 1)(functools.partial(arrived, kv.at[cp - 1], kv_recv.at[cp - 1]))

        def earlier(j, inner):
            s = scores(q, kv[j, 0], seg[j] == seg_q)
            m_prev = m_s[...]
            m_new = jnp.maximum(m_prev, jnp.max(s, axis=-1, keepdims=True))
            p = jnp.exp2(s - m_new[:, :1])
            alpha = jnp.exp2(m_prev - m_new)
            m_s[...] = m_new
            l_s[...] = l_s[...] * alpha + jnp.sum(p, axis=-1, keepdims=True)
            acc_s[...] = acc_s[...] * alpha + jnp.dot(p.astype(BF16), kv[j, 1], preferred_element_type=F32)
            return inner

        lax.fori_loop(0, cp, earlier, 0)
        rows = pl.ds(pl.multiple_of(r * tile, tile), tile)
        for h in range(heads):
            part_o = acc_s[h * tile:(h + 1) * tile, :] / l_s[h * tile:(h + 1) * tile, :]
            o_all[g, rows, h * HEAD_DIM:(h + 1) * HEAD_DIM] = part_o.astype(BF16)

        events = {0: [(o_event, g_a, 'z')], 1: [(q_event, 'x', 'y')], 2: [(o_event, g_b, 'z')], 3: [(q_event, 'd')],
                  4: [(o_event, g_a, 'x', 'y')], 5: [(o_event, g_c, 'z'), (o_event, g_a, 'd')], 6: [(o_event, g_b, 'x', 'y')],
                  7: [(o_event, g_b, 'd')]}
        for when, todo in events.items():
            @pl.when(t == when)
            def _():
                for what, *about in todo:
                    what(*about)

        o_tile = o_all.at[g, rows, :]
        copy = pltpu.make_async_remote_copy(src_ref=o_tile, dst_ref=o_tile, send_sem=o_send.at[t], recv_sem=o_recv.at[t],
                                            device_id={'tp': 3 - z}, device_id_type=MESH)
        pl.when((z > 0) & (z < 3))(lambda: copy.start())
        return carry

    lax.fori_loop(0, 8, attend, 0)

    n_col = min(512, d_model)

    def project_o(g, rows, n_rows):
        def cols(n, carry):
            at = pl.ds(pl.multiple_of(n * n_col, n_col), n_col)
            part[g, rows, at] = jnp.dot(o_all[g, rows, :], wo[pl.ds(pl.multiple_of(g * width, width), width), at],
                                        preferred_element_type=F32).astype(BF16)
            return carry

        lax.fori_loop(0, d_model // n_col, cols, 0)

    loads[5].wait()
    loads[9].wait()
    every = pl.ds(0, tok)
    project_o(z, every, tok)
    from_core(functools.partial(wo_piece, g_a), lambda p: wo_recv.at[g_a, p])
    from_core(functools.partial(wo_piece, g_b), lambda p: wo_recv.at[g_b, p])
    project_o(pair, every, tok)

    def other(u, carry):
        r = u % 4
        g_1, g_2 = 2 - z // 2, 3 - 3 * (z // 2)
        g = jnp.where(u < 4, g_1, g_2)
        rows = pl.ds(pl.multiple_of(r * tile, tile), tile)
        o_tile = o_all.at[g, rows, :]
        arrived(o_tile, o_recv.at[u])
        for edge, cond in ((0, z == 1), (3, z == 2)):
            copy = pltpu.make_async_remote_copy(src_ref=o_tile, dst_ref=o_tile, send_sem=o_send.at[8 + u], recv_sem=o_recv.at[u],
                                                device_id={'tp': edge}, device_id_type=MESH)
            pl.when(cond)(lambda copy=copy: copy.start())

        @pl.when(u == 2)
        def _():
            o_event(g_c, 'x', 'y')

        @pl.when(u == 3)
        def _():
            o_event(g_c, 'd')
            from_core(functools.partial(wo_piece, g_c), lambda p: wo_recv.at[g_c, p])

        project_o(g, rows, tile)

        @pl.when(u >= 4)
        def _():
            def finish(i, inner):
                f_rows = tile // 4
                at = pl.ds(pl.multiple_of(r * tile + i * f_rows, f_rows), f_rows)
                total = part[0, at, :].astype(F32)
                for gg in (1, 2, 3):
                    total = total + part[gg, at, :].astype(F32)
                y_ref[at, :] = (hid[at, :].astype(F32) + total + bo_ref[...].astype(F32)).astype(BF16)
                return inner

            lax.fori_loop(0, 4, finish, 0)

        return carry

    lax.fori_loop(0, 8, other, 0)

    sends.finish()

    @pl.when((z > 0) & (z < 3))
    def _():
        def sent(u, carry):
            g = jnp.where(u < 4, z, pair)
            g_1, g_2 = 2 - z // 2, 3 - 3 * (z // 2)
            rows = pl.ds(pl.multiple_of((u % 4) * tile, tile), tile)
            for which, gg in ((u, g), (u + 8, jnp.where(u < 4, g_1, g_2))):
                o_tile = o_all.at[gg, rows, :]
                pltpu.make_async_copy(o_tile, o_tile, o_send.at[which]).wait()
            return carry

        lax.fori_loop(0, 8, sent, 0)


def solution(mesh):
    def local_block(hidden, seg_ids, w_q, b_q, w_kv, b_kv, w_o, b_o, ln_gain, ln_bias):
        tok, d_model = hidden.shape
        width = w_q.shape[1]
        heads = width // HEAD_DIM
        tile = tok // 4
        hbm = pl.BlockSpec(memory_space=pltpu.HBM)
        vmem = pl.BlockSpec(memory_space=pltpu.VMEM)
        dma = pltpu.SemaphoreType.DMA
        far = lambda a: pltpu.with_memory_space_constraint(a, pltpu.HBM)
        return pl.pallas_call(
            kernel,
            out_shape=(jax.ShapeDtypeStruct((tok, d_model), BF16), jax.ShapeDtypeStruct((tok, HEAD_DIM), BF16),
                       jax.ShapeDtypeStruct((tok, HEAD_DIM), BF16)),
            in_specs=[hbm] * 10,
            out_specs=(vmem, vmem, vmem),
            scratch_shapes=[
                pltpu.VMEM((tok, d_model), BF16),
                pltpu.VMEM((tok, d_model), BF16),
                pltpu.VMEM((d_model, 2 * HEAD_DIM), BF16),
                pltpu.VMEM((2, d_model, width), BF16),
                pltpu.VMEM((4 * width, d_model), BF16),
                pltpu.VMEM((width,), BF16),
                pltpu.VMEM((width,), BF16),
                pltpu.VMEM((2 * HEAD_DIM,), BF16),
                pltpu.VMEM((d_model,), BF16),
                pltpu.VMEM((d_model,), BF16),
                pltpu.VMEM((d_model,), BF16),
                pltpu.VMEM((4, 1, tok), jnp.int32),
                pltpu.VMEM((4, tile, tile), jnp.int32),
                pltpu.VMEM((4, 2, tok, HEAD_DIM), BF16),
                pltpu.VMEM((8, heads * tile, HEAD_DIM), BF16),
                pltpu.VMEM((4, tok, width), BF16),
                pltpu.VMEM((4, tok, d_model), BF16),
                pltpu.VMEM((heads * tile, HEAD_DIM), F32),
                pltpu.VMEM((heads * tile, HEAD_DIM), F32),
                pltpu.VMEM((heads * tile, HEAD_DIM), F32),
                dma((10,)), dma((N_SENDS,)), dma((16,)), dma(()), dma((4,)), dma((4,)), dma((8,)), dma((4, 8)), dma((8,)),
            ],
            compiler_params=pltpu.CompilerParams(collective_id=0, has_side_effects=True, vmem_limit_bytes=44 * 2 ** 20),
            name='block',
        )(far(hidden), far(seg_ids.reshape(1, -1)), far(w_q), far(b_q), far(w_kv), far(b_kv), far(w_o), far(b_o), far(ln_gain), far(ln_bias))

    row_spec = P(('dp', 'cp'), None)
    tok_spec = P(('dp', 'cp'))
    return jax.shard_map(local_block, mesh=mesh,
                         in_specs=(row_spec, tok_spec, P(None, 'tp'), P('tp'), P(None, None), P(None), P('tp', None), P(None), P(None), P(None)),
                         out_specs=(row_spec, row_spec, row_spec), check_vma=False)
```

```python
import functools
import jax
import jax.numpy as jnp
from jax import lax
from jax.experimental import pallas as pl
from jax.experimental.pallas import tpu as pltpu
from jax.sharding import PartitionSpec as P

HEAD_DIM = 128
LN_EPS = 1e-5
SCORE_SCALE = HEAD_DIM ** -0.5 * 1.4426950408889634
MESH = pl.DeviceIdType.MESH
BF16 = jnp.bfloat16
F32 = jnp.float32


class Sends:
    def __init__(self, sems):
        self.sems, self.made, self.under = sems, [], None

    def go(self, src, dst, recv, to, cond=None):
        slot = len(self.made)
        make = lambda: pltpu.make_async_remote_copy(src_ref=src(), dst_ref=dst(), send_sem=self.sems.at[slot], recv_sem=recv(),
                                                    device_id=to, device_id_type=MESH)
        self.made.append((make, cond, self.under))
        if cond is None:
            make().start()
        else:
            pl.when(cond())(lambda: make().start())

    def finish(self):
        for make, cond, under in self.made:
            if cond is None and under is None:
                make().wait_send()
            else:
                both = under if cond is None else cond() if under is None else cond() & under
                pl.when(both)(lambda: make().wait_send())


def scoped(fn):
    def run(*about):
        with jax.named_scope(fn.__name__ + '_'.join(a for a in about if isinstance(a, str))):
            return fn(*about)
    return run


def arrived(dst, recv):
    pltpu.make_async_copy(dst, dst, recv).wait()


N_SENDS = 64


def kernel(hid_hbm, seg_hbm, wq_hbm, bq_hbm, wkv_hbm, bkv_hbm, wo_hbm, bo_hbm, gain_hbm, lnb_hbm,
           y_ref, k_ref, v_ref,
           hid, normed, wkv, wq, wo, bq_own, bq_pair, bkv_ref, bo_ref, gain_ref, lnb_ref, seg, segcol, kv, q_s, o_all, part, m_s, l_s, acc_s,
           load_sem, send_sem, o_send, bq_recv, seg_recv, kv_recv, wq_recv, wo_recv, o_recv):
    tok, d_model = hid.shape
    width = wq.shape[2]
    heads = width // HEAD_DIM
    tile = tok // 4
    q_rows, o_rows = d_model // 8, width // 8
    dp, z, cp = lax.axis_index('dp'), lax.axis_index('tp'), lax.axis_index('cp')
    y, c = cp // 2, cp % 2
    pair = z + 1 - 2 * (z % 2)
    below, above = {'tp': z - 1}, {'tp': z + 1}
    to_x, to_y, to_core = {'dp': 1 - dp}, {'cp': cp + 2 - 4 * y}, {'cp': cp + 1 - 2 * c}
    pos = lambda px, py, pc: px * 4 + py * 2 + pc
    p_me, p_x, p_y, p_d = pos(dp, y, c), pos(1 - dp, y, c), pos(dp, 1 - y, c), pos(1 - dp, 1 - y, c)
    g_a = 1 + z % 2
    g_c = 3 - 3 * (z // 2)
    g_b = 6 - z - g_a - g_c
    sends = Sends(send_sem)

    loads = [pltpu.make_async_copy(hid_hbm, hid, load_sem.at[0]),
             pltpu.make_async_copy(wkv_hbm, wkv, load_sem.at[1]),
             pltpu.make_async_copy(wq_hbm, wq.at[0], load_sem.at[2]),
             pltpu.make_async_copy(bq_hbm, bq_own, load_sem.at[3]),
             pltpu.make_async_copy(seg_hbm, seg.at[cp], load_sem.at[4]),
             pltpu.make_async_copy(wo_hbm, wo.at[pl.ds(z * width, width), :], load_sem.at[5]),
             pltpu.make_async_copy(gain_hbm, gain_ref, load_sem.at[6]),
             pltpu.make_async_copy(lnb_hbm, lnb_ref, load_sem.at[7]),
             pltpu.make_async_copy(bkv_hbm, bkv_ref, load_sem.at[8]),
             pltpu.make_async_copy(bo_hbm, bo_ref, load_sem.at[9])]
    for load in loads:
        load.start()

    barrier = pltpu.get_barrier_semaphore()
    for step in (1, 2, 3):
        pl.semaphore_signal(barrier, inc=1, device_id={'cp': (cp + step) % 4}, device_id_type=MESH)
    pl.semaphore_signal(barrier, inc=1, device_id=to_x, device_id_type=MESH)

    @pl.when(z > 0)
    def _():
        pl.semaphore_signal(barrier, inc=1, device_id={'tp': z - 1}, device_id_type=MESH)

    @pl.when(z < 3)
    def _():
        pl.semaphore_signal(barrier, inc=1, device_id={'tp': z + 1}, device_id_type=MESH)

    with jax.named_scope('barr'):
        pl.semaphore_wait(barrier, 5 + (z + 1) // 2 - 2 * (z // 3))

    wq_piece = lambda p: wq.at[1, pl.ds(p * q_rows, q_rows), :]
    wo_piece = lambda g, p: wo.at[pl.ds(g * width + p * o_rows, o_rows), :]

    own_q, own_o = lambda: wq_hbm.at[pl.ds(p_me * q_rows, q_rows), :], lambda: wo_hbm.at[pl.ds(p_me * o_rows, o_rows), :]
    sends.go(lambda: bq_hbm, lambda: bq_pair, lambda: bq_recv, {'tp': pair})
    sends.go(own_q, lambda: wq_piece(p_me), lambda: wq_recv.at[p_me], {'tp': pair})
    sends.go(own_o, lambda: wo_piece(z, p_me), lambda: wo_recv.at[z, p_me], {'tp': z - 1}, lambda: z > 0)
    sends.go(own_o, lambda: wo_piece(z, p_me), lambda: wo_recv.at[z, p_me], {'tp': z + 1}, lambda: z < 3)
    for step in (1, 2, 3):
        sends.go(lambda: seg_hbm, lambda: seg.at[cp], lambda: seg_recv.at[cp], {'cp': cp + step}, lambda step=step: cp + step < 4)

    def pass_on(piece, recv, source, g=None):
        p = {'z': p_me, 'x': p_x, 'y': p_y, 'd': p_d}[source]
        src, sem = lambda: piece(p), lambda: recv(p)
        arrived(src(), sem())
        if source == 'z':
            if g is not None:
                sends.go(src, src, sem, below, lambda: (g > z) & (z > 0))
                sends.go(src, src, sem, above, lambda: (g < z) & (z < 3))
            sends.go(src, src, sem, to_x)
            sends.go(src, src, sem, to_y)
        elif source == 'x':
            sends.go(src, src, sem, to_y, lambda: c == 1)
        elif source == 'y':
            sends.go(src, src, sem, to_x, lambda: c == 0)
        sends.go(src, src, sem, to_core)

    @scoped
    def from_core(piece, recv):
        for px in (0, 1):
            for py in (0, 1):
                p = pos(px, py, 1 - c)
                arrived(piece(p), recv(p))

    @scoped
    def q_event(*sources):
        for source in sources:
            pass_on(wq_piece, lambda p: wq_recv.at[p], source)

    @scoped
    def o_event(g, *sources):
        for source in sources:
            pass_on(functools.partial(wo_piece, g), lambda p: wo_recv.at[g, p], source, g)

    with jax.named_scope('load_wait'):
        for i in (0, 6, 7):
            loads[i].wait()
    gain = gain_ref[...].astype(F32)
    lnb = lnb_ref[...].astype(F32)
    ln_rows = min(64, tok)

    def ln_step(i, carry):
        rows = pl.ds(pl.multiple_of(i * ln_rows, ln_rows), ln_rows)
        x = hid[rows, :].astype(F32)
        cen = x - jnp.mean(x, axis=-1, keepdims=True)
        var = jnp.mean(cen * cen, axis=-1, keepdims=True)
        normed[rows, :] = (cen * lax.rsqrt(var + LN_EPS) * gain + lnb).astype(BF16)
        return carry

    with jax.named_scope('ln'):
        lax.fori_loop(0, tok // ln_rows, ln_step, 0)

    loads[1].wait()
    loads[8].wait()
    kv_new = (jnp.dot(normed[...], wkv[...], preferred_element_type=F32) + bkv_ref[...].astype(F32)).astype(BF16)
    kv[cp, 0] = kv_new[:, :HEAD_DIM]
    kv[cp, 1] = kv_new[:, HEAD_DIM:]
    k_ref[...] = kv_new[:, :HEAD_DIM]
    v_ref[...] = kv_new[:, HEAD_DIM:]

    @scoped
    def project_q(which, bias):
        qf = jnp.dot(normed[...], wq[which], preferred_element_type=F32) + bias[...].astype(F32)
        for r in range(4):
            for h in range(heads):
                q_s[which * 4 + r, h * tile:(h + 1) * tile, :] = qf[r * tile:(r + 1) * tile, h * HEAD_DIM:(h + 1) * HEAD_DIM].astype(BF16)

    loads[2].wait()
    loads[3].wait()
    sends.go(lambda: kv.at[cp], lambda: kv.at[cp], lambda: kv_recv.at[cp], to_core, lambda: c == 0)
    sends.go(lambda: kv.at[cp], lambda: kv.at[cp], lambda: kv_recv.at[cp], to_y, lambda: y == 0)
    project_q(0, bq_own)
    loads[4].wait()
    for r in range(4):
        row = jnp.broadcast_to(seg[cp, :, r * tile:(r + 1) * tile], (tile, tile))
        segcol[r] = row.T

    g_1, g_2 = 2 - z // 2, 3 - 3 * (z // 2)
    middle, edge = (z > 0) & (z < 3), (z == 0) | (z == 3)
    tile_rows = lambda r: pl.ds(pl.multiple_of(r * tile, tile), tile)
    every = pl.ds(0, tok)

    def scores(q, k_blk, mask):
        keys = k_blk.shape[0]
        s = lax.dot_general(q, k_blk, (((1,), (1,)), ((), ())), preferred_element_type=F32) * SCORE_SCALE
        return jnp.where(mask[None], s.reshape(heads, tile, keys), -jnp.inf).reshape(heads * tile, keys)

    @scoped
    def attend_own(t, carry):
        r = t % 4
        k_pos = lax.broadcasted_iota(jnp.int32, (tile, tok), 1)
        q_pos = lax.broadcasted_iota(jnp.int32, (tile, tok), 0) + r * tile
        s = scores(q_s[t], kv[cp, 0], (seg[cp] == segcol[r][:, :1]) & (k_pos <= q_pos))
        m_new = jnp.max(s, axis=-1, keepdims=True)
        p = jnp.exp2(s - m_new)
        m_s[r] = jnp.broadcast_to(m_new, m_s.shape[1:])
        l_s[r] = jnp.broadcast_to(jnp.sum(p, axis=-1, keepdims=True), l_s.shape[1:])
        acc_s[r] = jnp.dot(p.astype(BF16), kv[cp, 1], preferred_element_type=F32)
        return carry

    @scoped
    def attend_earlier(t, g):
        r = t % 4
        q = q_s[t]
        seg_q = segcol[r][:, :1]

        def block(j, inner):
            s = scores(q, kv[j, 0], seg[j] == seg_q)
            m_prev = m_s[r]
            m_new = jnp.maximum(m_prev, jnp.max(s, axis=-1, keepdims=True))
            p = jnp.exp2(s - m_new[:, :1])
            alpha = jnp.exp2(m_prev - m_new)
            m_s[r] = m_new
            l_s[r] = l_s[r] * alpha + jnp.sum(p, axis=-1, keepdims=True)
            acc_s[r] = acc_s[r] * alpha + jnp.dot(p.astype(BF16), kv[j, 1], preferred_element_type=F32)
            return inner

        lax.fori_loop(0, cp, block, 0)
        for h in range(heads):
            at = slice(h * tile, (h + 1) * tile)
            o_all[g, tile_rows(r), h * HEAD_DIM:(h + 1) * HEAD_DIM] = (acc_s[r, at, :] / l_s[r, at, :]).astype(BF16)

    def send_heads(t, g):
        o_tile = o_all.at[g, tile_rows(t % 4), :]
        copy = pltpu.make_async_remote_copy(src_ref=o_tile, dst_ref=o_tile, send_sem=o_send.at[t], recv_sem=o_recv.at[t],
                                            device_id={'tp': 3 - z}, device_id_type=MESH)
        pl.when(middle)(lambda: copy.start())

    @scoped
    def heads_event(u):
        o_tile = o_all.at[g_1 if u < 4 else g_2, tile_rows(u % 4), :]
        arrived(o_tile, o_recv.at[u])
        for to, cond in ((0, z == 1), (3, z == 2)):
            copy = pltpu.make_async_remote_copy(src_ref=o_tile, dst_ref=o_tile, send_sem=o_send.at[8 + u], recv_sem=o_recv.at[u],
                                                device_id={'tp': to}, device_id_type=MESH)
            pl.when(cond)(lambda copy=copy: copy.start())

    def heads_here(*tiles):
        pl.when(middle)(lambda: [heads_event(u) for u in tiles] and None)

    def on(cond, what, *about):
        sends.under = cond
        pl.when(cond)(lambda: what(*about))
        sends.under = None

    n_col = min(512, d_model)

    @scoped
    def project_o(g, rows):
        def cols(n, carry):
            at = pl.ds(pl.multiple_of(n * n_col, n_col), n_col)
            part[g, rows, at] = jnp.dot(o_all[g, rows, :], wo[pl.ds(pl.multiple_of(g * width, width), width), at],
                                        preferred_element_type=F32).astype(BF16)
            return carry

        lax.fori_loop(0, d_model // n_col, cols, 0)

    wo_whole = lambda g: from_core(functools.partial(wo_piece, g), lambda p: wo_recv.at[g, p])

    lax.fori_loop(0, 4, attend_own, 0)
    q_event('z')

    with jax.named_scope('kvf'):
        pl.when(y == 1)(lambda: arrived(kv.at[c], kv_recv.at[c]))
        sends.go(lambda: kv.at[c], lambda: kv.at[c], lambda: kv_recv.at[c], to_core, lambda: y == 1)
    on(middle, o_event, g_a, 'z')
    with jax.named_scope('kvw'):
        for j in range(3):
            pl.when(j < cp)(functools.partial(arrived, seg.at[j], seg_recv.at[j]))
        pl.when(y == 1)(lambda: arrived(kv.at[1 - c], kv_recv.at[1 - c]))
        pl.when(c == 1)(lambda: arrived(kv.at[cp - 1], kv_recv.at[cp - 1]))

    def own_heads(t, carry):
        attend_earlier(t, z)

        @pl.when(t == 0)
        def _():
            on(edge, o_event, g_a, 'z')
            on(middle, o_event, g_b, 'z')

        @pl.when(t == 1)
        def _():
            q_event('x', 'y')

        @pl.when(t == 2)
        def _():
            on(edge, o_event, g_b, 'z')
            heads_here(0)

        @pl.when(t == 3)
        def _():
            o_event(g_a, 'x', 'y')
            heads_here(1)
            on(middle, o_event, g_c, 'z')

        send_heads(t, z)
        return carry

    lax.fori_loop(0, 4, own_heads, 0)
    loads[5].wait()
    loads[9].wait()
    project_o(z, every)
    heads_here(2)
    q_event('d')
    from_core(wq_piece, lambda p: wq_recv.at[p])
    arrived(bq_pair, bq_recv)
    project_q(1, bq_pair)
    heads_here(3)
    lax.fori_loop(4, 8, attend_own, 0)
    o_event(g_b, 'x', 'y')
    on(edge, o_event, g_c, 'z')

    def pair_heads(t, carry):
        attend_earlier(t, pair)

        @pl.when(t == 4)
        def _():
            o_event(g_a, 'd')

        @pl.when(t == 5)
        def _():
            o_event(g_c, 'x', 'y')

        @pl.when(t == 6)
        def _():
            heads_here(4)
            o_event(g_b, 'd')

        @pl.when(t == 7)
        def _():
            heads_here(5)

        send_heads(t, pair)
        return carry

    lax.fori_loop(4, 8, pair_heads, 0)
    heads_here(6, 7)
    o_event(g_c, 'd')
    wo_whole(g_a)
    wo_whole(g_b)
    project_o(pair, every)

    def edge_heads(*tiles):
        pl.when(edge)(lambda: [heads_event(u) for u in tiles] and None)

    edge_heads(0, 1, 2, 3)
    project_o(g_1, every)
    wo_whole(g_c)

    @scoped
    def last(r, carry):
        pl.when(edge)(lambda: arrived(o_all.at[g_2, tile_rows(r), :], o_recv.at[4 + r]))
        project_o(g_2, tile_rows(r))

        def finish(i, inner):
            f_rows = tile // 4
            at = pl.ds(pl.multiple_of(r * tile + i * f_rows, f_rows), f_rows)
            total = part[0, at, :].astype(F32)
            for gg in (1, 2, 3):
                total = total + part[gg, at, :].astype(F32)
            y_ref[at, :] = (hid[at, :].astype(F32) + total + bo_ref[...].astype(F32)).astype(BF16)
            return inner

        lax.fori_loop(0, 4, finish, 0)
        return carry

    lax.fori_loop(0, 4, last, 0)

    with jax.named_scope('drain'):
        sends.finish()

    @pl.when((z > 0) & (z < 3))
    def _():
        def sent(u, carry):
            for which, gg in ((u, jnp.where(u < 4, z, pair)), (u + 8, jnp.where(u < 4, g_1, g_2))):
                o_tile = o_all.at[gg, tile_rows(u % 4), :]
                pltpu.make_async_copy(o_tile, o_tile, o_send.at[which]).wait()
            return carry

        lax.fori_loop(0, 8, sent, 0)


def solution(mesh):
    def local_block(hidden, seg_ids, w_q, b_q, w_kv, b_kv, w_o, b_o, ln_gain, ln_bias):
        tok, d_model = hidden.shape
        width = w_q.shape[1]
        heads = width // HEAD_DIM
        tile = tok // 4
        hbm = pl.BlockSpec(memory_space=pltpu.HBM)
        vmem = pl.BlockSpec(memory_space=pltpu.VMEM)
        dma = pltpu.SemaphoreType.DMA
        far = lambda a: pltpu.with_memory_space_constraint(a, pltpu.HBM)
        return pl.pallas_call(
            kernel,
            out_shape=(jax.ShapeDtypeStruct((tok, d_model), BF16), jax.ShapeDtypeStruct((tok, HEAD_DIM), BF16),
                       jax.ShapeDtypeStruct((tok, HEAD_DIM), BF16)),
            in_specs=[hbm] * 10,
            out_specs=(vmem, vmem, vmem),
            scratch_shapes=[
                pltpu.VMEM((tok, d_model), BF16),
                pltpu.VMEM((tok, d_model), BF16),
                pltpu.VMEM((d_model, 2 * HEAD_DIM), BF16),
                pltpu.VMEM((2, d_model, width), BF16),
                pltpu.VMEM((4 * width, d_model), BF16),
                pltpu.VMEM((width,), BF16),
                pltpu.VMEM((width,), BF16),
                pltpu.VMEM((2 * HEAD_DIM,), BF16),
                pltpu.VMEM((d_model,), BF16),
                pltpu.VMEM((d_model,), BF16),
                pltpu.VMEM((d_model,), BF16),
                pltpu.VMEM((4, 1, tok), jnp.int32),
                pltpu.VMEM((4, tile, tile), jnp.int32),
                pltpu.VMEM((4, 2, tok, HEAD_DIM), BF16),
                pltpu.VMEM((8, heads * tile, HEAD_DIM), BF16),
                pltpu.VMEM((4, tok, width), BF16),
                pltpu.VMEM((4, tok, d_model), BF16),
                pltpu.VMEM((4, heads * tile, HEAD_DIM), F32),
                pltpu.VMEM((4, heads * tile, HEAD_DIM), F32),
                pltpu.VMEM((4, heads * tile, HEAD_DIM), F32),
                dma((10,)), dma((N_SENDS,)), dma((16,)), dma(()), dma((4,)), dma((4,)), dma((8,)), dma((4, 8)), dma((8,)),
            ],
            compiler_params=pltpu.CompilerParams(collective_id=0, has_side_effects=True, vmem_limit_bytes=48 * 2 ** 20),
            name='block',
        )(far(hidden), far(seg_ids.reshape(1, -1)), far(w_q), far(b_q), far(w_kv), far(b_kv), far(w_o), far(b_o), far(ln_gain), far(ln_bias))

    row_spec = P(('dp', 'cp'), None)
    tok_spec = P(('dp', 'cp'))
    return jax.shard_map(local_block, mesh=mesh,
                         in_specs=(row_spec, tok_spec, P(None, 'tp'), P('tp'), P(None, None), P(None), P('tp', None), P(None), P(None), P(None)),
                         out_specs=(row_spec, row_spec, row_spec), check_vma=False)
```

```python
import functools
import jax
import jax.numpy as jnp
from jax import lax
from jax.experimental import pallas as pl
from jax.experimental.pallas import tpu as pltpu
from jax.sharding import PartitionSpec as P

HEAD_DIM = 128
LN_EPS = 1e-5
SCORE_SCALE = HEAD_DIM ** -0.5 * 1.4426950408889634
MESH = pl.DeviceIdType.MESH
BF16 = jnp.bfloat16
F32 = jnp.float32


class Sends:
    def __init__(self, sems):
        self.sems, self.made, self.keys = sems, [], {}

    def go(self, src, dst, recv, to, cond=None, key=None):
        slot = self.keys.get(key, len(self.made)) if key else len(self.made)
        make = lambda: pltpu.make_async_remote_copy(src_ref=src(), dst_ref=dst(), send_sem=self.sems.at[slot], recv_sem=recv(),
                                                    device_id=to, device_id_type=MESH)
        if slot == len(self.made):
            self.made.append((make, cond))
            if key:
                self.keys[key] = slot
        if cond is None:
            make().start()
        else:
            pl.when(cond())(lambda: make().start())

    def finish(self):
        for make, cond in self.made:
            if cond is None:
                make().wait_send()
            else:
                pl.when(cond())(lambda: make().wait_send())


def scoped(fn):
    def run(*about):
        with jax.named_scope(fn.__name__ + '_'.join(str(a) for a in about if isinstance(a, (str, int)))):
            return fn(*about)
    return run


def arrived(dst, recv):
    pltpu.make_async_copy(dst, dst, recv).wait()


N_SENDS = 100


def kernel(hid_hbm, seg_hbm, wq_hbm, bq_hbm, wkv_hbm, bkv_hbm, wo_hbm, bo_hbm, gain_hbm, lnb_hbm,
           y_ref, k_ref, v_ref,
           hid, normed, wkv, wq, wo, bq_own, bq_pair, bkv_ref, bo_ref, gain_ref, lnb_ref, seg, segcol, kv, q_s, o_all, part, m_s, l_s, acc_s,
           load_sem, send_sem, o_send, bq_recv, seg_recv, kv_recv, wq_recv, wo_recv, o_recv):
    tok, d_model = hid.shape
    width = wq.shape[2]
    heads = width // HEAD_DIM
    tile = tok // 4
    q_rows, o_rows = d_model // 8, width // 8
    dp, z, cp = lax.axis_index('dp'), lax.axis_index('tp'), lax.axis_index('cp')
    y, c = cp // 2, cp % 2
    pair = z + 1 - 2 * (z % 2)
    below, above = {'tp': z - 1}, {'tp': z + 1}
    to_x, to_y, to_core = {'dp': 1 - dp}, {'cp': cp + 2 - 4 * y}, {'cp': cp + 1 - 2 * c}
    pos = lambda px, py, pc: px * 4 + py * 2 + pc
    p_me, p_x, p_y, p_d = pos(dp, y, c), pos(1 - dp, y, c), pos(dp, 1 - y, c), pos(1 - dp, 1 - y, c)
    g_a = 1 + z % 2
    g_c = 3 - 3 * (z // 2)
    g_b = 6 - z - g_a - g_c
    sends = Sends(send_sem)

    loads = [pltpu.make_async_copy(hid_hbm, hid, load_sem.at[0]),
             pltpu.make_async_copy(wkv_hbm, wkv, load_sem.at[1]),
             pltpu.make_async_copy(wq_hbm, wq.at[0], load_sem.at[2]),
             pltpu.make_async_copy(bq_hbm, bq_own, load_sem.at[3]),
             pltpu.make_async_copy(seg_hbm, seg.at[cp], load_sem.at[4]),
             pltpu.make_async_copy(wo_hbm, wo.at[pl.ds(z * width, width), :], load_sem.at[5]),
             pltpu.make_async_copy(gain_hbm, gain_ref, load_sem.at[6]),
             pltpu.make_async_copy(lnb_hbm, lnb_ref, load_sem.at[7]),
             pltpu.make_async_copy(bkv_hbm, bkv_ref, load_sem.at[8]),
             pltpu.make_async_copy(bo_hbm, bo_ref, load_sem.at[9])]
    for load in loads:
        load.start()

    barrier = pltpu.get_barrier_semaphore()
    for step in (1, 2, 3):
        pl.semaphore_signal(barrier, inc=1, device_id={'cp': (cp + step) % 4}, device_id_type=MESH)
    pl.semaphore_signal(barrier, inc=1, device_id=to_x, device_id_type=MESH)

    @pl.when(z > 0)
    def _():
        pl.semaphore_signal(barrier, inc=1, device_id={'tp': z - 1}, device_id_type=MESH)

    @pl.when(z < 3)
    def _():
        pl.semaphore_signal(barrier, inc=1, device_id={'tp': z + 1}, device_id_type=MESH)

    with jax.named_scope('barr'):
        pl.semaphore_wait(barrier, 5 + (z + 1) // 2 - 2 * (z // 3))

    def q_piece(p, h):
        half = q_rows // 2
        return wq.at[1, pl.ds(pl.multiple_of(p * q_rows + h * half, half), half), :]

    def o_piece(g, p, h):
        half = o_rows // 2
        return wo.at[pl.ds(pl.multiple_of(g * width + p * o_rows + h * half, half), half), :]

    q_sem, o_sem = lambda p, h: wq_recv.at[p, h], lambda g, p, h: wo_recv.at[g, p, h]

    sends.go(lambda: bq_hbm, lambda: bq_pair, lambda: bq_recv, {'tp': pair})
    for h in (0, 1):
        half = q_rows // 2
        sends.go(lambda h=h, half=half: wq_hbm.at[pl.ds(pl.multiple_of(p_me * q_rows + h * half, half), half), :],
                 lambda h=h: q_piece(p_me, h), lambda h=h: q_sem(p_me, h), {'tp': pair})
    for h in (0, 1):
        half = o_rows // 2
        own_o = lambda h=h, half=half: wo_hbm.at[pl.ds(pl.multiple_of(p_me * o_rows + h * half, half), half), :]
        sends.go(own_o, lambda h=h: o_piece(z, p_me, h), lambda h=h: o_sem(z, p_me, h), below, lambda: z > 0)
        sends.go(own_o, lambda h=h: o_piece(z, p_me, h), lambda h=h: o_sem(z, p_me, h), above, lambda: z < 3)
    for step in (1, 2, 3):
        sends.go(lambda: seg_hbm, lambda: seg.at[cp], lambda: seg_recv.at[cp], {'cp': cp + step}, lambda step=step: cp + step < 4)

    def pass_on(name, g, source, h):
        p = {'z': p_me, 's': p_me, 'x': p_x, 'y': p_y, 'd': p_d}[source]
        src = (lambda: q_piece(p, h)) if g is None else (lambda: o_piece(g, p, h))
        sem = (lambda: q_sem(p, h)) if g is None else (lambda: o_sem(g, p, h))
        if source == 's':
            sends.go(src, src, sem, to_x, None, (name, h, 'x'))
            sends.go(src, src, sem, to_y, None, (name, h, 'y'))
            return
        arrived(src(), sem())
        if source == 'z' and g is not None:
            sends.go(src, src, sem, below, lambda: (g > z) & (z > 0), (name, h, 'below'))
            sends.go(src, src, sem, above, lambda: (g < z) & (z < 3), (name, h, 'above'))
        elif source == 'x':
            sends.go(src, src, sem, to_y, lambda: c == 1, (name, h, 'xy'))
        elif source == 'y':
            sends.go(src, src, sem, to_x, lambda: c == 0, (name, h, 'yx'))
        sends.go(src, src, sem, to_core, None, (name, h, 'core' + source))

    groups = {'q': None, 'a': g_a, 'b': g_b, 'c': g_c}

    @scoped
    def ev(name, sources, *halves):
        for h in halves or (0, 1):
            for source in sources:
                pass_on(name, groups[name], source, h)

    @scoped
    def whole(name):
        for px in (0, 1):
            for py in (0, 1):
                for h in (0, 1):
                    p = pos(px, py, 1 - c)
                    if name == 'q':
                        arrived(q_piece(p, h), q_sem(p, h))
                    else:
                        arrived(o_piece(groups[name], p, h), o_sem(groups[name], p, h))

    with jax.named_scope('load_wait'):
        for i in (0, 6, 7):
            loads[i].wait()
    gain = gain_ref[...].astype(F32)
    lnb = lnb_ref[...].astype(F32)
    ln_rows = min(64, tok)

    def ln_step(i, carry):
        rows = pl.ds(pl.multiple_of(i * ln_rows, ln_rows), ln_rows)
        x = hid[rows, :].astype(F32)
        cen = x - jnp.mean(x, axis=-1, keepdims=True)
        var = jnp.mean(cen * cen, axis=-1, keepdims=True)
        normed[rows, :] = (cen * lax.rsqrt(var + LN_EPS) * gain + lnb).astype(BF16)
        return carry

    with jax.named_scope('ln'):
        lax.fori_loop(0, tok // ln_rows, ln_step, 0)

    loads[1].wait()
    loads[8].wait()
    kv_new = (jnp.dot(normed[...], wkv[...], preferred_element_type=F32) + bkv_ref[...].astype(F32)).astype(BF16)
    kv[cp, 0] = kv_new[:, :HEAD_DIM]
    kv[cp, 1] = kv_new[:, HEAD_DIM:]
    k_ref[...] = kv_new[:, :HEAD_DIM]
    v_ref[...] = kv_new[:, HEAD_DIM:]

    @scoped
    def project_q(which, bias):
        qf = jnp.dot(normed[...], wq[which], preferred_element_type=F32) + bias[...].astype(F32)
        for r in range(4):
            for h in range(heads):
                q_s[which * 4 + r, h * tile:(h + 1) * tile, :] = qf[r * tile:(r + 1) * tile, h * HEAD_DIM:(h + 1) * HEAD_DIM].astype(BF16)

    loads[2].wait()
    loads[3].wait()
    sends.go(lambda: kv.at[cp], lambda: kv.at[cp], lambda: kv_recv.at[cp], to_core, lambda: c == 0)
    sends.go(lambda: kv.at[cp], lambda: kv.at[cp], lambda: kv_recv.at[cp], to_y, lambda: y == 0)
    project_q(0, bq_own)
    loads[4].wait()
    for r in range(4):
        row = jnp.broadcast_to(seg[cp, :, r * tile:(r + 1) * tile], (tile, tile))
        segcol[r] = row.T

    g_1, g_2 = 2 - z // 2, 3 - 3 * (z // 2)
    middle, edge = (z > 0) & (z < 3), (z == 0) | (z == 3)
    tile_rows = lambda r: pl.ds(pl.multiple_of(r * tile, tile), tile)
    every = pl.ds(0, tok)

    def scores(q, k_blk, mask):
        keys = k_blk.shape[0]
        s = lax.dot_general(q, k_blk, (((1,), (1,)), ((), ())), preferred_element_type=F32) * SCORE_SCALE
        return jnp.where(mask[None], s.reshape(heads, tile, keys), -jnp.inf).reshape(heads * tile, keys)

    @scoped
    def attend_own(t, carry):
        r = t % 4
        k_pos = lax.broadcasted_iota(jnp.int32, (tile, tok), 1)
        q_pos = lax.broadcasted_iota(jnp.int32, (tile, tok), 0) + r * tile
        s = scores(q_s[t], kv[cp, 0], (seg[cp] == segcol[r][:, :1]) & (k_pos <= q_pos))
        m_new = jnp.max(s, axis=-1, keepdims=True)
        p = jnp.exp2(s - m_new)
        m_s[r] = jnp.broadcast_to(m_new, m_s.shape[1:])
        l_s[r] = jnp.broadcast_to(jnp.sum(p, axis=-1, keepdims=True), l_s.shape[1:])
        acc_s[r] = jnp.dot(p.astype(BF16), kv[cp, 1], preferred_element_type=F32)
        return carry

    @scoped
    def attend_earlier(t, g):
        r = t % 4
        q = q_s[t]
        seg_q = segcol[r][:, :1]

        def block(j, inner):
            s = scores(q, kv[j, 0], seg[j] == seg_q)
            m_prev = m_s[r]
            m_new = jnp.maximum(m_prev, jnp.max(s, axis=-1, keepdims=True))
            p = jnp.exp2(s - m_new[:, :1])
            alpha = jnp.exp2(m_prev - m_new)
            m_s[r] = m_new
            l_s[r] = l_s[r] * alpha + jnp.sum(p, axis=-1, keepdims=True)
            acc_s[r] = acc_s[r] * alpha + jnp.dot(p.astype(BF16), kv[j, 1], preferred_element_type=F32)
            return inner

        lax.fori_loop(0, cp, block, 0)
        for h in range(heads):
            at = slice(h * tile, (h + 1) * tile)
            o_all[g, tile_rows(r), h * HEAD_DIM:(h + 1) * HEAD_DIM] = (acc_s[r, at, :] / l_s[r, at, :]).astype(BF16)

    def send_heads(t, g):
        o_tile = o_all.at[g, tile_rows(t % 4), :]
        copy = pltpu.make_async_remote_copy(src_ref=o_tile, dst_ref=o_tile, send_sem=o_send.at[t], recv_sem=o_recv.at[t],
                                            device_id={'tp': 3 - z}, device_id_type=MESH)
        pl.when(middle)(lambda: copy.start())

    @scoped
    def heads_event(u):
        o_tile = o_all.at[g_1 if u < 4 else g_2, tile_rows(u % 4), :]
        arrived(o_tile, o_recv.at[u])
        for to, cond in ((0, z == 1), (3, z == 2)):
            copy = pltpu.make_async_remote_copy(src_ref=o_tile, dst_ref=o_tile, send_sem=o_send.at[8 + u], recv_sem=o_recv.at[u],
                                                device_id={'tp': to}, device_id_type=MESH)
            pl.when(cond)(lambda copy=copy: copy.start())

    def heads_here(*tiles):
        on(middle, *((heads_event, u) for u in tiles))

    def on(cond, *todo):
        @pl.when(cond)
        def _():
            for what, *about in todo:
                what(*about)

    n_col = min(512, d_model)

    @scoped
    def project_o(g, rows):
        def cols(n, carry):
            at = pl.ds(pl.multiple_of(n * n_col, n_col), n_col)
            part[g, rows, at] = jnp.dot(o_all[g, rows, :], wo[pl.ds(pl.multiple_of(g * width, width), width), at],
                                        preferred_element_type=F32).astype(BF16)
            return carry

        lax.fori_loop(0, d_model // n_col, cols, 0)

    def own_block(t, carry):
        attend_own(t, carry)
        on(t == 0, (ev, 'q', 'zs', 0))
        return carry

    lax.fori_loop(0, 4, own_block, 0)
    ev('q', 'zs', 1)
    on(middle, (ev, 'a', 'z'))

    with jax.named_scope('kvf'):
        pl.when(y == 1)(lambda: arrived(kv.at[c], kv_recv.at[c]))
        sends.go(lambda: kv.at[c], lambda: kv.at[c], lambda: kv_recv.at[c], to_core, lambda: y == 1)
    ev('q', 'xy', 0)
    with jax.named_scope('kvw'):
        for j in range(3):
            pl.when(j < cp)(functools.partial(arrived, seg.at[j], seg_recv.at[j]))
        pl.when(y == 1)(lambda: arrived(kv.at[1 - c], kv_recv.at[1 - c]))
        pl.when(c == 1)(lambda: arrived(kv.at[cp - 1], kv_recv.at[cp - 1]))

    def own_heads(t, carry):
        attend_earlier(t, z)
        send_heads(t, z)

        @pl.when(t == 0)
        def _():
            ev('q', 'xy', 1)
            on(middle, (ev, 'a', 's'), (ev, 'b', 'z'))
            on(edge, (ev, 'a', 'zs'))

        @pl.when(t == 1)
        def _():
            ev('q', 'd')
            on(middle, (ev, 'b', 's'), (ev, 'c', 'z'))

        @pl.when(t == 2)
        def _():
            on(middle, (ev, 'c', 's'))
            on(edge, (ev, 'b', 'zs'))

        on(t == 3, (ev, 'a', 'xy'))
        return carry

    lax.fori_loop(0, 4, own_heads, 0)
    whole('q')
    arrived(bq_pair, bq_recv)
    project_q(1, bq_pair)
    on(edge, (ev, 'c', 'zs'))
    lax.fori_loop(4, 8, attend_own, 0)
    ev('a', 'd')
    heads_here(0, 1)
    ev('b', 'xy')

    def pair_heads(t, carry):
        attend_earlier(t, pair)
        send_heads(t, pair)
        on(t == 4, (heads_here, 2, 3))
        on(t == 5, (ev, 'b', 'd'), (ev, 'c', 'xy'))
        on(t == 6, (heads_here, 4))
        on(t == 7, (heads_here, 5))
        return carry

    lax.fori_loop(4, 8, pair_heads, 0)
    loads[5].wait()
    loads[9].wait()
    project_o(z, every)
    heads_here(6)
    ev('c', 'd')
    whole('a')
    whole('b')
    project_o(pair, every)
    heads_here(7)
    on(edge, *((heads_event, u) for u in range(4)))
    project_o(g_1, every)
    whole('c')

    @scoped
    def last(r, carry):
        pl.when(edge)(lambda: arrived(o_all.at[g_2, tile_rows(r), :], o_recv.at[4 + r]))
        project_o(g_2, tile_rows(r))

        def finish(i, inner):
            f_rows = tile // 4
            at = pl.ds(pl.multiple_of(r * tile + i * f_rows, f_rows), f_rows)
            total = part[0, at, :].astype(F32)
            for gg in (1, 2, 3):
                total = total + part[gg, at, :].astype(F32)
            y_ref[at, :] = (hid[at, :].astype(F32) + total + bo_ref[...].astype(F32)).astype(BF16)
            return inner

        lax.fori_loop(0, 4, finish, 0)
        return carry

    lax.fori_loop(0, 4, last, 0)

    with jax.named_scope('drain'):
        sends.finish()

    @pl.when((z > 0) & (z < 3))
    def _():
        def sent(u, carry):
            for which, gg in ((u, jnp.where(u < 4, z, pair)), (u + 8, jnp.where(u < 4, g_1, g_2))):
                o_tile = o_all.at[gg, tile_rows(u % 4), :]
                pltpu.make_async_copy(o_tile, o_tile, o_send.at[which]).wait()
            return carry

        lax.fori_loop(0, 8, sent, 0)


def solution(mesh):
    def local_block(hidden, seg_ids, w_q, b_q, w_kv, b_kv, w_o, b_o, ln_gain, ln_bias):
        tok, d_model = hidden.shape
        width = w_q.shape[1]
        heads = width // HEAD_DIM
        tile = tok // 4
        hbm = pl.BlockSpec(memory_space=pltpu.HBM)
        vmem = pl.BlockSpec(memory_space=pltpu.VMEM)
        dma = pltpu.SemaphoreType.DMA
        far = lambda a: pltpu.with_memory_space_constraint(a, pltpu.HBM)
        return pl.pallas_call(
            kernel,
            out_shape=(jax.ShapeDtypeStruct((tok, d_model), BF16), jax.ShapeDtypeStruct((tok, HEAD_DIM), BF16),
                       jax.ShapeDtypeStruct((tok, HEAD_DIM), BF16)),
            in_specs=[hbm] * 10,
            out_specs=(vmem, vmem, vmem),
            scratch_shapes=[
                pltpu.VMEM((tok, d_model), BF16),
                pltpu.VMEM((tok, d_model), BF16),
                pltpu.VMEM((d_model, 2 * HEAD_DIM), BF16),
                pltpu.VMEM((2, d_model, width), BF16),
                pltpu.VMEM((4 * width, d_model), BF16),
                pltpu.VMEM((width,), BF16),
                pltpu.VMEM((width,), BF16),
                pltpu.VMEM((2 * HEAD_DIM,), BF16),
                pltpu.VMEM((d_model,), BF16),
                pltpu.VMEM((d_model,), BF16),
                pltpu.VMEM((d_model,), BF16),
                pltpu.VMEM((4, 1, tok), jnp.int32),
                pltpu.VMEM((4, tile, tile), jnp.int32),
                pltpu.VMEM((4, 2, tok, HEAD_DIM), BF16),
                pltpu.VMEM((8, heads * tile, HEAD_DIM), BF16),
                pltpu.VMEM((4, tok, width), BF16),
                pltpu.VMEM((4, tok, d_model), BF16),
                pltpu.VMEM((4, heads * tile, HEAD_DIM), F32),
                pltpu.VMEM((4, heads * tile, HEAD_DIM), F32),
                pltpu.VMEM((4, heads * tile, HEAD_DIM), F32),
                dma((10,)), dma((N_SENDS,)), dma((16,)), dma(()), dma((4,)), dma((4,)), dma((8, 2)), dma((4, 8, 2)), dma((8,)),
            ],
            compiler_params=pltpu.CompilerParams(collective_id=0, has_side_effects=True, vmem_limit_bytes=48 * 2 ** 20),
            name='block',
        )(far(hidden), far(seg_ids.reshape(1, -1)), far(w_q), far(b_q), far(w_kv), far(b_kv), far(w_o), far(b_o), far(ln_gain), far(ln_bias))

    row_spec = P(('dp', 'cp'), None)
    tok_spec = P(('dp', 'cp'))
    return jax.shard_map(local_block, mesh=mesh,
                         in_specs=(row_spec, tok_spec, P(None, 'tp'), P('tp'), P(None, None), P(None), P('tp', None), P(None), P(None), P(None)),
                         out_specs=(row_spec, row_spec, row_spec), check_vma=False)
```

```python
import functools
import jax
import jax.numpy as jnp
from jax import lax
from jax.experimental import pallas as pl
from jax.experimental.pallas import tpu as pltpu
from jax.sharding import PartitionSpec as P

HEAD_DIM = 128
LN_EPS = 1e-5
SCORE_SCALE = HEAD_DIM ** -0.5 * 1.4426950408889634
MESH = pl.DeviceIdType.MESH
BF16 = jnp.bfloat16
F32 = jnp.float32


class Sends:
    def __init__(self, sems):
        self.sems, self.made, self.keys = sems, [], {}

    def go(self, src, dst, recv, to, cond=None, key=None):
        slot = self.keys.get(key, len(self.made)) if key else len(self.made)
        make = lambda: pltpu.make_async_remote_copy(src_ref=src(), dst_ref=dst(), send_sem=self.sems.at[slot], recv_sem=recv(),
                                                    device_id=to, device_id_type=MESH)
        if slot == len(self.made):
            self.made.append((make, cond))
            if key:
                self.keys[key] = slot
        if cond is None:
            make().start()
        else:
            pl.when(cond())(lambda: make().start())

    def finish(self):
        for make, cond in self.made:
            if cond is None:
                make().wait_send()
            else:
                pl.when(cond())(lambda: make().wait_send())


def scoped(fn):
    def run(*about):
        with jax.named_scope(fn.__name__ + '_'.join(str(a) for a in about if isinstance(a, (str, int)))):
            return fn(*about)
    return run


def arrived(dst, recv):
    pltpu.make_async_copy(dst, dst, recv).wait()


N_SENDS = 100


def kernel(hid_hbm, seg_hbm, wq_hbm, bq_hbm, wkv_hbm, bkv_hbm, wo_hbm, bo_hbm, gain_hbm, lnb_hbm,
           y_ref, k_ref, v_ref,
           hid, normed, wkv, wq, wo, bq_own, bq_pair, bkv_ref, bo_ref, gain_ref, lnb_ref, seg, segcol, kv, q_s, o_all, part, m_s, l_s, acc_s,
           load_sem, send_sem, o_send, bq_recv, seg_recv, kv_recv, wq_recv, wo_recv, o_recv):
    tok, d_model = hid.shape
    width = wq.shape[2]
    heads = width // HEAD_DIM
    tile = tok // 4
    q_rows, o_rows = d_model // 8, width // 8
    dp, z, cp = lax.axis_index('dp'), lax.axis_index('tp'), lax.axis_index('cp')
    y, c = cp // 2, cp % 2
    pair = z + 1 - 2 * (z % 2)
    below, above = {'tp': z - 1}, {'tp': z + 1}
    to_x, to_y, to_core = {'dp': 1 - dp}, {'cp': cp + 2 - 4 * y}, {'cp': cp + 1 - 2 * c}
    pos = lambda px, py, pc: px * 4 + py * 2 + pc
    p_me, p_x, p_y, p_d = pos(dp, y, c), pos(1 - dp, y, c), pos(dp, 1 - y, c), pos(1 - dp, 1 - y, c)
    g_a = 1 + z % 2
    g_c = 3 - 3 * (z // 2)
    g_b = 6 - z - g_a - g_c
    sends = Sends(send_sem)

    loads = [pltpu.make_async_copy(hid_hbm, hid, load_sem.at[0]),
             pltpu.make_async_copy(wkv_hbm, wkv, load_sem.at[1]),
             pltpu.make_async_copy(wq_hbm, wq.at[0], load_sem.at[2]),
             pltpu.make_async_copy(bq_hbm, bq_own, load_sem.at[3]),
             pltpu.make_async_copy(seg_hbm, seg.at[cp], load_sem.at[4]),
             pltpu.make_async_copy(wo_hbm, wo.at[pl.ds(z * width, width), :], load_sem.at[5]),
             pltpu.make_async_copy(gain_hbm, gain_ref, load_sem.at[6]),
             pltpu.make_async_copy(lnb_hbm, lnb_ref, load_sem.at[7]),
             pltpu.make_async_copy(bkv_hbm, bkv_ref, load_sem.at[8]),
             pltpu.make_async_copy(bo_hbm, bo_ref, load_sem.at[9])]
    for load in loads:
        load.start()

    barrier = pltpu.get_barrier_semaphore()
    for step in (1, 2, 3):
        pl.semaphore_signal(barrier, inc=1, device_id={'cp': (cp + step) % 4}, device_id_type=MESH)
    pl.semaphore_signal(barrier, inc=1, device_id=to_x, device_id_type=MESH)

    @pl.when(z > 0)
    def _():
        pl.semaphore_signal(barrier, inc=1, device_id={'tp': z - 1}, device_id_type=MESH)

    @pl.when(z < 3)
    def _():
        pl.semaphore_signal(barrier, inc=1, device_id={'tp': z + 1}, device_id_type=MESH)

    with jax.named_scope('barr'):
        pl.semaphore_wait(barrier, 5 + (z + 1) // 2 - 2 * (z // 3))

    def q_piece(p, h):
        half = q_rows // 2
        return wq.at[1, pl.ds(pl.multiple_of(p * q_rows + h * half, half), half), :]

    def o_piece(g, p, h):
        half = o_rows // 2
        return wo.at[pl.ds(pl.multiple_of(g * width + p * o_rows + h * half, half), half), :]

    q_sem, o_sem = lambda p, h: wq_recv.at[p, h], lambda g, p, h: wo_recv.at[g, p, h]

    sends.go(lambda: bq_hbm, lambda: bq_pair, lambda: bq_recv, {'tp': pair})
    for h in (0, 1):
        half = q_rows // 2
        sends.go(lambda h=h, half=half: wq_hbm.at[pl.ds(pl.multiple_of(p_me * q_rows + h * half, half), half), :],
                 lambda h=h: q_piece(p_me, h), lambda h=h: q_sem(p_me, h), {'tp': pair})
    for h in (0, 1):
        half = o_rows // 2
        own_o = lambda h=h, half=half: wo_hbm.at[pl.ds(pl.multiple_of(p_me * o_rows + h * half, half), half), :]
        sends.go(own_o, lambda h=h: o_piece(z, p_me, h), lambda h=h: o_sem(z, p_me, h), below, lambda: z > 0)
        sends.go(own_o, lambda h=h: o_piece(z, p_me, h), lambda h=h: o_sem(z, p_me, h), above, lambda: z < 3)
    for step in (1, 2, 3):
        sends.go(lambda: seg_hbm, lambda: seg.at[cp], lambda: seg_recv.at[cp], {'cp': cp + step}, lambda step=step: cp + step < 4)

    def pass_on(name, g, source, h):
        p = {'z': p_me, 's': p_me, 'x': p_x, 'y': p_y, 'd': p_d}[source]
        src = (lambda: q_piece(p, h)) if g is None else (lambda: o_piece(g, p, h))
        sem = (lambda: q_sem(p, h)) if g is None else (lambda: o_sem(g, p, h))
        if source == 's':
            sends.go(src, src, sem, to_x, None, (name, h, 'x'))
            sends.go(src, src, sem, to_y, None, (name, h, 'y'))
            return
        arrived(src(), sem())
        if source == 'z' and g is not None:
            sends.go(src, src, sem, below, lambda: (g > z) & (z > 0), (name, h, 'below'))
            sends.go(src, src, sem, above, lambda: (g < z) & (z < 3), (name, h, 'above'))
        elif source == 'x':
            sends.go(src, src, sem, to_y, lambda: c == 1, (name, h, 'xy'))
        elif source == 'y':
            sends.go(src, src, sem, to_x, lambda: c == 0, (name, h, 'yx'))
        sends.go(src, src, sem, to_core, None, (name, h, 'core' + source))

    groups = {'q': None, 'a': g_a, 'b': g_b, 'c': g_c}

    @scoped
    def ev(name, sources, *halves):
        for h in halves or (0, 1):
            for source in sources:
                pass_on(name, groups[name], source, h)

    @scoped
    def whole(name):
        for px in (0, 1):
            for py in (0, 1):
                for h in (0, 1):
                    p = pos(px, py, 1 - c)
                    if name == 'q':
                        arrived(q_piece(p, h), q_sem(p, h))
                    else:
                        arrived(o_piece(groups[name], p, h), o_sem(groups[name], p, h))

    with jax.named_scope('load_wait'):
        for i in (0, 6, 7):
            loads[i].wait()
    gain = gain_ref[...].astype(F32)
    lnb = lnb_ref[...].astype(F32)
    ln_rows = min(64, tok)

    def ln_step(i, carry):
        rows = pl.ds(pl.multiple_of(i * ln_rows, ln_rows), ln_rows)
        x = hid[rows, :].astype(F32)
        cen = x - jnp.mean(x, axis=-1, keepdims=True)
        var = jnp.mean(cen * cen, axis=-1, keepdims=True)
        normed[rows, :] = (cen * lax.rsqrt(var + LN_EPS) * gain + lnb).astype(BF16)
        return carry

    with jax.named_scope('ln'):
        lax.fori_loop(0, tok // ln_rows, ln_step, 0)

    loads[1].wait()
    loads[8].wait()
    kv_new = (jnp.dot(normed[...], wkv[...], preferred_element_type=F32) + bkv_ref[...].astype(F32)).astype(BF16)
    kv[cp, 0] = kv_new[:, :HEAD_DIM]
    kv[cp, 1] = kv_new[:, HEAD_DIM:]
    k_ref[...] = kv_new[:, :HEAD_DIM]
    v_ref[...] = kv_new[:, HEAD_DIM:]

    @scoped
    def project_q(which, bias):
        qf = jnp.dot(normed[...], wq[which], preferred_element_type=F32) + bias[...].astype(F32)
        for r in range(4):
            for h in range(heads):
                q_s[which * 4 + r, h * tile:(h + 1) * tile, :] = qf[r * tile:(r + 1) * tile, h * HEAD_DIM:(h + 1) * HEAD_DIM].astype(BF16)

    loads[2].wait()
    loads[3].wait()
    sends.go(lambda: kv.at[cp], lambda: kv.at[cp], lambda: kv_recv.at[cp], to_core, lambda: c == 0)
    sends.go(lambda: kv.at[cp], lambda: kv.at[cp], lambda: kv_recv.at[cp], to_y, lambda: y == 0)
    project_q(0, bq_own)
    loads[4].wait()
    for r in range(4):
        row = jnp.broadcast_to(seg[cp, :, r * tile:(r + 1) * tile], (tile, tile))
        segcol[r] = row.T

    g_1, g_2 = 2 - z // 2, 3 - 3 * (z // 2)
    middle, edge = (z > 0) & (z < 3), (z == 0) | (z == 3)
    tile_rows = lambda r: pl.ds(pl.multiple_of(r * tile, tile), tile)
    every = pl.ds(0, tok)

    def scores(q, k_blk, mask):
        keys = k_blk.shape[0]
        s = lax.dot_general(q, k_blk, (((1,), (1,)), ((), ())), preferred_element_type=F32) * SCORE_SCALE
        return jnp.where(mask[None], s.reshape(heads, tile, keys), -jnp.inf).reshape(heads * tile, keys)

    @scoped
    def attend_own(t, carry):
        r = t % 4
        k_pos = lax.broadcasted_iota(jnp.int32, (tile, tok), 1)
        q_pos = lax.broadcasted_iota(jnp.int32, (tile, tok), 0) + r * tile
        s = scores(q_s[t], kv[cp, 0], (seg[cp] == segcol[r][:, :1]) & (k_pos <= q_pos))
        m_new = jnp.max(s, axis=-1, keepdims=True)
        p = jnp.exp2(s - m_new)
        m_s[r] = jnp.broadcast_to(m_new, m_s.shape[1:])
        l_s[r] = jnp.broadcast_to(jnp.sum(p, axis=-1, keepdims=True), l_s.shape[1:])
        acc_s[r] = jnp.dot(p.astype(BF16), kv[cp, 1], preferred_element_type=F32)
        return carry

    @scoped
    def attend_earlier(t, g):
        r = t % 4
        q = q_s[t]
        seg_q = segcol[r][:, :1]

        def block(j, inner):
            s = scores(q, kv[j, 0], seg[j] == seg_q)
            m_prev = m_s[r]
            m_new = jnp.maximum(m_prev, jnp.max(s, axis=-1, keepdims=True))
            p = jnp.exp2(s - m_new[:, :1])
            alpha = jnp.exp2(m_prev - m_new)
            m_s[r] = m_new
            l_s[r] = l_s[r] * alpha + jnp.sum(p, axis=-1, keepdims=True)
            acc_s[r] = acc_s[r] * alpha + jnp.dot(p.astype(BF16), kv[j, 1], preferred_element_type=F32)
            return inner

        lax.fori_loop(0, cp, block, 0)
        for h in range(heads):
            at = slice(h * tile, (h + 1) * tile)
            o_all[g, tile_rows(r), h * HEAD_DIM:(h + 1) * HEAD_DIM] = (acc_s[r, at, :] / l_s[r, at, :]).astype(BF16)

    def send_heads(t, g):
        o_tile = o_all.at[g, tile_rows(t % 4), :]
        copy = pltpu.make_async_remote_copy(src_ref=o_tile, dst_ref=o_tile, send_sem=o_send.at[t], recv_sem=o_recv.at[t],
                                            device_id={'tp': 3 - z}, device_id_type=MESH)
        pl.when(middle)(lambda: copy.start())

    @scoped
    def heads_event(u):
        o_tile = o_all.at[g_1 if u < 4 else g_2, tile_rows(u % 4), :]
        arrived(o_tile, o_recv.at[u])
        for to, cond in ((0, z == 1), (3, z == 2)):
            copy = pltpu.make_async_remote_copy(src_ref=o_tile, dst_ref=o_tile, send_sem=o_send.at[8 + u], recv_sem=o_recv.at[u],
                                                device_id={'tp': to}, device_id_type=MESH)
            pl.when(cond)(lambda copy=copy: copy.start())

    def heads_here(*tiles):
        on(middle, *((heads_event, u) for u in tiles))

    def on(cond, *todo):
        @pl.when(cond)
        def _():
            for what, *about in todo:
                what(*about)

    n_col = min(512, d_model)

    @scoped
    def project_o(g, rows):
        def cols(n, carry):
            at = pl.ds(pl.multiple_of(n * n_col, n_col), n_col)
            part[g, rows, at] = jnp.dot(o_all[g, rows, :], wo[pl.ds(pl.multiple_of(g * width, width), width), at],
                                        preferred_element_type=F32).astype(BF16)
            return carry

        lax.fori_loop(0, d_model // n_col, cols, 0)

    def own_block(t, carry):
        attend_own(t, carry)
        on(t == 0, (ev, 'q', 'zs', 0))
        return carry

    lax.fori_loop(0, 4, own_block, 0)
    ev('q', 'zs', 1)
    on(middle, (ev, 'a', 'z'))

    with jax.named_scope('kvf'):
        pl.when(y == 1)(lambda: arrived(kv.at[c], kv_recv.at[c]))
        sends.go(lambda: kv.at[c], lambda: kv.at[c], lambda: kv_recv.at[c], to_core, lambda: y == 1)
    on(middle, (ev, 'a', 's'), (ev, 'b', 'z', 0))
    on(edge, (ev, 'a', 'zs', 0))
    ev('q', 'xy', 0)
    with jax.named_scope('kvw'):
        for j in range(3):
            pl.when(j < cp)(functools.partial(arrived, seg.at[j], seg_recv.at[j]))
        pl.when(y == 1)(lambda: arrived(kv.at[1 - c], kv_recv.at[1 - c]))
        pl.when(c == 1)(lambda: arrived(kv.at[cp - 1], kv_recv.at[cp - 1]))

    def own_heads(t, carry):
        attend_earlier(t, z)
        send_heads(t, z)

        @pl.when(t == 0)
        def _():
            on(middle, (ev, 'b', 'z', 1))
            on(edge, (ev, 'a', 'zs', 1))
            ev('q', 'xy', 1)
            on(middle, (ev, 'b', 's'))

        on((t == 1) & middle, (ev, 'c', 'z', 0))

        @pl.when(t == 2)
        def _():
            ev('q', 'd')
            on(edge, (ev, 'b', 'zs'))

        @pl.when(t == 3)
        def _():
            on(middle, (ev, 'c', 'z', 1), (heads_event, 0))
            ev('a', 'xy')
            on(middle, (ev, 'c', 's'))
        return carry

    lax.fori_loop(0, 4, own_heads, 0)
    whole('q')
    arrived(bq_pair, bq_recv)
    project_q(1, bq_pair)
    heads_here(1)
    lax.fori_loop(4, 8, attend_own, 0)
    on(edge, (ev, 'c', 'zs'))
    heads_here(2)
    ev('b', 'xy')

    def pair_heads(t, carry):
        attend_earlier(t, pair)
        send_heads(t, pair)
        on(t == 4, (heads_here, 3))
        on(t == 5, (ev, 'a', 'd'))
        on(t == 6, (heads_here, 4), (ev, 'c', 'xy'))
        on(t == 7, (heads_here, 5))
        return carry

    lax.fori_loop(4, 8, pair_heads, 0)
    heads_here(6)
    loads[5].wait()
    loads[9].wait()
    project_o(z, every)
    heads_here(7)
    ev('b', 'd')
    ev('c', 'd')
    whole('a')
    whole('b')
    project_o(pair, every)
    on(edge, *((heads_event, u) for u in range(4)))
    project_o(g_1, every)
    whole('c')

    @scoped
    def last(r, carry):
        pl.when(edge)(lambda: arrived(o_all.at[g_2, tile_rows(r), :], o_recv.at[4 + r]))
        project_o(g_2, tile_rows(r))

        def finish(i, inner):
            f_rows = tile // 4
            at = pl.ds(pl.multiple_of(r * tile + i * f_rows, f_rows), f_rows)
            total = part[0, at, :].astype(F32)
            for gg in (1, 2, 3):
                total = total + part[gg, at, :].astype(F32)
            y_ref[at, :] = (hid[at, :].astype(F32) + total + bo_ref[...].astype(F32)).astype(BF16)
            return inner

        lax.fori_loop(0, 4, finish, 0)
        return carry

    lax.fori_loop(0, 4, last, 0)

    with jax.named_scope('drain'):
        sends.finish()

    @pl.when((z > 0) & (z < 3))
    def _():
        def sent(u, carry):
            for which, gg in ((u, jnp.where(u < 4, z, pair)), (u + 8, jnp.where(u < 4, g_1, g_2))):
                o_tile = o_all.at[gg, tile_rows(u % 4), :]
                pltpu.make_async_copy(o_tile, o_tile, o_send.at[which]).wait()
            return carry

        lax.fori_loop(0, 8, sent, 0)


def solution(mesh):
    def local_block(hidden, seg_ids, w_q, b_q, w_kv, b_kv, w_o, b_o, ln_gain, ln_bias):
        tok, d_model = hidden.shape
        width = w_q.shape[1]
        heads = width // HEAD_DIM
        tile = tok // 4
        hbm = pl.BlockSpec(memory_space=pltpu.HBM)
        vmem = pl.BlockSpec(memory_space=pltpu.VMEM)
        dma = pltpu.SemaphoreType.DMA
        far = lambda a: pltpu.with_memory_space_constraint(a, pltpu.HBM)
        return pl.pallas_call(
            kernel,
            out_shape=(jax.ShapeDtypeStruct((tok, d_model), BF16), jax.ShapeDtypeStruct((tok, HEAD_DIM), BF16),
                       jax.ShapeDtypeStruct((tok, HEAD_DIM), BF16)),
            in_specs=[hbm] * 10,
            out_specs=(vmem, vmem, vmem),
            scratch_shapes=[
                pltpu.VMEM((tok, d_model), BF16),
                pltpu.VMEM((tok, d_model), BF16),
                pltpu.VMEM((d_model, 2 * HEAD_DIM), BF16),
                pltpu.VMEM((2, d_model, width), BF16),
                pltpu.VMEM((4 * width, d_model), BF16),
                pltpu.VMEM((width,), BF16),
                pltpu.VMEM((width,), BF16),
                pltpu.VMEM((2 * HEAD_DIM,), BF16),
                pltpu.VMEM((d_model,), BF16),
                pltpu.VMEM((d_model,), BF16),
                pltpu.VMEM((d_model,), BF16),
                pltpu.VMEM((4, 1, tok), jnp.int32),
                pltpu.VMEM((4, tile, tile), jnp.int32),
                pltpu.VMEM((4, 2, tok, HEAD_DIM), BF16),
                pltpu.VMEM((8, heads * tile, HEAD_DIM), BF16),
                pltpu.VMEM((4, tok, width), BF16),
                pltpu.VMEM((4, tok, d_model), BF16),
                pltpu.VMEM((4, heads * tile, HEAD_DIM), F32),
                pltpu.VMEM((4, heads * tile, HEAD_DIM), F32),
                pltpu.VMEM((4, heads * tile, HEAD_DIM), F32),
                dma((10,)), dma((N_SENDS,)), dma((16,)), dma(()), dma((4,)), dma((4,)), dma((8, 2)), dma((4, 8, 2)), dma((8,)),
            ],
            compiler_params=pltpu.CompilerParams(collective_id=0, has_side_effects=True, vmem_limit_bytes=48 * 2 ** 20),
            name='block',
        )(far(hidden), far(seg_ids.reshape(1, -1)), far(w_q), far(b_q), far(w_kv), far(b_kv), far(w_o), far(b_o), far(ln_gain), far(ln_bias))

    row_spec = P(('dp', 'cp'), None)
    tok_spec = P(('dp', 'cp'))
    return jax.shard_map(local_block, mesh=mesh,
                         in_specs=(row_spec, tok_spec, P(None, 'tp'), P('tp'), P(None, None), P(None), P('tp', None), P(None), P(None), P(None)),
                         out_specs=(row_spec, row_spec, row_spec), check_vma=False)
```

```python
import functools
import jax
import jax.numpy as jnp
from jax import lax
from jax.experimental import pallas as pl
from jax.experimental.pallas import tpu as pltpu
from jax.sharding import PartitionSpec as P

HEAD_DIM = 128
LN_EPS = 1e-5
SCORE_SCALE = HEAD_DIM ** -0.5 * 1.4426950408889634
MESH = pl.DeviceIdType.MESH
BF16 = jnp.bfloat16
F32 = jnp.float32


class Sends:
    def __init__(self, sems):
        self.sems, self.made, self.keys = sems, [], {}

    def go(self, src, dst, recv, to, cond=None, key=None):
        slot = self.keys.get(key, len(self.made)) if key else len(self.made)
        make = lambda: pltpu.make_async_remote_copy(src_ref=src(), dst_ref=dst(), send_sem=self.sems.at[slot], recv_sem=recv(),
                                                    device_id=to, device_id_type=MESH)
        if slot == len(self.made):
            self.made.append((make, cond))
            if key:
                self.keys[key] = slot
        if cond is None:
            make().start()
        else:
            pl.when(cond())(lambda: make().start())

    def finish(self):
        for make, cond in self.made:
            if cond is None:
                make().wait_send()
            else:
                pl.when(cond())(lambda: make().wait_send())


def scoped(fn):
    def run(*about):
        with jax.named_scope(fn.__name__ + '_'.join(str(a) for a in about if isinstance(a, (str, int)))):
            return fn(*about)
    return run


def arrived(dst, recv):
    pltpu.make_async_copy(dst, dst, recv).wait()


N_SENDS = 100


def kernel(hid_hbm, seg_hbm, wq_hbm, bq_hbm, wkv_hbm, bkv_hbm, wo_hbm, bo_hbm, gain_hbm, lnb_hbm,
           y_ref, k_ref, v_ref,
           hid, normed, wkv, wq, wo, bq_own, bq_pair, bkv_ref, bo_ref, gain_ref, lnb_ref, seg, segcol, kv, q_s, o_all, part, run_s, m_s, l_s, acc_s,
           load_sem, send_sem, o_send, bq_recv, seg_recv, kv_recv, wq_recv, wo_recv, o_recv):
    tok, d_model = hid.shape
    width = wq.shape[2]
    heads = width // HEAD_DIM
    tile = tok // 4
    q_rows, o_rows = d_model // 8, width // 8
    dp, z, cp = lax.axis_index('dp'), lax.axis_index('tp'), lax.axis_index('cp')
    y, c = cp // 2, cp % 2
    pair = z + 1 - 2 * (z % 2)
    below, above = {'tp': z - 1}, {'tp': z + 1}
    to_x, to_y, to_core = {'dp': 1 - dp}, {'cp': cp + 2 - 4 * y}, {'cp': cp + 1 - 2 * c}
    pos = lambda px, py, pc: px * 4 + py * 2 + pc
    p_me, p_x, p_y, p_d = pos(dp, y, c), pos(1 - dp, y, c), pos(dp, 1 - y, c), pos(1 - dp, 1 - y, c)
    g_a = 1 + z % 2
    g_c = 3 - 3 * (z // 2)
    g_b = 6 - z - g_a - g_c
    sends = Sends(send_sem)

    loads = [pltpu.make_async_copy(hid_hbm, hid, load_sem.at[0]),
             pltpu.make_async_copy(wkv_hbm, wkv, load_sem.at[1]),
             pltpu.make_async_copy(wq_hbm, wq.at[0], load_sem.at[2]),
             pltpu.make_async_copy(bq_hbm, bq_own, load_sem.at[3]),
             pltpu.make_async_copy(seg_hbm, seg.at[cp], load_sem.at[4]),
             pltpu.make_async_copy(wo_hbm, wo.at[pl.ds(z * width, width), :], load_sem.at[5]),
             pltpu.make_async_copy(gain_hbm, gain_ref, load_sem.at[6]),
             pltpu.make_async_copy(lnb_hbm, lnb_ref, load_sem.at[7]),
             pltpu.make_async_copy(bkv_hbm, bkv_ref, load_sem.at[8]),
             pltpu.make_async_copy(bo_hbm, bo_ref, load_sem.at[9])]
    for i in (0, 6, 7, 8, 3, 4, 9):
        loads[i].start()

    barrier = pltpu.get_barrier_semaphore()
    for step in (1, 2, 3):
        pl.semaphore_signal(barrier, inc=1, device_id={'cp': (cp + step) % 4}, device_id_type=MESH)
    pl.semaphore_signal(barrier, inc=1, device_id=to_x, device_id_type=MESH)

    @pl.when(z > 0)
    def _():
        pl.semaphore_signal(barrier, inc=1, device_id={'tp': z - 1}, device_id_type=MESH)

    @pl.when(z < 3)
    def _():
        pl.semaphore_signal(barrier, inc=1, device_id={'tp': z + 1}, device_id_type=MESH)

    loads[1].start()
    with jax.named_scope('barr'):
        pl.semaphore_wait(barrier, 5 + (z + 1) // 2 - 2 * (z // 3))

    loads[2].start()
    def q_piece(p, h):
        half = q_rows // 2
        return wq.at[1, pl.ds(pl.multiple_of(p * q_rows + h * half, half), half), :]

    def o_piece(g, p, h):
        half = o_rows // 2
        return wo.at[pl.ds(pl.multiple_of(g * width + p * o_rows + h * half, half), half), :]

    q_sem, o_sem = lambda p, h: wq_recv.at[p, h], lambda g, p, h: wo_recv.at[g, p, h]

    sends.go(lambda: bq_hbm, lambda: bq_pair, lambda: bq_recv, {'tp': pair})
    for h in (0, 1):
        half = q_rows // 2
        sends.go(lambda h=h, half=half: wq_hbm.at[pl.ds(pl.multiple_of(p_me * q_rows + h * half, half), half), :],
                 lambda h=h: q_piece(p_me, h), lambda h=h: q_sem(p_me, h), {'tp': pair})
    for h in (0, 1):
        half = o_rows // 2
        own_o = lambda h=h, half=half: wo_hbm.at[pl.ds(pl.multiple_of(p_me * o_rows + h * half, half), half), :]
        sends.go(own_o, lambda h=h: o_piece(z, p_me, h), lambda h=h: o_sem(z, p_me, h), below, lambda: z > 0)
        sends.go(own_o, lambda h=h: o_piece(z, p_me, h), lambda h=h: o_sem(z, p_me, h), above, lambda: z < 3)
    for step in (1, 2, 3):
        sends.go(lambda: seg_hbm, lambda: seg.at[cp], lambda: seg_recv.at[cp], {'cp': cp + step}, lambda step=step: cp + step < 4)

    def pass_on(name, g, source, h):
        p = {'z': p_me, 's': p_me, 'x': p_x, 'y': p_y, 'd': p_d}[source]
        src = (lambda: q_piece(p, h)) if g is None else (lambda: o_piece(g, p, h))
        sem = (lambda: q_sem(p, h)) if g is None else (lambda: o_sem(g, p, h))
        if source == 's':
            sends.go(src, src, sem, to_x, None, (name, h, 'x'))
            sends.go(src, src, sem, to_y, None, (name, h, 'y'))
            return
        arrived(src(), sem())
        if source == 'z' and g is not None:
            sends.go(src, src, sem, below, lambda: (g > z) & (z > 0), (name, h, 'below'))
            sends.go(src, src, sem, above, lambda: (g < z) & (z < 3), (name, h, 'above'))
        elif source == 'x':
            sends.go(src, src, sem, to_y, lambda: c == 1, (name, h, 'xy'))
        elif source == 'y':
            sends.go(src, src, sem, to_x, lambda: c == 0, (name, h, 'yx'))
        sends.go(src, src, sem, to_core, None, (name, h, 'core' + source))

    groups = {'q': None, 'a': g_a, 'b': g_b, 'c': g_c}

    @scoped
    def ev(name, sources, *halves):
        for h in halves or (0, 1):
            for source in sources:
                pass_on(name, groups[name], source, h)

    @scoped
    def whole(name):
        for px in (0, 1):
            for py in (0, 1):
                for h in (0, 1):
                    p = pos(px, py, 1 - c)
                    if name == 'q':
                        arrived(q_piece(p, h), q_sem(p, h))
                    else:
                        arrived(o_piece(groups[name], p, h), o_sem(groups[name], p, h))

    loads[5].start()

    with jax.named_scope('load_wait'):
        for i in (0, 6, 7):
            loads[i].wait()
    gain = gain_ref[...].astype(F32)
    lnb = lnb_ref[...].astype(F32)
    ln_rows = min(64, tok)

    def ln_step(i, carry):
        rows = pl.ds(pl.multiple_of(i * ln_rows, ln_rows), ln_rows)
        x = hid[rows, :].astype(F32)
        cen = x - jnp.mean(x, axis=-1, keepdims=True)
        var = jnp.mean(cen * cen, axis=-1, keepdims=True)
        normed[rows, :] = (cen * lax.rsqrt(var + LN_EPS) * gain + lnb).astype(BF16)
        return carry

    with jax.named_scope('ln'):
        lax.fori_loop(0, tok // ln_rows, ln_step, 0)

    loads[1].wait()
    loads[8].wait()
    kv_new = (jnp.dot(normed[...], wkv[...], preferred_element_type=F32) + bkv_ref[...].astype(F32)).astype(BF16)
    kv[cp, 0] = kv_new[:, :HEAD_DIM]
    kv[cp, 1] = kv_new[:, HEAD_DIM:]
    k_ref[...] = kv_new[:, :HEAD_DIM]
    v_ref[...] = kv_new[:, HEAD_DIM:]

    @scoped
    def project_q(which, bias):
        qf = jnp.dot(normed[...], wq[which], preferred_element_type=F32) + bias[...].astype(F32)
        for r in range(4):
            for h in range(heads):
                q_s[which * 4 + r, h * tile:(h + 1) * tile, :] = qf[r * tile:(r + 1) * tile, h * HEAD_DIM:(h + 1) * HEAD_DIM].astype(BF16)

    loads[2].wait()
    loads[3].wait()
    for i in (0, 1):
        sends.go(lambda i=i: kv.at[cp, i], lambda i=i: kv.at[cp, i], lambda i=i: kv_recv.at[cp, i], to_y, lambda: y == 0)
    for i in (0, 1):
        sends.go(lambda i=i: kv.at[cp, i], lambda i=i: kv.at[cp, i], lambda i=i: kv_recv.at[cp, i], to_core, lambda: c == 0)
    project_q(0, bq_own)
    loads[4].wait()
    for r in range(4):
        row = jnp.broadcast_to(seg[cp, :, r * tile:(r + 1) * tile], (tile, tile))
        segcol[r] = row.T

    g_1, g_2 = 2 - z // 2, 3 - 3 * (z // 2)
    middle, edge = (z > 0) & (z < 3), (z == 0) | (z == 3)
    tile_rows = lambda r: pl.ds(pl.multiple_of(r * tile, tile), tile)
    every = pl.ds(0, tok)

    def scores(q, k_blk, mask):
        keys = k_blk.shape[0]
        s = lax.dot_general(q, k_blk, (((1,), (1,)), ((), ())), preferred_element_type=F32) * SCORE_SCALE
        return jnp.where(mask[None], s.reshape(heads, tile, keys), -jnp.inf).reshape(heads * tile, keys)

    @scoped
    def attend_own(t, carry):
        r = t % 4
        k_pos = lax.broadcasted_iota(jnp.int32, (tile, tok), 1)
        q_pos = lax.broadcasted_iota(jnp.int32, (tile, tok), 0) + r * tile
        s = scores(q_s[t], kv[cp, 0], (seg[cp] == segcol[r][:, :1]) & (k_pos <= q_pos))
        m_new = jnp.max(s, axis=-1, keepdims=True)
        p = jnp.exp2(s - m_new)
        m_s[r] = jnp.broadcast_to(m_new, m_s.shape[1:])
        l_s[r] = jnp.broadcast_to(jnp.sum(p, axis=-1, keepdims=True), l_s.shape[1:])
        acc_s[r] = jnp.dot(p.astype(BF16), kv[cp, 1], preferred_element_type=F32)
        return carry

    @scoped
    def attend_earlier(t, g):
        r = t % 4
        q = q_s[t]
        seg_q = segcol[r][:, :1]

        def block(j, inner):
            s = scores(q, kv[j, 0], seg[j] == seg_q)
            m_prev = m_s[r]
            m_new = jnp.maximum(m_prev, jnp.max(s, axis=-1, keepdims=True))
            p = jnp.exp2(s - m_new[:, :1])
            alpha = jnp.exp2(m_prev - m_new)
            m_s[r] = m_new
            l_s[r] = l_s[r] * alpha + jnp.sum(p, axis=-1, keepdims=True)
            acc_s[r] = acc_s[r] * alpha + jnp.dot(p.astype(BF16), kv[j, 1], preferred_element_type=F32)
            return inner

        lax.fori_loop(0, cp, block, 0)
        for h in range(heads):
            at = slice(h * tile, (h + 1) * tile)
            o_all[g, tile_rows(r), h * HEAD_DIM:(h + 1) * HEAD_DIM] = (acc_s[r, at, :] / l_s[r, at, :]).astype(BF16)

    def send_heads(t, g):
        o_tile = o_all.at[g, tile_rows(t % 4), :]
        copy = pltpu.make_async_remote_copy(src_ref=o_tile, dst_ref=o_tile, send_sem=o_send.at[t], recv_sem=o_recv.at[t],
                                            device_id={'tp': 3 - z}, device_id_type=MESH)
        pl.when(middle)(lambda: copy.start())

    @scoped
    def heads_event(u):
        o_tile = o_all.at[g_1 if u < 4 else g_2, tile_rows(u % 4), :]
        arrived(o_tile, o_recv.at[u])
        for to, cond in ((0, z == 1), (3, z == 2)):
            copy = pltpu.make_async_remote_copy(src_ref=o_tile, dst_ref=o_tile, send_sem=o_send.at[8 + u], recv_sem=o_recv.at[u],
                                                device_id={'tp': to}, device_id_type=MESH)
            pl.when(cond)(lambda copy=copy: copy.start())

    def heads_here(*tiles):
        on(middle, *((heads_event, u) for u in tiles))

    def on(cond, *todo):
        @pl.when(cond)
        def _():
            for what, *about in todo:
                what(*about)

    n_col = min(512, d_model)

    def project(g, rows, use):
        def cols(n, carry):
            at = pl.ds(pl.multiple_of(n * n_col, n_col), n_col)
            use(rows, at, jnp.dot(o_all[g, rows, :], wo[pl.ds(pl.multiple_of(g * width, width), width), at],
                                  preferred_element_type=F32).astype(BF16))
            return carry

        lax.fori_loop(0, d_model // n_col, cols, 0)

    @scoped
    def project_o(g):
        def keep(rows, at, fresh):
            part[g % 2, rows, at] = fresh

        project(g, every, keep)

    @scoped
    def project_third(g):
        def add(rows, at, fresh):
            pair_sum = part[(3 - g) % 2, rows, at].astype(F32) + fresh.astype(F32)
            run_s[rows, at] = hid[rows, at].astype(F32) + bo_ref[at].astype(F32) + pair_sum

        project(g, every, add)

    @scoped
    def project_last(g, rows):
        def add(rows, at, fresh):
            y_ref[rows, at] = (run_s[rows, at] + (part[(3 - g) % 2, rows, at].astype(F32) + fresh.astype(F32))).astype(BF16)

        project(g, rows, add)

    @scoped
    def kv_pass(i):
        pl.when(y == 1)(lambda: arrived(kv.at[c, i], kv_recv.at[c, i]))
        sends.go(lambda: kv.at[c, i], lambda: kv.at[c, i], lambda: kv_recv.at[c, i], to_core, lambda: y == 1)

    def own_block(t, carry):
        attend_own(t, carry)
        on(t == 0, (ev, 'q', 'zs', 0))
        on(t == 3, (kv_pass, 0))
        return carry

    lax.fori_loop(0, 4, own_block, 0)
    ev('q', 'zs', 1)
    on(middle, (ev, 'a', 'z'))

    kv_pass(1)
    on(middle, (ev, 'b', 'z', 0))
    ev('q', 'xy', 0)
    on(middle, (ev, 'a', 's', 0))
    on(edge, (ev, 'a', 'zs', 0))
    with jax.named_scope('kvw'):
        for j in range(3):
            pl.when(j < cp)(functools.partial(arrived, seg.at[j], seg_recv.at[j]))
        for i in (0, 1):
            pl.when(y == 1)(lambda i=i: arrived(kv.at[1 - c, i], kv_recv.at[1 - c, i]))
            pl.when(c == 1)(lambda i=i: arrived(kv.at[cp - 1, i], kv_recv.at[cp - 1, i]))

    def own_heads(t, carry):
        attend_earlier(t, z)
        send_heads(t, z)

        @pl.when(t == 0)
        def _():
            on(middle, (ev, 'b', 'z', 1))
            ev('q', 'xy', 1)
            on(middle, (ev, 'a', 's', 1), (ev, 'b', 's'))
            on(edge, (ev, 'a', 'zs', 1))

        on((t == 1) & middle, (ev, 'c', 'z', 0))

        @pl.when(t == 2)
        def _():
            on(edge, (ev, 'b', 'zs'))

        @pl.when(t == 3)
        def _():
            on(middle, (ev, 'c', 'z', 1), (heads_event, 0))
            ev('a', 'xy')
            on(middle, (ev, 'c', 's'))
        return carry

    lax.fori_loop(0, 4, own_heads, 0)
    loads[5].wait()
    project_o(z)
    ev('q', 'd')
    whole('q')
    arrived(bq_pair, bq_recv)
    project_q(1, bq_pair)
    heads_here(1)
    lax.fori_loop(4, 8, attend_own, 0)
    on(edge, (ev, 'c', 'zs'))
    heads_here(2)
    ev('b', 'xy')

    def pair_heads(t, carry):
        attend_earlier(t, pair)
        send_heads(t, pair)
        on(t == 4, (heads_here, 3))
        on(t == 5, (ev, 'a', 'd'))
        on(t == 6, (heads_here, 4), (ev, 'c', 'xy'))
        on(t == 7, (heads_here, 5))
        return carry

    lax.fori_loop(4, 8, pair_heads, 0)
    heads_here(6)
    ev('b', 'd')
    whole('a')
    whole('b')
    project_o(pair)
    heads_here(7)
    on(edge, *((heads_event, u) for u in range(4)))
    loads[9].wait()
    project_third(g_1)
    ev('c', 'd')
    whole('c')

    def last(r, carry):
        pl.when(edge)(lambda: arrived(o_all.at[g_2, tile_rows(r), :], o_recv.at[4 + r]))
        project_last(g_2, tile_rows(r))
        return carry

    lax.fori_loop(0, 4, last, 0)

    with jax.named_scope('drain'):
        sends.finish()

    @pl.when((z > 0) & (z < 3))
    def _():
        def sent(u, carry):
            for which, gg in ((u, jnp.where(u < 4, z, pair)), (u + 8, jnp.where(u < 4, g_1, g_2))):
                o_tile = o_all.at[gg, tile_rows(u % 4), :]
                pltpu.make_async_copy(o_tile, o_tile, o_send.at[which]).wait()
            return carry

        lax.fori_loop(0, 8, sent, 0)


def write_out(y_in, k_in, v_in, y_out, k_out, v_out, sems):
    copies = [pltpu.make_async_copy(a, b, sems.at[i]) for i, (a, b) in enumerate(((y_in, y_out), (k_in, k_out), (v_in, v_out)))]
    for copy in copies:
        copy.start()
    for copy in copies:
        copy.wait()


def solution(mesh):
    def local_block(hidden, seg_ids, w_q, b_q, w_kv, b_kv, w_o, b_o, ln_gain, ln_bias):
        tok, d_model = hidden.shape
        width = w_q.shape[1]
        heads = width // HEAD_DIM
        tile = tok // 4
        hbm = pl.BlockSpec(memory_space=pltpu.HBM)
        vmem = pl.BlockSpec(memory_space=pltpu.VMEM)
        dma = pltpu.SemaphoreType.DMA
        far = lambda a: pltpu.with_memory_space_constraint(a, pltpu.HBM)
        outs = pl.pallas_call(
            kernel,
            out_shape=(jax.ShapeDtypeStruct((tok, d_model), BF16), jax.ShapeDtypeStruct((tok, HEAD_DIM), BF16),
                       jax.ShapeDtypeStruct((tok, HEAD_DIM), BF16)),
            in_specs=[hbm] * 10,
            out_specs=(vmem, vmem, vmem),
            scratch_shapes=[
                pltpu.VMEM((tok, d_model), BF16),
                pltpu.VMEM((tok, d_model), BF16),
                pltpu.VMEM((d_model, 2 * HEAD_DIM), BF16),
                pltpu.VMEM((2, d_model, width), BF16),
                pltpu.VMEM((4 * width, d_model), BF16),
                pltpu.VMEM((width,), BF16),
                pltpu.VMEM((width,), BF16),
                pltpu.VMEM((2 * HEAD_DIM,), BF16),
                pltpu.VMEM((d_model,), BF16),
                pltpu.VMEM((d_model,), BF16),
                pltpu.VMEM((d_model,), BF16),
                pltpu.VMEM((4, 1, tok), jnp.int32),
                pltpu.VMEM((4, tile, tile), jnp.int32),
                pltpu.VMEM((4, 2, tok, HEAD_DIM), BF16),
                pltpu.VMEM((8, heads * tile, HEAD_DIM), BF16),
                pltpu.VMEM((4, tok, width), BF16),
                pltpu.VMEM((2, tok, d_model), BF16),
                pltpu.VMEM((tok, d_model), F32),
                pltpu.VMEM((4, heads * tile, HEAD_DIM), F32),
                pltpu.VMEM((4, heads * tile, HEAD_DIM), F32),
                pltpu.VMEM((4, heads * tile, HEAD_DIM), F32),
                dma((10,)), dma((N_SENDS,)), dma((16,)), dma(()), dma((4,)), dma((4, 2)), dma((8, 2)), dma((4, 8, 2)), dma((8,)),
            ],
            compiler_params=pltpu.CompilerParams(collective_id=0, has_side_effects=True, vmem_limit_bytes=48 * 2 ** 20),
            name='block',
        )(far(hidden), far(seg_ids.reshape(1, -1)), far(w_q), far(b_q), far(w_kv), far(b_kv), far(w_o), far(b_o), far(ln_gain), far(ln_bias))
        near = lambda a: pltpu.with_memory_space_constraint(a, pltpu.VMEM)
        return pl.pallas_call(
            write_out,
            out_shape=tuple(jax.ShapeDtypeStruct(a.shape, a.dtype) for a in outs),
            in_specs=[vmem] * 3,
            out_specs=(pl.BlockSpec(memory_space=pl.ANY),) * 3,
            scratch_shapes=[dma((3,))],
            name='write',
        )(*map(near, outs))

    row_spec = P(('dp', 'cp'), None)
    tok_spec = P(('dp', 'cp'))
    return jax.shard_map(local_block, mesh=mesh,
                         in_specs=(row_spec, tok_spec, P(None, 'tp'), P('tp'), P(None, None), P(None), P('tp', None), P(None), P(None), P(None)),
                         out_specs=(row_spec, row_spec, row_spec), check_vma=False)
```

```python
import functools
import jax
import jax.numpy as jnp
from jax import lax
from jax.experimental import pallas as pl
from jax.experimental.pallas import tpu as pltpu
from jax.sharding import PartitionSpec as P

HEAD_DIM = 128
LN_EPS = 1e-5
SCORE_SCALE = HEAD_DIM ** -0.5 * 1.4426950408889634
MESH = pl.DeviceIdType.MESH
BF16 = jnp.bfloat16
F32 = jnp.float32


def send(src, dst, sent, recv, to):
    pltpu.make_async_remote_copy(src_ref=src, dst_ref=dst, send_sem=sent, recv_sem=recv, device_id=to, device_id_type=MESH).start()


def scoped(fn):
    def run(*about):
        with jax.named_scope(fn.__name__ + '_'.join(str(a) for a in about if isinstance(a, (str, int)))):
            return fn(*about)
    return run


def arrived(dst, recv):
    pltpu.make_async_copy(dst, dst, recv).wait()


def kernel(hid_hbm, seg_hbm, wq_hbm, bq_hbm, wkv_hbm, bkv_hbm, wo_hbm, bo_hbm, gain_hbm, lnb_hbm,
           y_ref, k_ref, v_ref,
           hid, normed, wkv, wq, wo, bq_own, bq_pair, bkv_ref, bo_ref, gain_ref, lnb_ref, seg, segcol, kv, q_s, o_all, part, run_s, m_s, l_s, acc_s,
           load_sem, spread_sem, line_sem, kv_sem, small_sem, bq_recv, seg_recv, kv_recv, wq_recv, wo_recv, o_recv):
    tok, d_model = hid.shape
    width = wq.shape[2]
    heads = width // HEAD_DIM
    tile = tok // 4
    q_rows, o_rows = d_model // 8, width // 8
    dp, z, cp = lax.axis_index('dp'), lax.axis_index('tp'), lax.axis_index('cp')
    y, c = cp // 2, cp % 2
    pair = z + 1 - 2 * (z % 2)
    below, above = {'tp': z - 1}, {'tp': z + 1}
    to_x, to_y, to_core = {'dp': 1 - dp}, {'cp': cp + 2 - 4 * y}, {'cp': cp + 1 - 2 * c}
    pos = lambda px, py, pc: px * 4 + py * 2 + pc
    p_me, p_x, p_y, p_d = pos(dp, y, c), pos(1 - dp, y, c), pos(dp, 1 - y, c), pos(1 - dp, 1 - y, c)
    g_a = 1 + z % 2
    g_c = 3 - 3 * (z // 2)
    g_b = 6 - z - g_a - g_c

    loads = [pltpu.make_async_copy(hid_hbm, hid, load_sem.at[0]),
             pltpu.make_async_copy(wkv_hbm, wkv, load_sem.at[1]),
             pltpu.make_async_copy(wq_hbm, wq.at[0], load_sem.at[2]),
             pltpu.make_async_copy(bq_hbm, bq_own, load_sem.at[3]),
             pltpu.make_async_copy(seg_hbm, seg.at[cp], load_sem.at[4]),
             pltpu.make_async_copy(wo_hbm, wo.at[pl.ds(z * width, width), :], load_sem.at[5]),
             pltpu.make_async_copy(gain_hbm, gain_ref, load_sem.at[6]),
             pltpu.make_async_copy(lnb_hbm, lnb_ref, load_sem.at[7]),
             pltpu.make_async_copy(bkv_hbm, bkv_ref, load_sem.at[8]),
             pltpu.make_async_copy(bo_hbm, bo_ref, load_sem.at[9])]
    for i in (0, 6, 7, 8, 3, 4, 9):
        loads[i].start()

    barrier = pltpu.get_barrier_semaphore()
    for step in (1, 2, 3):
        pl.semaphore_signal(barrier, inc=1, device_id={'cp': (cp + step) % 4}, device_id_type=MESH)
    pl.semaphore_signal(barrier, inc=1, device_id=to_x, device_id_type=MESH)

    @pl.when(z > 0)
    def _():
        pl.semaphore_signal(barrier, inc=1, device_id={'tp': z - 1}, device_id_type=MESH)

    @pl.when(z < 3)
    def _():
        pl.semaphore_signal(barrier, inc=1, device_id={'tp': z + 1}, device_id_type=MESH)

    loads[1].start()
    with jax.named_scope('barr'):
        pl.semaphore_wait(barrier, 5 + (z + 1) // 2 - 2 * (z // 3))

    loads[2].start()
    def q_piece(p, h):
        half = q_rows // 2
        return wq.at[1, pl.ds(pl.multiple_of(p * q_rows + h * half, half), half), :]

    def o_piece(g, p, h):
        half = o_rows // 2
        return wo.at[pl.ds(pl.multiple_of(g * width + p * o_rows + h * half, half), half), :]

    def sem(g, kind, h):
        at = {'z': 0, 'x': 2, 'y': 4, 'd': 6, 'core': 8}[kind] + (0 if kind == 'core' else h)
        return wq_recv.at[at] if g is None else wo_recv.at[g, at]

    middle, edge = (z > 0) & (z < 3), (z == 0) | (z == 3)

    send(bq_hbm, bq_pair, small_sem.at[0], bq_recv, {'tp': pair})
    for h in (0, 1):
        half = q_rows // 2
        send(wq_hbm.at[pl.ds(pl.multiple_of(p_me * q_rows + h * half, half), half), :], q_piece(p_me, h), spread_sem, sem(None, 'z', h),
             {'tp': pair})
    for h in (0, 1):
        half = o_rows // 2
        for to, cond in ((below, z > 0), (above, z < 3)):
            @pl.when(cond)
            def _():
                send(wo_hbm.at[pl.ds(pl.multiple_of(p_me * o_rows + h * half, half), half), :], o_piece(z, p_me, h), line_sem,
                     sem(z, 'z', h), to)
    for step in (1, 2, 3):
        pl.when(cp + step < 4)(lambda: send(seg_hbm, seg.at[cp], small_sem.at[step], seg_recv.at[cp], {'cp': cp + step}))

    def pass_on(g, source, h):
        p = {'z': p_me, 's': p_me, 'x': p_x, 'y': p_y, 'd': p_d}[source]
        piece = q_piece(p, h) if g is None else o_piece(g, p, h)
        if source == 's':
            send(piece, piece, spread_sem, sem(g, 'x', h), to_x)
            send(piece, piece, spread_sem, sem(g, 'y', h), to_y)
            return
        arrived(piece, sem(g, source, h))
        if source == 'z' and g is not None:
            pl.when((g > z) & (z > 0))(lambda: send(piece, piece, line_sem, sem(g, 'z', h), below))
            pl.when((g < z) & (z < 3))(lambda: send(piece, piece, line_sem, sem(g, 'z', h), above))
        elif source == 'x':
            pl.when(c == 1)(lambda: send(piece, piece, spread_sem, sem(g, 'd', h), to_y))
        elif source == 'y':
            pl.when(c == 0)(lambda: send(piece, piece, spread_sem, sem(g, 'd', h), to_x))
        send(piece, piece, spread_sem, sem(g, 'core', h), to_core)

    groups = {'q': None, 'a': g_a, 'b': g_b, 'c': g_c}

    @scoped
    def ev(name, sources, *halves):
        for h in halves or (0, 1):
            for source in sources:
                pass_on(groups[name], source, h)

    @scoped
    def whole(name):
        if name == 'q':
            arrived(wq.at[1, pl.ds(0, 4 * q_rows), :], sem(None, 'core', 0))
        else:
            arrived(wo.at[pl.ds(0, 4 * o_rows), :], sem(groups[name], 'core', 0))

    loads[5].start()

    with jax.named_scope('load_wait'):
        for i in (0, 6, 7):
            loads[i].wait()
    gain = gain_ref[...].astype(F32)
    lnb = lnb_ref[...].astype(F32)
    ln_rows = min(64, tok)

    def ln_step(i, carry):
        rows = pl.ds(pl.multiple_of(i * ln_rows, ln_rows), ln_rows)
        x = hid[rows, :].astype(F32)
        cen = x - jnp.mean(x, axis=-1, keepdims=True)
        var = jnp.mean(cen * cen, axis=-1, keepdims=True)
        normed[rows, :] = (cen * lax.rsqrt(var + LN_EPS) * gain + lnb).astype(BF16)
        return carry

    with jax.named_scope('ln'):
        lax.fori_loop(0, tok // ln_rows, ln_step, 0)

    loads[1].wait()
    loads[8].wait()
    kv_new = (jnp.dot(normed[...], wkv[...], preferred_element_type=F32) + bkv_ref[...].astype(F32)).astype(BF16)
    kv[cp, 0] = kv_new[:, :HEAD_DIM]
    kv[cp, 1] = kv_new[:, HEAD_DIM:]
    k_ref[...] = kv_new[:, :HEAD_DIM]
    v_ref[...] = kv_new[:, HEAD_DIM:]

    @scoped
    def project_q(which, bias):
        qf = jnp.dot(normed[...], wq[which], preferred_element_type=F32) + bias[...].astype(F32)
        for r in range(4):
            for h in range(heads):
                q_s[which * 4 + r, h * tile:(h + 1) * tile, :] = qf[r * tile:(r + 1) * tile, h * HEAD_DIM:(h + 1) * HEAD_DIM].astype(BF16)

    loads[2].wait()
    loads[3].wait()
    for i in (0, 1):
        pl.when(y == 0)(lambda: send(kv.at[cp, i], kv.at[cp, i], kv_sem, kv_recv.at[cp, i], to_y))
    for i in (0, 1):
        pl.when(c == 0)(lambda: send(kv.at[cp, i], kv.at[cp, i], kv_sem, kv_recv.at[cp, i], to_core))
    project_q(0, bq_own)
    loads[4].wait()
    for r in range(4):
        row = jnp.broadcast_to(seg[cp, :, r * tile:(r + 1) * tile], (tile, tile))
        segcol[r] = row.T

    g_1, g_2 = 2 - z // 2, 3 - 3 * (z // 2)
    tile_rows = lambda r: pl.ds(pl.multiple_of(r * tile, tile), tile)
    every = pl.ds(0, tok)

    def scores(q, k_blk, mask):
        keys = k_blk.shape[0]
        s = lax.dot_general(q, k_blk, (((1,), (1,)), ((), ())), preferred_element_type=F32) * SCORE_SCALE
        return jnp.where(mask[None], s.reshape(heads, tile, keys), -jnp.inf).reshape(heads * tile, keys)

    @scoped
    def attend_own(t, carry):
        r = t % 4
        k_pos = lax.broadcasted_iota(jnp.int32, (tile, tok), 1)
        q_pos = lax.broadcasted_iota(jnp.int32, (tile, tok), 0) + r * tile
        s = scores(q_s[t], kv[cp, 0], (seg[cp] == segcol[r][:, :1]) & (k_pos <= q_pos))
        m_new = jnp.max(s, axis=-1, keepdims=True)
        p = jnp.exp2(s - m_new)
        m_s[r] = jnp.broadcast_to(m_new, m_s.shape[1:])
        l_s[r] = jnp.broadcast_to(jnp.sum(p, axis=-1, keepdims=True), l_s.shape[1:])
        acc_s[r] = jnp.dot(p.astype(BF16), kv[cp, 1], preferred_element_type=F32)
        return carry

    def attend_block(t, j):
        r = t % 4
        s = scores(q_s[t], kv[j, 0], seg[j] == segcol[r][:, :1])
        m_prev = m_s[r]
        m_new = jnp.maximum(m_prev, jnp.max(s, axis=-1, keepdims=True))
        p = jnp.exp2(s - m_new[:, :1])
        alpha = jnp.exp2(m_prev - m_new)
        m_s[r] = m_new
        l_s[r] = l_s[r] * alpha + jnp.sum(p, axis=-1, keepdims=True)
        acc_s[r] = acc_s[r] * alpha + jnp.dot(p.astype(BF16), kv[j, 1], preferred_element_type=F32)

    def attend_end(t, g):
        r = t % 4
        for h in range(heads):
            at = slice(h * tile, (h + 1) * tile)
            o_all[g, tile_rows(r), h * HEAD_DIM:(h + 1) * HEAD_DIM] = (acc_s[r, at, :] / l_s[r, at, :]).astype(BF16)

    @scoped
    def attend_all(j):
        def step(t, carry):
            attend_block(t, j)
            return carry

        lax.fori_loop(0, 4, step, 0)

    def send_heads(t, g):
        o_tile = o_all.at[g, tile_rows(t % 4), :]
        pl.when(middle)(lambda: send(o_tile, o_tile, line_sem, o_recv.at[t], {'tp': 3 - z}))

    @scoped
    def heads_event(u):
        o_tile = o_all.at[g_1 if u < 4 else g_2, tile_rows(u % 4), :]
        arrived(o_tile, o_recv.at[u])
        for to, cond in ((0, z == 1), (3, z == 2)):
            pl.when(cond)(lambda: send(o_tile, o_tile, line_sem, o_recv.at[u], {'tp': to}))

    def heads_here(*tiles):
        on(middle, *((heads_event, u) for u in tiles))

    def on(cond, *todo):
        @pl.when(cond)
        def _():
            for what, *about in todo:
                what(*about)

    n_col = min(512, d_model)

    def project(g, rows, use):
        def cols(n, carry):
            at = pl.ds(pl.multiple_of(n * n_col, n_col), n_col)
            use(rows, at, jnp.dot(o_all[g, rows, :], wo[pl.ds(pl.multiple_of(g * width, width), width), at],
                                  preferred_element_type=F32).astype(BF16))
            return carry

        lax.fori_loop(0, d_model // n_col, cols, 0)

    @scoped
    def project_o(g):
        def keep(rows, at, fresh):
            part[g % 2, rows, at] = fresh

        project(g, every, keep)

    @scoped
    def project_third(g):
        def add(rows, at, fresh):
            pair_sum = part[(3 - g) % 2, rows, at].astype(F32) + fresh.astype(F32)
            run_s[rows, at] = hid[rows, at].astype(F32) + bo_ref[at].astype(F32) + pair_sum

        project(g, every, add)

    @scoped
    def project_last(g, rows):
        def add(rows, at, fresh):
            y_ref[rows, at] = (run_s[rows, at] + (part[(3 - g) % 2, rows, at].astype(F32) + fresh.astype(F32))).astype(BF16)

        project(g, rows, add)

    @scoped
    def kv_pass(i):
        @pl.when(y == 1)
        def _():
            arrived(kv.at[c, i], kv_recv.at[c, i])
            send(kv.at[c, i], kv.at[c, i], kv_sem, kv_recv.at[c, i], to_core)

    def own_block(t, carry):
        attend_own(t, carry)
        on(t == 0, (ev, 'q', 'zs', 0))
        on(t == 3, (kv_pass, 0))
        return carry

    lax.fori_loop(0, 4, own_block, 0)
    ev('q', 'zs', 1)
    on(middle, (ev, 'a', 'z'))

    @pl.when(c == 1)
    def _():
        arrived(seg.at[cp - 1], seg_recv.at[cp - 1])
        for i in (0, 1):
            arrived(kv.at[cp - 1, i], kv_recv.at[cp - 1, i])
        attend_all(cp - 1)

    kv_pass(1)
    ev('q', 'xy', 0)

    @pl.when(y == 1)
    def _():
        arrived(seg.at[c], seg_recv.at[c])
        attend_all(c)

    on(middle, (ev, 'b', 'z', 0), (ev, 'a', 's', 0))
    on(edge, (ev, 'a', 'zs', 0))
    ev('q', 'xy', 1)
    on(middle, (ev, 'b', 'z', 1), (ev, 'a', 's', 1))
    on(edge, (ev, 'a', 'zs', 1))

    @pl.when(y == 1)
    def _():
        arrived(seg.at[1 - c], seg_recv.at[1 - c])
        for i in (0, 1):
            arrived(kv.at[1 - c, i], kv_recv.at[1 - c, i])
        attend_all(1 - c)

    def own_heads(t, carry):
        attend_end(t, z)
        send_heads(t, z)
        return carry

    lax.fori_loop(0, 4, own_heads, 0)
    on(middle, (ev, 'b', 's'), (ev, 'c', 'z', 0))
    on(edge, (ev, 'b', 'zs', 0))
    loads[5].wait()
    project_o(z)
    ev('q', 'd')
    on(edge, (ev, 'b', 'zs', 1))
    ev('a', 'xy', 0)
    whole('q')
    arrived(bq_pair, bq_recv)
    project_q(1, bq_pair)
    on(middle, (ev, 'c', 'z', 1), (ev, 'c', 's'), (heads_event, 0))
    on(edge, (ev, 'c', 'zs', 0))
    ev('a', 'xy', 1)

    def pair_heads(t, carry):
        attend_own(t, carry)

        def block(j, inner):
            attend_block(t, j)
            return inner

        lax.fori_loop(0, cp, block, 0)
        attend_end(t, pair)
        send_heads(t, pair)
        on((t == 4) & middle, (heads_event, 1), (heads_event, 2))
        on((t == 4) & edge, (ev, 'c', 'zs', 1))
        on(t == 5, (ev, 'b', 'xy'))
        on((t == 5) & middle, (heads_event, 3))
        on(t == 6, (ev, 'a', 'd'))
        on((t == 6) & middle, (heads_event, 4))
        on((t == 7) & middle, (heads_event, 5))
        on(t == 7, (ev, 'c', 'xy'))
        return carry

    lax.fori_loop(4, 8, pair_heads, 0)
    heads_here(6)
    ev('b', 'd')
    whole('a')
    whole('b')
    project_o(pair)
    heads_here(7)
    on(edge, *((heads_event, u) for u in range(4)))
    loads[9].wait()
    project_third(g_1)
    ev('c', 'd')
    whole('c')

    def last(r, carry):
        pl.when(edge)(lambda: arrived(o_all.at[g_2, tile_rows(r), :], o_recv.at[4 + r]))
        project_last(g_2, tile_rows(r))
        return carry

    lax.fori_loop(0, 4, last, 0)

    with jax.named_scope('drain'):
        unit = o_rows // 2

        def sent(count, sems):
            arrived(wo.at[pl.ds(0, count * unit), :], sems)

        sent(58, spread_sem)
        pl.when(edge)(lambda: sent(2, line_sem))
        pl.when(middle)(lambda: sent(26, line_sem))
        for j in (0, 1):
            pl.when(c == j)(lambda: arrived(kv.at[pl.ds(0, 2 - j)], kv_sem))
        arrived(bq_pair, small_sem.at[0])
        for step in (1, 2, 3):
            pl.when(cp + step < 4)(lambda: arrived(seg.at[cp], small_sem.at[step]))


def write_out(y_in, k_in, v_in, y_out, k_out, v_out, sems):
    copies = [pltpu.make_async_copy(a, b, sems.at[i]) for i, (a, b) in enumerate(((y_in, y_out), (k_in, k_out), (v_in, v_out)))]
    for copy in copies:
        copy.start()
    for copy in copies:
        copy.wait()


def solution(mesh):
    def local_block(hidden, seg_ids, w_q, b_q, w_kv, b_kv, w_o, b_o, ln_gain, ln_bias):
        tok, d_model = hidden.shape
        width = w_q.shape[1]
        heads = width // HEAD_DIM
        tile = tok // 4
        hbm = pl.BlockSpec(memory_space=pltpu.HBM)
        vmem = pl.BlockSpec(memory_space=pltpu.VMEM)
        dma = pltpu.SemaphoreType.DMA
        far = lambda a: pltpu.with_memory_space_constraint(a, pltpu.HBM)
        outs = pl.pallas_call(
            kernel,
            out_shape=(jax.ShapeDtypeStruct((tok, d_model), BF16), jax.ShapeDtypeStruct((tok, HEAD_DIM), BF16),
                       jax.ShapeDtypeStruct((tok, HEAD_DIM), BF16)),
            in_specs=[hbm] * 10,
            out_specs=(vmem, vmem, vmem),
            scratch_shapes=[
                pltpu.VMEM((tok, d_model), BF16),
                pltpu.VMEM((tok, d_model), BF16),
                pltpu.VMEM((d_model, 2 * HEAD_DIM), BF16),
                pltpu.VMEM((2, d_model, width), BF16),
                pltpu.VMEM((4 * width, d_model), BF16),
                pltpu.VMEM((width,), BF16),
                pltpu.VMEM((width,), BF16),
                pltpu.VMEM((2 * HEAD_DIM,), BF16),
                pltpu.VMEM((d_model,), BF16),
                pltpu.VMEM((d_model,), BF16),
                pltpu.VMEM((d_model,), BF16),
                pltpu.VMEM((4, 1, tok), jnp.int32),
                pltpu.VMEM((4, tile, tile), jnp.int32),
                pltpu.VMEM((4, 2, tok, HEAD_DIM), BF16),
                pltpu.VMEM((8, heads * tile, HEAD_DIM), BF16),
                pltpu.VMEM((4, tok, width), BF16),
                pltpu.VMEM((2, tok, d_model), BF16),
                pltpu.VMEM((tok, d_model), F32),
                pltpu.VMEM((4, heads * tile, HEAD_DIM), F32),
                pltpu.VMEM((4, heads * tile, HEAD_DIM), F32),
                pltpu.VMEM((4, heads * tile, HEAD_DIM), F32),
                dma((10,)), dma(()), dma(()), dma(()), dma((4,)), dma(()), dma((4,)), dma((4, 2)), dma((9,)), dma((4, 9)), dma((8,)),
            ],
            compiler_params=pltpu.CompilerParams(collective_id=0, has_side_effects=True, vmem_limit_bytes=48 * 2 ** 20),
            name='block',
        )(far(hidden), far(seg_ids.reshape(1, -1)), far(w_q), far(b_q), far(w_kv), far(b_kv), far(w_o), far(b_o), far(ln_gain), far(ln_bias))
        near = lambda a: pltpu.with_memory_space_constraint(a, pltpu.VMEM)
        return pl.pallas_call(
            write_out,
            out_shape=tuple(jax.ShapeDtypeStruct(a.shape, a.dtype) for a in outs),
            in_specs=[vmem] * 3,
            out_specs=(pl.BlockSpec(memory_space=pl.ANY),) * 3,
            scratch_shapes=[dma((3,))],
            name='write',
        )(*map(near, outs))

    row_spec = P(('dp', 'cp'), None)
    tok_spec = P(('dp', 'cp'))
    return jax.shard_map(local_block, mesh=mesh,
                         in_specs=(row_spec, tok_spec, P(None, 'tp'), P('tp'), P(None, None), P(None), P('tp', None), P(None), P(None), P(None)),
                         out_specs=(row_spec, row_spec, row_spec), check_vma=False)
```

```python
import functools
import jax
import jax.numpy as jnp
from jax import lax
from jax.experimental import pallas as pl
from jax.experimental.pallas import tpu as pltpu
from jax.sharding import PartitionSpec as P

HEAD_DIM = 128
LN_EPS = 1e-5
SCORE_SCALE = HEAD_DIM ** -0.5 * 1.4426950408889634
MESH = pl.DeviceIdType.MESH
BF16 = jnp.bfloat16
F32 = jnp.float32


def send(src, dst, sent, recv, to):
    pltpu.make_async_remote_copy(src_ref=src, dst_ref=dst, send_sem=sent, recv_sem=recv, device_id=to, device_id_type=MESH).start()


def scoped(fn):
    def run(*about):
        with jax.named_scope(fn.__name__ + '_'.join(str(a) for a in about if isinstance(a, (str, int)))):
            return fn(*about)
    return run


def arrived(dst, recv):
    pltpu.make_async_copy(dst, dst, recv).wait()


def kernel(hid_hbm, seg_hbm, wq_hbm, bq_hbm, wkv_hbm, bkv_hbm, wo_hbm, bo_hbm, gain_hbm, lnb_hbm,
           y_ref, k_ref, v_ref,
           hid, normed, wkv, wq, wo, bq_own, bq_pair, bkv_ref, bo_ref, gain_ref, lnb_ref, seg, segcol, kv, q_s, o_all, part, run_s, m_s, l_s, acc_s,
           load_sem, spread_sem, line_sem, kv_sem, small_sem, bq_recv, seg_recv, kv_recv, wq_recv, wo_recv, o_recv):
    tok, d_model = hid.shape
    width = wq.shape[2]
    heads = width // HEAD_DIM
    tile = tok // 4
    q_rows, o_rows = d_model // 8, width // 8
    dp, z, cp = lax.axis_index('dp'), lax.axis_index('tp'), lax.axis_index('cp')
    y, c = cp // 2, cp % 2
    pair = z + 1 - 2 * (z % 2)
    below, above = {'tp': z - 1}, {'tp': z + 1}
    to_x, to_y, to_core = {'dp': 1 - dp}, {'cp': cp + 2 - 4 * y}, {'cp': cp + 1 - 2 * c}
    pos = lambda px, py, pc: px * 4 + py * 2 + pc
    p_me, p_x, p_y, p_d = pos(dp, y, c), pos(1 - dp, y, c), pos(dp, 1 - y, c), pos(1 - dp, 1 - y, c)
    g_a = 1 + z % 2
    g_c = 3 - 3 * (z // 2)
    g_b = 6 - z - g_a - g_c

    loads = [pltpu.make_async_copy(hid_hbm, hid, load_sem.at[0]),
             pltpu.make_async_copy(wkv_hbm, wkv, load_sem.at[1]),
             pltpu.make_async_copy(wq_hbm, wq.at[0], load_sem.at[2]),
             pltpu.make_async_copy(bq_hbm, bq_own, load_sem.at[3]),
             pltpu.make_async_copy(seg_hbm, seg.at[cp], load_sem.at[4]),
             pltpu.make_async_copy(wo_hbm, wo.at[pl.ds(z * width, width), :], load_sem.at[5]),
             pltpu.make_async_copy(gain_hbm, gain_ref, load_sem.at[6]),
             pltpu.make_async_copy(lnb_hbm, lnb_ref, load_sem.at[7]),
             pltpu.make_async_copy(bkv_hbm, bkv_ref, load_sem.at[8]),
             pltpu.make_async_copy(bo_hbm, bo_ref, load_sem.at[9])]
    for i in (0, 6, 7, 8, 3, 4, 9):
        loads[i].start()

    barrier = pltpu.get_barrier_semaphore()
    for step in (1, 2, 3):
        pl.semaphore_signal(barrier, inc=1, device_id={'cp': (cp + step) % 4}, device_id_type=MESH)
    pl.semaphore_signal(barrier, inc=1, device_id=to_x, device_id_type=MESH)

    @pl.when(z > 0)
    def _():
        pl.semaphore_signal(barrier, inc=1, device_id={'tp': z - 1}, device_id_type=MESH)

    @pl.when(z < 3)
    def _():
        pl.semaphore_signal(barrier, inc=1, device_id={'tp': z + 1}, device_id_type=MESH)

    loads[1].start()
    with jax.named_scope('barr'):
        pl.semaphore_wait(barrier, 5 + (z + 1) // 2 - 2 * (z // 3))

    loads[2].start()
    def q_piece(p, h):
        half = q_rows // 2
        return wq.at[1, pl.ds(pl.multiple_of(p * q_rows + h * half, half), half), :]

    def o_piece(g, p, h):
        half = o_rows // 2
        return wo.at[pl.ds(pl.multiple_of(g * width + p * o_rows + h * half, half), half), :]

    def sem(g, kind, h):
        at = {'z': 0, 'x': 2, 'y': 4, 'd': 6, 'core': 8}[kind] + (0 if kind == 'core' else h)
        return wq_recv.at[at] if g is None else wo_recv.at[g, at]

    middle, edge = (z > 0) & (z < 3), (z == 0) | (z == 3)

    send(bq_hbm, bq_pair, small_sem.at[0], bq_recv, {'tp': pair})
    for h in (0, 1):
        half = q_rows // 2
        send(wq_hbm.at[pl.ds(pl.multiple_of(p_me * q_rows + h * half, half), half), :], q_piece(p_me, h), spread_sem, sem(None, 'z', h),
             {'tp': pair})
    for h in (0, 1):
        half = o_rows // 2
        for to, cond in ((below, z > 0), (above, z < 3)):
            @pl.when(cond)
            def _():
                send(wo_hbm.at[pl.ds(pl.multiple_of(p_me * o_rows + h * half, half), half), :], o_piece(z, p_me, h), line_sem,
                     sem(z, 'z', h), to)
    for step in (1, 2, 3):
        pl.when(cp + step < 4)(lambda: send(seg_hbm, seg.at[cp], small_sem.at[step], seg_recv.at[cp], {'cp': cp + step}))

    def pass_on(g, source, h, by_x):
        p = {'z': p_me, 's': p_me, 'x': p_x, 'y': p_y, 'd': p_d}[source]
        piece = q_piece(p, h) if g is None else o_piece(g, p, h)
        if source == 's':
            send(piece, piece, spread_sem, sem(g, 'x', h), to_x)
            send(piece, piece, spread_sem, sem(g, 'y', h), to_y)
            return
        arrived(piece, sem(g, source, h))
        if source == 'z' and g is not None:
            pl.when((g > z) & (z > 0))(lambda: send(piece, piece, line_sem, sem(g, 'z', h), below))
            pl.when((g < z) & (z < 3))(lambda: send(piece, piece, line_sem, sem(g, 'z', h), above))
        elif source == 'x':
            if not by_x:
                pl.when(c == 1)(lambda: send(piece, piece, spread_sem, sem(g, 'd', h), to_y))
        elif source == 'y':
            pl.when((c == 0) | by_x)(lambda: send(piece, piece, spread_sem, sem(g, 'd', h), to_x))
        send(piece, piece, spread_sem, sem(g, 'core', h), to_core)

    groups = {'q': None, 'a': g_a, 'b': g_b, 'c': g_c}

    @scoped
    def ev(name, sources, *halves):
        for h in halves or (0, 1):
            for source in sources:
                pass_on(groups[name], source, h, name == 'a')

    @scoped
    def whole(name):
        if name == 'q':
            arrived(wq.at[1, pl.ds(0, 4 * q_rows), :], sem(None, 'core', 0))
        else:
            arrived(wo.at[pl.ds(0, 4 * o_rows), :], sem(groups[name], 'core', 0))

    loads[5].start()

    with jax.named_scope('load_wait'):
        for i in (0, 6, 7):
            loads[i].wait()
    gain = gain_ref[...].astype(F32)
    lnb = lnb_ref[...].astype(F32)
    ln_rows = min(64, tok)

    def ln_step(i, carry):
        rows = pl.ds(pl.multiple_of(i * ln_rows, ln_rows), ln_rows)
        x = hid[rows, :].astype(F32)
        cen = x - jnp.mean(x, axis=-1, keepdims=True)
        var = jnp.mean(cen * cen, axis=-1, keepdims=True)
        normed[rows, :] = (cen * lax.rsqrt(var + LN_EPS) * gain + lnb).astype(BF16)
        return carry

    with jax.named_scope('ln'):
        lax.fori_loop(0, tok // ln_rows, ln_step, 0)

    loads[1].wait()
    loads[8].wait()
    kv_new = (jnp.dot(normed[...], wkv[...], preferred_element_type=F32) + bkv_ref[...].astype(F32)).astype(BF16)
    kv[cp, 0] = kv_new[:, :HEAD_DIM]
    kv[cp, 1] = kv_new[:, HEAD_DIM:]
    k_ref[...] = kv_new[:, :HEAD_DIM]
    v_ref[...] = kv_new[:, HEAD_DIM:]

    @scoped
    def project_q(which, bias):
        qf = jnp.dot(normed[...], wq[which], preferred_element_type=F32) + bias[...].astype(F32)
        for r in range(4):
            for h in range(heads):
                q_s[which * 4 + r, h * tile:(h + 1) * tile, :] = qf[r * tile:(r + 1) * tile, h * HEAD_DIM:(h + 1) * HEAD_DIM].astype(BF16)

    loads[2].wait()
    loads[3].wait()
    for i in (0, 1):
        pl.when(y == 0)(lambda: send(kv.at[cp, i], kv.at[cp, i], kv_sem, kv_recv.at[cp, i], to_y))
    for i in (0, 1):
        pl.when(c == 0)(lambda: send(kv.at[cp, i], kv.at[cp, i], kv_sem, kv_recv.at[cp, i], to_core))
    project_q(0, bq_own)
    loads[4].wait()
    for r in range(4):
        row = jnp.broadcast_to(seg[cp, :, r * tile:(r + 1) * tile], (tile, tile))
        segcol[r] = row.T

    g_1, g_2 = 2 - z // 2, 3 - 3 * (z // 2)
    tile_rows = lambda r: pl.ds(pl.multiple_of(r * tile, tile), tile)
    every = pl.ds(0, tok)

    def scores(q, k_blk, mask):
        keys = k_blk.shape[0]
        s = lax.dot_general(q, k_blk, (((1,), (1,)), ((), ())), preferred_element_type=F32) * SCORE_SCALE
        return jnp.where(mask[None], s.reshape(heads, tile, keys), -jnp.inf).reshape(heads * tile, keys)

    @scoped
    def attend_own(t, carry):
        r = t % 4
        k_pos = lax.broadcasted_iota(jnp.int32, (tile, tok), 1)
        q_pos = lax.broadcasted_iota(jnp.int32, (tile, tok), 0) + r * tile
        s = scores(q_s[t], kv[cp, 0], (seg[cp] == segcol[r][:, :1]) & (k_pos <= q_pos))
        m_new = jnp.max(s, axis=-1, keepdims=True)
        p = jnp.exp2(s - m_new)
        m_s[r] = jnp.broadcast_to(m_new, m_s.shape[1:])
        l_s[r] = jnp.broadcast_to(jnp.sum(p, axis=-1, keepdims=True), l_s.shape[1:])
        acc_s[r] = jnp.dot(p.astype(BF16), kv[cp, 1], preferred_element_type=F32)
        return carry

    def attend_block(t, j):
        r = t % 4
        s = scores(q_s[t], kv[j, 0], seg[j] == segcol[r][:, :1])
        m_prev = m_s[r]
        m_new = jnp.maximum(m_prev, jnp.max(s, axis=-1, keepdims=True))
        p = jnp.exp2(s - m_new[:, :1])
        alpha = jnp.exp2(m_prev - m_new)
        m_s[r] = m_new
        l_s[r] = l_s[r] * alpha + jnp.sum(p, axis=-1, keepdims=True)
        acc_s[r] = acc_s[r] * alpha + jnp.dot(p.astype(BF16), kv[j, 1], preferred_element_type=F32)

    def attend_end(t, g):
        r = t % 4
        for h in range(heads):
            at = slice(h * tile, (h + 1) * tile)
            o_all[g, tile_rows(r), h * HEAD_DIM:(h + 1) * HEAD_DIM] = (acc_s[r, at, :] / l_s[r, at, :]).astype(BF16)

    def send_heads(t, g):
        o_tile = o_all.at[g, tile_rows(t % 4), :]
        pl.when(middle)(lambda: send(o_tile, o_tile, line_sem, o_recv.at[t], {'tp': 3 - z}))

    @scoped
    def heads_event(u):
        o_tile = o_all.at[g_1 if u < 4 else g_2, tile_rows(u % 4), :]
        arrived(o_tile, o_recv.at[u])
        for to, cond in ((0, z == 1), (3, z == 2)):
            pl.when(cond)(lambda: send(o_tile, o_tile, line_sem, o_recv.at[u], {'tp': to}))

    def heads_here(*tiles):
        on(middle, *((heads_event, u) for u in tiles))

    def on(cond, *todo):
        @pl.when(cond)
        def _():
            for what, *about in todo:
                what(*about)

    n_col = min(512, d_model)

    def project(g, rows, use):
        def cols(n, carry):
            at = pl.ds(pl.multiple_of(n * n_col, n_col), n_col)
            use(rows, at, jnp.dot(o_all[g, rows, :], wo[pl.ds(pl.multiple_of(g * width, width), width), at],
                                  preferred_element_type=F32).astype(BF16))
            return carry

        lax.fori_loop(0, d_model // n_col, cols, 0)

    @scoped
    def project_o(g):
        def keep(rows, at, fresh):
            part[g % 2, rows, at] = fresh

        project(g, every, keep)

    @scoped
    def project_third(g):
        def add(rows, at, fresh):
            pair_sum = part[(3 - g) % 2, rows, at].astype(F32) + fresh.astype(F32)
            run_s[rows, at] = hid[rows, at].astype(F32) + bo_ref[at].astype(F32) + pair_sum

        project(g, every, add)

    @scoped
    def project_last(g, rows):
        def add(rows, at, fresh):
            y_ref[rows, at] = (run_s[rows, at] + (part[(3 - g) % 2, rows, at].astype(F32) + fresh.astype(F32))).astype(BF16)

        project(g, rows, add)

    @scoped
    def kv_pass(i):
        @pl.when(y == 1)
        def _():
            arrived(kv.at[c, i], kv_recv.at[c, i])
            send(kv.at[c, i], kv.at[c, i], kv_sem, kv_recv.at[c, i], to_core)

    def own_block(t, carry):
        attend_own(t, carry)
        on(t == 0, (ev, 'q', 'zs', 0))
        on(t == 3, (kv_pass, 0))
        return carry

    lax.fori_loop(0, 4, own_block, 0)

    @pl.when(c == 1)
    def _():
        arrived(seg.at[cp - 1], seg_recv.at[cp - 1])
        for i in (0, 1):
            arrived(kv.at[cp - 1, i], kv_recv.at[cp - 1, i])

    def first_block(t, carry):
        pl.when(c == 1)(lambda: attend_block(t, cp - 1))
        on(t == 0, (ev, 'q', 'zs', 1))
        on(t == 1, (kv_pass, 1))
        on((t == 2) & middle, (ev, 'a', 'z', 0))
        on((t == 3) & middle, (ev, 'a', 'z', 1))
        on(t == 3, (ev, 'q', 'x', 0))
        return carry

    lax.fori_loop(0, 4, first_block, 0)
    pl.when(y == 1)(lambda: arrived(seg.at[c], seg_recv.at[c]))

    def second_block(t, carry):
        pl.when(y == 1)(lambda: attend_block(t, c))
        on(t == 1, (ev, 'q', 'y', 0))
        on((t == 2) & middle, (ev, 'b', 'z', 0), (ev, 'a', 's', 0))
        on((t == 2) & edge, (ev, 'a', 'zs', 0))
        on(t == 3, (ev, 'q', 'x', 1))
        return carry

    lax.fori_loop(0, 4, second_block, 0)

    @pl.when(y == 1)
    def _():
        arrived(seg.at[1 - c], seg_recv.at[1 - c])
        for i in (0, 1):
            arrived(kv.at[1 - c, i], kv_recv.at[1 - c, i])

    def third_block(t, carry):
        pl.when(y == 1)(lambda: attend_block(t, 1 - c))
        attend_end(t, z)
        send_heads(t, z)
        on((t == 0) & middle, (ev, 'b', 'z', 1))
        on(t == 1, (ev, 'q', 'y', 1))
        on((t == 2) & middle, (ev, 'a', 's', 1))
        on((t == 2) & edge, (ev, 'a', 'zs', 1))
        return carry

    lax.fori_loop(0, 4, third_block, 0)
    on(middle, (ev, 'b', 's'))
    on(edge, (ev, 'b', 'zs', 0))
    ev('q', 'd', 0)
    loads[5].wait()
    project_o(z)
    on(middle, (ev, 'c', 'z', 0))
    ev('q', 'd', 1)
    whole('q')
    arrived(bq_pair, bq_recv)
    project_q(1, bq_pair)
    on(edge, (ev, 'b', 'zs', 1))
    ev('a', 'xy', 0)
    on(middle, (ev, 'c', 'z', 1), (ev, 'c', 's'), (heads_event, 0))
    on(edge, (ev, 'c', 'zs', 0))

    def pair_heads(t, carry):
        attend_own(t, carry)

        def block(j, inner):
            attend_block(t, j)
            return inner

        lax.fori_loop(0, cp, block, 0)
        attend_end(t, pair)
        send_heads(t, pair)
        on(t == 4, (ev, 'a', 'xy', 1))
        on((t == 4) & middle, (heads_event, 1), (heads_event, 2))
        on((t == 4) & edge, (ev, 'c', 'zs', 1))
        on(t == 5, (ev, 'b', 'xy'))
        on((t == 5) & middle, (heads_event, 3))
        on(t == 6, (ev, 'a', 'd'))
        on((t == 6) & middle, (heads_event, 4))
        on((t == 7) & middle, (heads_event, 5))
        on(t == 7, (ev, 'c', 'xy'))
        return carry

    lax.fori_loop(4, 8, pair_heads, 0)
    heads_here(6)
    ev('b', 'd')
    whole('a')
    whole('b')
    project_o(pair)
    heads_here(7)
    on(edge, *((heads_event, u) for u in range(4)))
    loads[9].wait()
    project_third(g_1)
    ev('c', 'd')
    whole('c')

    pl.when(middle)(lambda: project_last(g_2, every))

    def last(r, carry):
        arrived(o_all.at[g_2, tile_rows(r), :], o_recv.at[4 + r])
        project_last(g_2, tile_rows(r))
        return carry

    @pl.when(edge)
    def _():
        lax.fori_loop(0, 4, last, 0)

    with jax.named_scope('drain'):
        unit = o_rows // 2

        def sent(count, sems):
            arrived(wo.at[pl.ds(0, count * unit), :], sems)

        sent(58, spread_sem)
        pl.when(edge)(lambda: sent(2, line_sem))
        pl.when(middle)(lambda: sent(26, line_sem))
        for j in (0, 1):
            pl.when(c == j)(lambda: arrived(kv.at[pl.ds(0, 2 - j)], kv_sem))
        arrived(bq_pair, small_sem.at[0])
        for step in (1, 2, 3):
            pl.when(cp + step < 4)(lambda: arrived(seg.at[cp], small_sem.at[step]))


def write_out(y_in, k_in, v_in, y_out, k_out, v_out, sems):
    copies = [pltpu.make_async_copy(a, b, sems.at[i]) for i, (a, b) in enumerate(((y_in, y_out), (k_in, k_out), (v_in, v_out)))]
    for copy in copies:
        copy.start()
    for copy in copies:
        copy.wait()


def solution(mesh):
    def local_block(hidden, seg_ids, w_q, b_q, w_kv, b_kv, w_o, b_o, ln_gain, ln_bias):
        tok, d_model = hidden.shape
        width = w_q.shape[1]
        heads = width // HEAD_DIM
        tile = tok // 4
        hbm = pl.BlockSpec(memory_space=pltpu.HBM)
        vmem = pl.BlockSpec(memory_space=pltpu.VMEM)
        dma = pltpu.SemaphoreType.DMA
        far = lambda a: pltpu.with_memory_space_constraint(a, pltpu.HBM)
        outs = pl.pallas_call(
            kernel,
            out_shape=(jax.ShapeDtypeStruct((tok, d_model), BF16), jax.ShapeDtypeStruct((tok, HEAD_DIM), BF16),
                       jax.ShapeDtypeStruct((tok, HEAD_DIM), BF16)),
            in_specs=[hbm] * 10,
            out_specs=(vmem, vmem, vmem),
            scratch_shapes=[
                pltpu.VMEM((tok, d_model), BF16),
                pltpu.VMEM((tok, d_model), BF16),
                pltpu.VMEM((d_model, 2 * HEAD_DIM), BF16),
                pltpu.VMEM((2, d_model, width), BF16),
                pltpu.VMEM((4 * width, d_model), BF16),
                pltpu.VMEM((width,), BF16),
                pltpu.VMEM((width,), BF16),
                pltpu.VMEM((2 * HEAD_DIM,), BF16),
                pltpu.VMEM((d_model,), BF16),
                pltpu.VMEM((d_model,), BF16),
                pltpu.VMEM((d_model,), BF16),
                pltpu.VMEM((4, 1, tok), jnp.int32),
                pltpu.VMEM((4, tile, tile), jnp.int32),
                pltpu.VMEM((4, 2, tok, HEAD_DIM), BF16),
                pltpu.VMEM((8, heads * tile, HEAD_DIM), BF16),
                pltpu.VMEM((4, tok, width), BF16),
                pltpu.VMEM((2, tok, d_model), BF16),
                pltpu.VMEM((tok, d_model), F32),
                pltpu.VMEM((4, heads * tile, HEAD_DIM), F32),
                pltpu.VMEM((4, heads * tile, HEAD_DIM), F32),
                pltpu.VMEM((4, heads * tile, HEAD_DIM), F32),
                dma((10,)), dma(()), dma(()), dma(()), dma((4,)), dma(()), dma((4,)), dma((4, 2)), dma((9,)), dma((4, 9)), dma((8,)),
            ],
            compiler_params=pltpu.CompilerParams(collective_id=0, has_side_effects=True, vmem_limit_bytes=48 * 2 ** 20),
            name='block',
        )(far(hidden), far(seg_ids.reshape(1, -1)), far(w_q), far(b_q), far(w_kv), far(b_kv), far(w_o), far(b_o), far(ln_gain), far(ln_bias))
        near = lambda a: pltpu.with_memory_space_constraint(a, pltpu.VMEM)
        return pl.pallas_call(
            write_out,
            out_shape=tuple(jax.ShapeDtypeStruct(a.shape, a.dtype) for a in outs),
            in_specs=[vmem] * 3,
            out_specs=(pl.BlockSpec(memory_space=pl.ANY),) * 3,
            scratch_shapes=[dma((3,))],
            name='write',
        )(*map(near, outs))

    row_spec = P(('dp', 'cp'), None)
    tok_spec = P(('dp', 'cp'))
    return jax.shard_map(local_block, mesh=mesh,
                         in_specs=(row_spec, tok_spec, P(None, 'tp'), P('tp'), P(None, None), P(None), P('tp', None), P(None), P(None), P(None)),
                         out_specs=(row_spec, row_spec, row_spec), check_vma=False)
```

```python
import functools
import jax
import jax.numpy as jnp
from jax import lax
from jax.experimental import pallas as pl
from jax.experimental.pallas import tpu as pltpu
from jax.sharding import PartitionSpec as P

HEAD_DIM = 128
LN_EPS = 1e-5
SCORE_SCALE = HEAD_DIM ** -0.5 * 1.4426950408889634
MESH = pl.DeviceIdType.MESH
BF16 = jnp.bfloat16
F32 = jnp.float32


def send(src, dst, sent, recv, to):
    pltpu.make_async_remote_copy(src_ref=src, dst_ref=dst, send_sem=sent, recv_sem=recv, device_id=to, device_id_type=MESH).start()


def scoped(fn):
    def run(*about):
        with jax.named_scope(fn.__name__ + '_'.join(str(a) for a in about if isinstance(a, (str, int)))):
            return fn(*about)
    return run


def arrived(dst, recv):
    pltpu.make_async_copy(dst, dst, recv).wait()


def kernel(hid_hbm, seg_hbm, wq_hbm, bq_hbm, wkv_hbm, bkv_hbm, wo_hbm, bo_hbm, gain_hbm, lnb_hbm,
           y_ref, k_ref, v_ref,
           hid, normed, wkv, wq, wo, bq_own, bq_pair, bkv_ref, bo_ref, gain_ref, lnb_ref, seg, segcol, kv, q_s, o_all, part, run_s, m_s, l_s, acc_s,
           load_sem, spread_sem, line_sem, kv_sem, small_sem, bq_recv, seg_recv, kv_recv, wq_recv, wo_recv, o_recv):
    tok, d_model = hid.shape
    width = wq.shape[2]
    heads = width // HEAD_DIM
    tile = tok // 4
    q_rows, o_rows = d_model // 8, width // 8
    dp, z, cp = lax.axis_index('dp'), lax.axis_index('tp'), lax.axis_index('cp')
    y, c = cp // 2, cp % 2
    pair = z + 1 - 2 * (z % 2)
    below, above = {'tp': z - 1}, {'tp': z + 1}
    to_x, to_y, to_core = {'dp': 1 - dp}, {'cp': cp + 2 - 4 * y}, {'cp': cp + 1 - 2 * c}
    pos = lambda px, py, pc: px * 4 + py * 2 + pc
    p_me, p_x, p_y, p_d = pos(dp, y, c), pos(1 - dp, y, c), pos(dp, 1 - y, c), pos(1 - dp, 1 - y, c)
    g_a = 1 + z % 2
    g_c = 3 - 3 * (z // 2)
    g_b = 6 - z - g_a - g_c

    loads = [pltpu.make_async_copy(hid_hbm, hid, load_sem.at[0]),
             pltpu.make_async_copy(wkv_hbm, wkv, load_sem.at[1]),
             pltpu.make_async_copy(wq_hbm, wq.at[0], load_sem.at[2]),
             pltpu.make_async_copy(bq_hbm, bq_own, load_sem.at[3]),
             pltpu.make_async_copy(seg_hbm, seg.at[cp], load_sem.at[4]),
             pltpu.make_async_copy(wo_hbm, wo.at[pl.ds(z * width, width), :], load_sem.at[5]),
             pltpu.make_async_copy(gain_hbm, gain_ref, load_sem.at[6]),
             pltpu.make_async_copy(lnb_hbm, lnb_ref, load_sem.at[7]),
             pltpu.make_async_copy(bkv_hbm, bkv_ref, load_sem.at[8]),
             pltpu.make_async_copy(bo_hbm, bo_ref, load_sem.at[9])]
    for i in (0, 6, 7, 8, 3, 4, 9):
        loads[i].start()

    barrier = pltpu.get_barrier_semaphore()
    for step in (1, 2, 3):
        pl.semaphore_signal(barrier, inc=1, device_id={'cp': (cp + step) % 4}, device_id_type=MESH)
    pl.semaphore_signal(barrier, inc=1, device_id=to_x, device_id_type=MESH)

    @pl.when(z > 0)
    def _():
        pl.semaphore_signal(barrier, inc=1, device_id={'tp': z - 1}, device_id_type=MESH)

    @pl.when(z < 3)
    def _():
        pl.semaphore_signal(barrier, inc=1, device_id={'tp': z + 1}, device_id_type=MESH)

    loads[1].start()
    with jax.named_scope('barr'):
        pl.semaphore_wait(barrier, 5 + (z + 1) // 2 - 2 * (z // 3))

    loads[2].start()
    def q_piece(p, h):
        half = q_rows // 2
        return wq.at[1, pl.ds(pl.multiple_of(p * q_rows + h * half, half), half), :]

    def o_piece(g, p, h):
        half = o_rows // 2
        return wo.at[pl.ds(pl.multiple_of(g * width + p * o_rows + h * half, half), half), :]

    def sem(g, kind, h):
        at = {'z': 0, 'x': 2, 'y': 4, 'd': 6, 'core': 8}[kind] + (0 if kind == 'core' else h)
        return wq_recv.at[at] if g is None else wo_recv.at[g, at]

    middle, edge = (z > 0) & (z < 3), (z == 0) | (z == 3)

    send(bq_hbm, bq_pair, small_sem.at[0], bq_recv, {'tp': pair})
    for h in (0, 1):
        half = q_rows // 2
        send(wq_hbm.at[pl.ds(pl.multiple_of(p_me * q_rows + h * half, half), half), :], q_piece(p_me, h), spread_sem, sem(None, 'z', h),
             {'tp': pair})
    for h in (0, 1):
        half = o_rows // 2
        for to, cond in ((below, z > 0), (above, z < 3)):
            @pl.when(cond)
            def _():
                send(wo_hbm.at[pl.ds(pl.multiple_of(p_me * o_rows + h * half, half), half), :], o_piece(z, p_me, h), line_sem,
                     sem(z, 'z', h), to)
    for step in (1, 2, 3):
        pl.when(cp + step < 4)(lambda: send(seg_hbm, seg.at[cp], small_sem.at[step], seg_recv.at[cp], {'cp': cp + step}))

    def pass_on(g, source, h, by_x):
        p = {'z': p_me, 's': p_me, 'x': p_x, 'y': p_y, 'd': p_d}[source]
        piece = q_piece(p, h) if g is None else o_piece(g, p, h)
        if source == 's':
            send(piece, piece, spread_sem, sem(g, 'x', h), to_x)
            send(piece, piece, spread_sem, sem(g, 'y', h), to_y)
            return
        arrived(piece, sem(g, source, h))
        if source == 'z' and g is not None:
            pl.when((g > z) & (z > 0))(lambda: send(piece, piece, line_sem, sem(g, 'z', h), below))
            pl.when((g < z) & (z < 3))(lambda: send(piece, piece, line_sem, sem(g, 'z', h), above))
        elif source == 'x':
            if not by_x:
                pl.when(c == 1)(lambda: send(piece, piece, spread_sem, sem(g, 'd', h), to_y))
        elif source == 'y':
            pl.when((c == 0) | by_x)(lambda: send(piece, piece, spread_sem, sem(g, 'd', h), to_x))
        send(piece, piece, spread_sem, sem(g, 'core', h), to_core)

    groups = {'q': None, 'a': g_a, 'b': g_b, 'c': g_c}

    @scoped
    def ev(name, sources, *halves):
        for h in halves or (0, 1):
            for source in sources:
                pass_on(groups[name], source, h, name == 'a')

    @scoped
    def whole(name):
        if name == 'q':
            arrived(wq.at[1, pl.ds(0, 4 * q_rows), :], sem(None, 'core', 0))
        else:
            arrived(wo.at[pl.ds(0, 4 * o_rows), :], sem(groups[name], 'core', 0))

    loads[5].start()

    with jax.named_scope('load_wait'):
        for i in (0, 6, 7):
            loads[i].wait()
    gain = gain_ref[...].astype(F32)
    lnb = lnb_ref[...].astype(F32)
    ln_rows = min(64, tok)

    def ln_step(i, carry):
        rows = pl.ds(pl.multiple_of(i * ln_rows, ln_rows), ln_rows)
        x = hid[rows, :].astype(F32)
        cen = x - jnp.mean(x, axis=-1, keepdims=True)
        var = jnp.mean(cen * cen, axis=-1, keepdims=True)
        normed[rows, :] = (cen * lax.rsqrt(var + LN_EPS) * gain + lnb).astype(BF16)
        return carry

    with jax.named_scope('ln'):
        lax.fori_loop(0, tok // ln_rows, ln_step, 0)

    loads[1].wait()
    loads[8].wait()
    kv_new = (jnp.dot(normed[...], wkv[...], preferred_element_type=F32) + bkv_ref[...].astype(F32)).astype(BF16)
    kv[cp, 0] = kv_new[:, :HEAD_DIM]
    kv[cp, 1] = kv_new[:, HEAD_DIM:]
    k_ref[...] = kv_new[:, :HEAD_DIM]
    v_ref[...] = kv_new[:, HEAD_DIM:]

    @scoped
    def project_q(which, bias):
        qf = jnp.dot(normed[...], wq[which], preferred_element_type=F32) + bias[...].astype(F32)
        for r in range(4):
            for h in range(heads):
                q_s[which * 4 + r, h * tile:(h + 1) * tile, :] = qf[r * tile:(r + 1) * tile, h * HEAD_DIM:(h + 1) * HEAD_DIM].astype(BF16)

    loads[2].wait()
    loads[3].wait()
    for i in (0, 1):
        pl.when(y == 0)(lambda: send(kv.at[cp, i], kv.at[cp, i], kv_sem, kv_recv.at[cp, i], to_y))
    for i in (0, 1):
        pl.when(c == 0)(lambda: send(kv.at[cp, i], kv.at[cp, i], kv_sem, kv_recv.at[cp, i], to_core))
    project_q(0, bq_own)
    loads[4].wait()
    for r in range(4):
        row = jnp.broadcast_to(seg[cp, :, r * tile:(r + 1) * tile], (tile, tile))
        segcol[r] = row.T

    g_1, g_2 = 2 - z // 2, 3 - 3 * (z // 2)
    tile_rows = lambda r: pl.ds(pl.multiple_of(r * tile, tile), tile)
    every = pl.ds(0, tok)

    def scores(q, k_blk, mask):
        keys = k_blk.shape[0]
        s = lax.dot_general(q, k_blk, (((1,), (1,)), ((), ())), preferred_element_type=F32) * SCORE_SCALE
        return jnp.where(mask[None], s.reshape(heads, tile, keys), -jnp.inf).reshape(heads * tile, keys)

    @scoped
    def attend_own(t, carry):
        r = t % 4
        k_pos = lax.broadcasted_iota(jnp.int32, (tile, tok), 1)
        q_pos = lax.broadcasted_iota(jnp.int32, (tile, tok), 0) + r * tile
        s = scores(q_s[t], kv[cp, 0], (seg[cp] == segcol[r][:, :1]) & (k_pos <= q_pos))
        m_new = jnp.max(s, axis=-1, keepdims=True)
        p = jnp.exp2(s - m_new)
        m_s[r] = jnp.broadcast_to(m_new, m_s.shape[1:])
        l_s[r] = jnp.broadcast_to(jnp.sum(p, axis=-1, keepdims=True), l_s.shape[1:])
        acc_s[r] = jnp.dot(p.astype(BF16), kv[cp, 1], preferred_element_type=F32)
        return carry

    def attend_block(t, j):
        r = t % 4
        s = scores(q_s[t], kv[j, 0], seg[j] == segcol[r][:, :1])
        m_prev = m_s[r]
        m_new = jnp.maximum(m_prev, jnp.max(s, axis=-1, keepdims=True))
        p = jnp.exp2(s - m_new[:, :1])
        alpha = jnp.exp2(m_prev - m_new)
        m_s[r] = m_new
        l_s[r] = l_s[r] * alpha + jnp.sum(p, axis=-1, keepdims=True)
        acc_s[r] = acc_s[r] * alpha + jnp.dot(p.astype(BF16), kv[j, 1], preferred_element_type=F32)

    def attend_end(t, g):
        r = t % 4
        for h in range(heads):
            at = slice(h * tile, (h + 1) * tile)
            o_all[g, tile_rows(r), h * HEAD_DIM:(h + 1) * HEAD_DIM] = (acc_s[r, at, :] / l_s[r, at, :]).astype(BF16)

    def send_heads(t, g):
        o_tile = o_all.at[g, tile_rows(t % 4), :]
        pl.when(middle)(lambda: send(o_tile, o_tile, line_sem, o_recv.at[t], {'tp': 3 - z}))

    @scoped
    def heads_event(u):
        o_tile = o_all.at[g_1 if u < 4 else g_2, tile_rows(u % 4), :]
        arrived(o_tile, o_recv.at[u])
        for to, cond in ((0, z == 1), (3, z == 2)):
            pl.when(cond)(lambda: send(o_tile, o_tile, line_sem, o_recv.at[u], {'tp': to}))

    def heads_here(*tiles):
        on(middle, *((heads_event, u) for u in tiles))

    def on(cond, *todo):
        @pl.when(cond)
        def _():
            for what, *about in todo:
                what(*about)

    n_col = min(512, d_model)

    def project(g, rows, use):
        def cols(n, carry):
            at = pl.ds(pl.multiple_of(n * n_col, n_col), n_col)
            use(rows, at, jnp.dot(o_all[g, rows, :], wo[pl.ds(pl.multiple_of(g * width, width), width), at],
                                  preferred_element_type=F32).astype(BF16))
            return carry

        lax.fori_loop(0, d_model // n_col, cols, 0)

    @scoped
    def project_o(g):
        def keep(rows, at, fresh):
            part[g % 2, rows, at] = fresh

        project(g, every, keep)

    @scoped
    def project_third(g):
        def add(rows, at, fresh):
            pair_sum = part[(3 - g) % 2, rows, at].astype(F32) + fresh.astype(F32)
            run_s[rows, at] = hid[rows, at].astype(F32) + bo_ref[at].astype(F32) + pair_sum

        project(g, every, add)

    @scoped
    def project_last(g, rows):
        def add(rows, at, fresh):
            y_ref[rows, at] = (run_s[rows, at] + (part[(3 - g) % 2, rows, at].astype(F32) + fresh.astype(F32))).astype(BF16)

        project(g, rows, add)

    @scoped
    def kv_pass(i):
        @pl.when(y == 1)
        def _():
            arrived(kv.at[c, i], kv_recv.at[c, i])
            send(kv.at[c, i], kv.at[c, i], kv_sem, kv_recv.at[c, i], to_core)

    def own_block(t, carry):
        attend_own(t, carry)
        on(t == 0, (ev, 'q', 'zs', 0))
        on(t == 3, (kv_pass, 0))
        return carry

    lax.fori_loop(0, 4, own_block, 0)

    @pl.when(c == 1)
    def _():
        arrived(seg.at[cp - 1], seg_recv.at[cp - 1])
        for i in (0, 1):
            arrived(kv.at[cp - 1, i], kv_recv.at[cp - 1, i])

    def first_block(t, carry):
        pl.when(c == 1)(lambda: attend_block(t, cp - 1))
        on(t == 0, (ev, 'q', 'zs', 1))
        on(t == 1, (kv_pass, 1))
        on((t == 2) & middle, (ev, 'a', 'z', 0))
        on((t == 3) & middle, (ev, 'a', 'z', 1))
        on(t == 3, (ev, 'q', 'x', 0))
        on((t == 3) & middle, (ev, 'a', 's', 0))
        return carry

    lax.fori_loop(0, 4, first_block, 0)
    pl.when(y == 1)(lambda: arrived(seg.at[c], seg_recv.at[c]))

    def second_block(t, carry):
        pl.when(y == 1)(lambda: attend_block(t, c))
        on(t == 1, (ev, 'q', 'y', 0))
        on((t == 2) & middle, (ev, 'b', 'z', 0))
        on((t == 2) & edge, (ev, 'a', 'zs', 0))
        on(t == 3, (ev, 'q', 'x', 1))
        return carry

    lax.fori_loop(0, 4, second_block, 0)

    @pl.when(y == 1)
    def _():
        arrived(seg.at[1 - c], seg_recv.at[1 - c])
        for i in (0, 1):
            arrived(kv.at[1 - c, i], kv_recv.at[1 - c, i])

    def third_block(t, carry):
        pl.when(y == 1)(lambda: attend_block(t, 1 - c))
        attend_end(t, z)
        send_heads(t, z)
        on((t == 0) & middle, (ev, 'b', 'z', 1))
        on(t == 1, (ev, 'q', 'y', 1))
        on((t == 1) & middle, (ev, 'a', 's', 1))
        on((t == 2) & middle, (ev, 'b', 's', 0))
        on((t == 2) & edge, (ev, 'a', 'zs', 1))
        return carry

    lax.fori_loop(0, 4, third_block, 0)
    on(edge, (ev, 'b', 'zs', 0))
    on(middle, (ev, 'c', 'z', 0))
    ev('a', 'xy', 0)
    ev('q', 'd', 0)
    on(middle, (ev, 'b', 's', 1))
    loads[5].wait()
    project_o(z)
    on(edge, (ev, 'b', 'zs', 1))
    ev('q', 'd', 1)
    whole('q')
    arrived(bq_pair, bq_recv)
    project_q(1, bq_pair)
    ev('a', 'xy', 1)
    on(middle, (ev, 'c', 'z', 1), (ev, 'c', 's', 0), (heads_event, 0))
    on(edge, (ev, 'c', 'zs', 0))

    def pair_heads(t, carry):
        attend_own(t, carry)
        on((t == 4) & middle, (heads_event, 1))
        on(t == 5, (ev, 'b', 'xy', 0))

        def block(j, inner):
            attend_block(t, j)
            return inner

        lax.fori_loop(0, cp, block, 0)
        attend_end(t, pair)
        send_heads(t, pair)
        on(t == 4, (ev, 'a', 'd', 0))
        on((t == 4) & edge, (ev, 'c', 'zs', 1))
        on((t == 4) & middle, (heads_event, 2))
        on(t == 5, (ev, 'a', 'd', 1))
        on((t == 5) & middle, (ev, 'c', 's', 1), (heads_event, 3))
        on(t == 6, (ev, 'b', 'xy', 1))
        on((t == 6) & middle, (heads_event, 4))
        on(t == 7, (ev, 'c', 'xy', 0))
        on((t == 7) & middle, (heads_event, 5))
        return carry

    lax.fori_loop(4, 8, pair_heads, 0)
    heads_here(6)
    ev('b', 'd', 0)
    ev('c', 'xy', 1)
    ev('b', 'd', 1)
    whole('a')
    whole('b')
    project_o(pair)
    heads_here(7)
    on(edge, *((heads_event, u) for u in range(4)))
    loads[9].wait()
    project_third(g_1)
    ev('c', 'd')
    whole('c')

    pl.when(middle)(lambda: project_last(g_2, every))

    def last(r, carry):
        arrived(o_all.at[g_2, tile_rows(r), :], o_recv.at[4 + r])
        project_last(g_2, tile_rows(r))
        return carry

    @pl.when(edge)
    def _():
        lax.fori_loop(0, 4, last, 0)

    with jax.named_scope('drain'):
        unit = o_rows // 2

        def sent(count, sems):
            arrived(wo.at[pl.ds(0, count * unit), :], sems)

        sent(58, spread_sem)
        pl.when(edge)(lambda: sent(2, line_sem))
        pl.when(middle)(lambda: sent(26, line_sem))
        for j in (0, 1):
            pl.when(c == j)(lambda: arrived(kv.at[pl.ds(0, 2 - j)], kv_sem))
        arrived(bq_pair, small_sem.at[0])
        for step in (1, 2, 3):
            pl.when(cp + step < 4)(lambda: arrived(seg.at[cp], small_sem.at[step]))


def write_out(y_in, k_in, v_in, y_out, k_out, v_out, sems):
    copies = [pltpu.make_async_copy(a, b, sems.at[i]) for i, (a, b) in enumerate(((y_in, y_out), (k_in, k_out), (v_in, v_out)))]
    for copy in copies:
        copy.start()
    for copy in copies:
        copy.wait()


def solution(mesh):
    def local_block(hidden, seg_ids, w_q, b_q, w_kv, b_kv, w_o, b_o, ln_gain, ln_bias):
        tok, d_model = hidden.shape
        width = w_q.shape[1]
        heads = width // HEAD_DIM
        tile = tok // 4
        hbm = pl.BlockSpec(memory_space=pltpu.HBM)
        vmem = pl.BlockSpec(memory_space=pltpu.VMEM)
        dma = pltpu.SemaphoreType.DMA
        far = lambda a: pltpu.with_memory_space_constraint(a, pltpu.HBM)
        outs = pl.pallas_call(
            kernel,
            out_shape=(jax.ShapeDtypeStruct((tok, d_model), BF16), jax.ShapeDtypeStruct((tok, HEAD_DIM), BF16),
                       jax.ShapeDtypeStruct((tok, HEAD_DIM), BF16)),
            in_specs=[hbm] * 10,
            out_specs=(vmem, vmem, vmem),
            scratch_shapes=[
                pltpu.VMEM((tok, d_model), BF16),
                pltpu.VMEM((tok, d_model), BF16),
                pltpu.VMEM((d_model, 2 * HEAD_DIM), BF16),
                pltpu.VMEM((2, d_model, width), BF16),
                pltpu.VMEM((4 * width, d_model), BF16),
                pltpu.VMEM((width,), BF16),
                pltpu.VMEM((width,), BF16),
                pltpu.VMEM((2 * HEAD_DIM,), BF16),
                pltpu.VMEM((d_model,), BF16),
                pltpu.VMEM((d_model,), BF16),
                pltpu.VMEM((d_model,), BF16),
                pltpu.VMEM((4, 1, tok), jnp.int32),
                pltpu.VMEM((4, tile, tile), jnp.int32),
                pltpu.VMEM((4, 2, tok, HEAD_DIM), BF16),
                pltpu.VMEM((8, heads * tile, HEAD_DIM), BF16),
                pltpu.VMEM((4, tok, width), BF16),
                pltpu.VMEM((2, tok, d_model), BF16),
                pltpu.VMEM((tok, d_model), F32),
                pltpu.VMEM((4, heads * tile, HEAD_DIM), F32),
                pltpu.VMEM((4, heads * tile, HEAD_DIM), F32),
                pltpu.VMEM((4, heads * tile, HEAD_DIM), F32),
                dma((10,)), dma(()), dma(()), dma(()), dma((4,)), dma(()), dma((4,)), dma((4, 2)), dma((9,)), dma((4, 9)), dma((8,)),
            ],
            compiler_params=pltpu.CompilerParams(collective_id=0, has_side_effects=True, vmem_limit_bytes=48 * 2 ** 20),
            name='block',
        )(far(hidden), far(seg_ids.reshape(1, -1)), far(w_q), far(b_q), far(w_kv), far(b_kv), far(w_o), far(b_o), far(ln_gain), far(ln_bias))
        near = lambda a: pltpu.with_memory_space_constraint(a, pltpu.VMEM)
        return pl.pallas_call(
            write_out,
            out_shape=tuple(jax.ShapeDtypeStruct(a.shape, a.dtype) for a in outs),
            in_specs=[vmem] * 3,
            out_specs=(pl.BlockSpec(memory_space=pl.ANY),) * 3,
            scratch_shapes=[dma((3,))],
            name='write',
        )(*map(near, outs))

    row_spec = P(('dp', 'cp'), None)
    tok_spec = P(('dp', 'cp'))
    return jax.shard_map(local_block, mesh=mesh,
                         in_specs=(row_spec, tok_spec, P(None, 'tp'), P('tp'), P(None, None), P(None), P('tp', None), P(None), P(None), P(None)),
                         out_specs=(row_spec, row_spec, row_spec), check_vma=False)
```

```python
import functools
import jax
import jax.numpy as jnp
from jax import lax
from jax.experimental import pallas as pl
from jax.experimental.pallas import tpu as pltpu
from jax.sharding import PartitionSpec as P

HEAD_DIM = 128
LN_EPS = 1e-5
SCORE_SCALE = HEAD_DIM ** -0.5 * 1.4426950408889634
MESH = pl.DeviceIdType.MESH
BF16 = jnp.bfloat16
F32 = jnp.float32


def send(src, dst, sent, recv, to):
    pltpu.make_async_remote_copy(src_ref=src, dst_ref=dst, send_sem=sent, recv_sem=recv, device_id=to, device_id_type=MESH).start()


def scoped(fn):
    def run(*about):
        with jax.named_scope(fn.__name__ + '_'.join(str(a) for a in about if isinstance(a, (str, int)))):
            return fn(*about)
    return run


def arrived(dst, recv):
    pltpu.make_async_copy(dst, dst, recv).wait()


def kernel(hid_hbm, seg_hbm, wq_hbm, bq_hbm, wkv_hbm, bkv_hbm, wo_hbm, bo_hbm, gain_hbm, lnb_hbm,
           y_ref, k_ref, v_ref,
           hid, normed, wkv, wq, wo, bq_own, bq_pair, bkv_ref, bo_ref, gain_ref, lnb_ref, seg, segcol, kv, q_s, o_all, part, run_s, m_s, l_s, acc_s,
           load_sem, spread_sem, line_sem, kv_sem, small_sem, bq_recv, seg_recv, kv_recv, wq_recv, wo_recv, o_recv):
    tok, d_model = hid.shape
    width = wq.shape[2]
    heads = width // HEAD_DIM
    tile = tok // 4
    q_rows, o_rows = d_model // 8, width // 8
    dp, z, cp = lax.axis_index('dp'), lax.axis_index('tp'), lax.axis_index('cp')
    y, c = cp // 2, cp % 2
    pair = z + 1 - 2 * (z % 2)
    below, above = {'tp': z - 1}, {'tp': z + 1}
    to_x, to_y, to_core = {'dp': 1 - dp}, {'cp': cp + 2 - 4 * y}, {'cp': cp + 1 - 2 * c}
    pos = lambda px, py, pc: px * 4 + py * 2 + pc
    p_me, p_x, p_y, p_d = pos(dp, y, c), pos(1 - dp, y, c), pos(dp, 1 - y, c), pos(1 - dp, 1 - y, c)
    g_a = 1 + z % 2
    g_c = 3 - 3 * (z // 2)
    g_b = 6 - z - g_a - g_c

    loads = [pltpu.make_async_copy(hid_hbm, hid, load_sem.at[0]),
             pltpu.make_async_copy(wkv_hbm, wkv, load_sem.at[1]),
             pltpu.make_async_copy(wq_hbm, wq.at[0], load_sem.at[2]),
             pltpu.make_async_copy(bq_hbm, bq_own, load_sem.at[3]),
             pltpu.make_async_copy(seg_hbm, seg.at[cp], load_sem.at[4]),
             pltpu.make_async_copy(wo_hbm, wo.at[pl.ds(z * width, width), :], load_sem.at[5]),
             pltpu.make_async_copy(gain_hbm, gain_ref, load_sem.at[6]),
             pltpu.make_async_copy(lnb_hbm, lnb_ref, load_sem.at[7]),
             pltpu.make_async_copy(bkv_hbm, bkv_ref, load_sem.at[8]),
             pltpu.make_async_copy(bo_hbm, bo_ref, load_sem.at[9])]
    for i in (0, 6, 7, 8, 3, 4, 9):
        loads[i].start()

    barrier = pltpu.get_barrier_semaphore()
    for step in (1, 2, 3):
        pl.semaphore_signal(barrier, inc=1, device_id={'cp': (cp + step) % 4}, device_id_type=MESH)
    pl.semaphore_signal(barrier, inc=1, device_id=to_x, device_id_type=MESH)

    @pl.when(z > 0)
    def _():
        pl.semaphore_signal(barrier, inc=1, device_id={'tp': z - 1}, device_id_type=MESH)

    @pl.when(z < 3)
    def _():
        pl.semaphore_signal(barrier, inc=1, device_id={'tp': z + 1}, device_id_type=MESH)

    loads[1].start()
    with jax.named_scope('barr'):
        pl.semaphore_wait(barrier, 5 + (z + 1) // 2 - 2 * (z // 3))

    loads[2].start()
    def q_piece(p, h):
        half = q_rows // 2
        return wq.at[1, pl.ds(pl.multiple_of(p * q_rows + h * half, half), half), :]

    def o_piece(g, p, h):
        half = o_rows // 2
        return wo.at[pl.ds(pl.multiple_of(g * width + p * o_rows + h * half, half), half), :]

    def sem(g, kind, h):
        at = {'z': 0, 'x': 2, 'y': 4, 'd': 6, 'core': 8}[kind] + (0 if kind == 'core' else h)
        return wq_recv.at[at] if g is None else wo_recv.at[g, at]

    middle, edge = (z > 0) & (z < 3), (z == 0) | (z == 3)

    send(bq_hbm, bq_pair, small_sem.at[0], bq_recv, {'tp': pair})
    for h in (0, 1):
        half = q_rows // 2
        send(wq_hbm.at[pl.ds(pl.multiple_of(p_me * q_rows + h * half, half), half), :], q_piece(p_me, h), spread_sem, sem(None, 'z', h),
             {'tp': pair})
    for h in (0, 1):
        half = o_rows // 2
        for to, cond in ((below, z > 0), (above, z < 3)):
            @pl.when(cond)
            def _():
                send(wo_hbm.at[pl.ds(pl.multiple_of(p_me * o_rows + h * half, half), half), :], o_piece(z, p_me, h), line_sem,
                     sem(z, 'z', h), to)
    for step in (1, 2, 3):
        pl.when(cp + step < 4)(lambda: send(seg_hbm, seg.at[cp], small_sem.at[step], seg_recv.at[cp], {'cp': cp + step}))

    def pass_on(g, source, h, by_x):
        p = {'z': p_me, 's': p_me, 'x': p_x, 'y': p_y, 'd': p_d}[source]
        piece = q_piece(p, h) if g is None else o_piece(g, p, h)
        if source == 's':
            send(piece, piece, spread_sem, sem(g, 'x', h), to_x)
            send(piece, piece, spread_sem, sem(g, 'y', h), to_y)
            return
        arrived(piece, sem(g, source, h))
        if source == 'z' and g is not None:
            pl.when((g > z) & (z > 0))(lambda: send(piece, piece, line_sem, sem(g, 'z', h), below))
            pl.when((g < z) & (z < 3))(lambda: send(piece, piece, line_sem, sem(g, 'z', h), above))
        elif source == 'x':
            if not by_x:
                pl.when(c == 1)(lambda: send(piece, piece, spread_sem, sem(g, 'd', h), to_y))
        elif source == 'y':
            pl.when((c == 0) | by_x)(lambda: send(piece, piece, spread_sem, sem(g, 'd', h), to_x))
        send(piece, piece, spread_sem, sem(g, 'core', h), to_core)

    groups = {'q': None, 'a': g_a, 'b': g_b, 'c': g_c}

    @scoped
    def ev(name, sources, *halves):
        for h in halves or (0, 1):
            for source in sources:
                pass_on(groups[name], source, h, name == 'q')

    @scoped
    def whole(name):
        if name == 'q':
            arrived(wq.at[1, pl.ds(0, 4 * q_rows), :], sem(None, 'core', 0))
        else:
            arrived(wo.at[pl.ds(0, 4 * o_rows), :], sem(groups[name], 'core', 0))

    loads[5].start()

    with jax.named_scope('load_wait'):
        for i in (0, 6, 7):
            loads[i].wait()
    gain = gain_ref[...].astype(F32)
    lnb = lnb_ref[...].astype(F32)
    ln_rows = min(64, tok)

    def ln_step(i, carry):
        rows = pl.ds(pl.multiple_of(i * ln_rows, ln_rows), ln_rows)
        x = hid[rows, :].astype(F32)
        cen = x - jnp.mean(x, axis=-1, keepdims=True)
        var = jnp.mean(cen * cen, axis=-1, keepdims=True)
        normed[rows, :] = (cen * lax.rsqrt(var + LN_EPS) * gain + lnb).astype(BF16)
        return carry

    with jax.named_scope('ln'):
        lax.fori_loop(0, tok // ln_rows, ln_step, 0)

    loads[1].wait()
    loads[8].wait()
    kv_new = (jnp.dot(normed[...], wkv[...], preferred_element_type=F32) + bkv_ref[...].astype(F32)).astype(BF16)
    kv[cp, 0] = kv_new[:, :HEAD_DIM]
    kv[cp, 1] = kv_new[:, HEAD_DIM:]
    k_ref[...] = kv_new[:, :HEAD_DIM]
    v_ref[...] = kv_new[:, HEAD_DIM:]

    @scoped
    def project_q(which, bias):
        qf = jnp.dot(normed[...], wq[which], preferred_element_type=F32) + bias[...].astype(F32)
        for r in range(4):
            for h in range(heads):
                q_s[which * 4 + r, h * tile:(h + 1) * tile, :] = qf[r * tile:(r + 1) * tile, h * HEAD_DIM:(h + 1) * HEAD_DIM].astype(BF16)

    loads[2].wait()
    loads[3].wait()
    for i in (0, 1):
        pl.when(y == 0)(lambda: send(kv.at[cp, i], kv.at[cp, i], kv_sem, kv_recv.at[cp, i], to_y))
    for i in (0, 1):
        pl.when(c == 0)(lambda: send(kv.at[cp, i], kv.at[cp, i], kv_sem, kv_recv.at[cp, i], to_core))
    project_q(0, bq_own)
    loads[4].wait()
    for r in range(4):
        row = jnp.broadcast_to(seg[cp, :, r * tile:(r + 1) * tile], (tile, tile))
        segcol[r] = row.T

    g_1, g_2 = 2 - z // 2, 3 - 3 * (z // 2)
    tile_rows = lambda r: pl.ds(pl.multiple_of(r * tile, tile), tile)
    every = pl.ds(0, tok)

    def scores(q, k_blk, mask):
        keys = k_blk.shape[0]
        s = lax.dot_general(q, k_blk, (((1,), (1,)), ((), ())), preferred_element_type=F32) * SCORE_SCALE
        return jnp.where(mask[None], s.reshape(heads, tile, keys), -jnp.inf).reshape(heads * tile, keys)

    @scoped
    def attend_own(t, carry):
        r = t % 4
        k_pos = lax.broadcasted_iota(jnp.int32, (tile, tok), 1)
        q_pos = lax.broadcasted_iota(jnp.int32, (tile, tok), 0) + r * tile
        s = scores(q_s[t], kv[cp, 0], (seg[cp] == segcol[r][:, :1]) & (k_pos <= q_pos))
        m_new = jnp.max(s, axis=-1, keepdims=True)
        p = jnp.exp2(s - m_new)
        m_s[r] = jnp.broadcast_to(m_new, m_s.shape[1:])
        l_s[r] = jnp.broadcast_to(jnp.sum(p, axis=-1, keepdims=True), l_s.shape[1:])
        acc_s[r] = jnp.dot(p.astype(BF16), kv[cp, 1], preferred_element_type=F32)
        return carry

    def attend_block(t, j):
        r = t % 4
        s = scores(q_s[t], kv[j, 0], seg[j] == segcol[r][:, :1])
        m_prev = m_s[r]
        m_new = jnp.maximum(m_prev, jnp.max(s, axis=-1, keepdims=True))
        p = jnp.exp2(s - m_new[:, :1])
        alpha = jnp.exp2(m_prev - m_new)
        m_s[r] = m_new
        l_s[r] = l_s[r] * alpha + jnp.sum(p, axis=-1, keepdims=True)
        acc_s[r] = acc_s[r] * alpha + jnp.dot(p.astype(BF16), kv[j, 1], preferred_element_type=F32)

    def attend_end(t, g):
        r = t % 4
        for h in range(heads):
            at = slice(h * tile, (h + 1) * tile)
            o_all[g, tile_rows(r), h * HEAD_DIM:(h + 1) * HEAD_DIM] = (acc_s[r, at, :] / l_s[r, at, :]).astype(BF16)

    def send_heads(t, g):
        o_tile = o_all.at[g, tile_rows(t % 4), :]
        pl.when(middle)(lambda: send(o_tile, o_tile, line_sem, o_recv.at[t], {'tp': 3 - z}))

    @scoped
    def heads_event(u):
        o_tile = o_all.at[g_1 if u < 4 else g_2, tile_rows(u % 4), :]
        arrived(o_tile, o_recv.at[u])
        for to, cond in ((0, z == 1), (3, z == 2)):
            pl.when(cond)(lambda: send(o_tile, o_tile, line_sem, o_recv.at[u], {'tp': to}))

    def heads_here(*tiles):
        on(middle, *((heads_event, u) for u in tiles))

    def on(cond, *todo):
        @pl.when(cond)
        def _():
            for what, *about in todo:
                what(*about)

    n_col = min(512, d_model)

    def project(g, rows, use):
        def cols(n, carry):
            at = pl.ds(pl.multiple_of(n * n_col, n_col), n_col)
            use(rows, at, jnp.dot(o_all[g, rows, :], wo[pl.ds(pl.multiple_of(g * width, width), width), at],
                                  preferred_element_type=F32).astype(BF16))
            return carry

        lax.fori_loop(0, d_model // n_col, cols, 0)

    @scoped
    def project_o(g):
        def keep(rows, at, fresh):
            part[g % 2, rows, at] = fresh

        project(g, every, keep)

    @scoped
    def project_third(g):
        def add(rows, at, fresh):
            pair_sum = part[(3 - g) % 2, rows, at].astype(F32) + fresh.astype(F32)
            run_s[rows, at] = hid[rows, at].astype(F32) + bo_ref[at].astype(F32) + pair_sum

        project(g, every, add)

    @scoped
    def project_last(g, rows):
        def add(rows, at, fresh):
            y_ref[rows, at] = (run_s[rows, at] + (part[(3 - g) % 2, rows, at].astype(F32) + fresh.astype(F32))).astype(BF16)

        project(g, rows, add)

    @scoped
    def kv_pass(i):
        @pl.when(y == 1)
        def _():
            arrived(kv.at[c, i], kv_recv.at[c, i])
            send(kv.at[c, i], kv.at[c, i], kv_sem, kv_recv.at[c, i], to_core)

    def own_block(t, carry):
        attend_own(t, carry)
        on(t == 0, (ev, 'q', 'zs', 0))
        on(t == 3, (kv_pass, 0))
        return carry

    lax.fori_loop(0, 4, own_block, 0)

    @pl.when(c == 1)
    def _():
        arrived(seg.at[cp - 1], seg_recv.at[cp - 1])
        for i in (0, 1):
            arrived(kv.at[cp - 1, i], kv_recv.at[cp - 1, i])

    def first_block(t, carry):
        pl.when(c == 1)(lambda: attend_block(t, cp - 1))
        on(t == 0, (ev, 'q', 'zs', 1))
        on(t == 1, (kv_pass, 1))
        on((t == 2) & middle, (ev, 'a', 'z', 0))
        on((t == 3) & middle, (ev, 'a', 'z', 1))
        on(t == 3, (ev, 'q', 'x', 0))
        on((t == 3) & middle, (ev, 'a', 's', 0))
        return carry

    lax.fori_loop(0, 4, first_block, 0)
    pl.when(y == 1)(lambda: arrived(seg.at[c], seg_recv.at[c]))

    def second_block(t, carry):
        pl.when(y == 1)(lambda: attend_block(t, c))
        on(t == 1, (ev, 'q', 'y', 0))
        on((t == 2) & middle, (ev, 'b', 'z', 0))
        on((t == 2) & edge, (ev, 'a', 'zs', 0))
        on(t == 3, (ev, 'q', 'x', 1))
        return carry

    lax.fori_loop(0, 4, second_block, 0)

    @pl.when(y == 1)
    def _():
        arrived(seg.at[1 - c], seg_recv.at[1 - c])
        for i in (0, 1):
            arrived(kv.at[1 - c, i], kv_recv.at[1 - c, i])

    def third_block(t, carry):
        pl.when(y == 1)(lambda: attend_block(t, 1 - c))
        attend_end(t, z)
        send_heads(t, z)
        on((t == 0) & middle, (ev, 'b', 'z', 1))
        on(t == 1, (ev, 'q', 'y', 1))
        on((t == 1) & middle, (ev, 'a', 's', 1))
        on((t == 2) & middle, (ev, 'b', 's', 0))
        on((t == 2) & edge, (ev, 'a', 'zs', 1))
        return carry

    lax.fori_loop(0, 4, third_block, 0)
    on(edge, (ev, 'b', 'zs', 0))
    on(middle, (ev, 'b', 's', 1), (ev, 'c', 'z', 0))
    ev('q', 'd', 0)
    loads[5].wait()
    project_o(z)
    ev('a', 'xy', 0)
    on(edge, (ev, 'b', 'zs', 1))
    on(middle, (ev, 'c', 'z', 1))
    ev('q', 'd', 1)
    whole('q')
    arrived(bq_pair, bq_recv)
    project_q(1, bq_pair)
    ev('a', 'xy', 1)
    on(middle, (ev, 'c', 's', 0), (heads_event, 0))
    on(edge, (ev, 'c', 'zs', 0))

    def pair_heads(t, carry):
        attend_own(t, carry)
        on((t == 4) & middle, (ev, 'c', 's', 1), (heads_event, 1))
        on(t == 5, (ev, 'b', 'xy', 0))
        on(t == 6, (ev, 'b', 'xy', 1))

        def block(j, inner):
            attend_block(t, j)
            return inner

        lax.fori_loop(0, cp, block, 0)
        attend_end(t, pair)
        send_heads(t, pair)
        on((t == 4) & edge, (ev, 'c', 'zs', 1))
        on((t == 4) & middle, (heads_event, 2))
        on(t == 4, (ev, 'a', 'd', 0))
        on((t == 5) & middle, (heads_event, 3))
        on(t == 5, (ev, 'a', 'd', 1))
        on((t == 6) & middle, (heads_event, 4))
        on(t == 6, (ev, 'c', 'xy', 0))
        on((t == 7) & middle, (heads_event, 5))
        on(t == 7, (ev, 'c', 'xy', 1))
        return carry

    lax.fori_loop(4, 8, pair_heads, 0)
    heads_here(6)
    ev('b', 'd')
    heads_here(7)
    whole('a')
    whole('b')
    project_o(pair)
    on(edge, *((heads_event, u) for u in range(4)))
    loads[9].wait()
    project_third(g_1)
    ev('c', 'd')
    whole('c')

    pl.when(middle)(lambda: project_last(g_2, every))

    def last(r, carry):
        arrived(o_all.at[g_2, tile_rows(r), :], o_recv.at[4 + r])
        project_last(g_2, tile_rows(r))
        return carry

    @pl.when(edge)
    def _():
        lax.fori_loop(0, 4, last, 0)

    with jax.named_scope('drain'):
        unit = o_rows // 2

        def sent(count, sems):
            arrived(wo.at[pl.ds(0, count * unit), :], sems)

        sent(58, spread_sem)
        pl.when(edge)(lambda: sent(2, line_sem))
        pl.when(middle)(lambda: sent(26, line_sem))
        for j in (0, 1):
            pl.when(c == j)(lambda: arrived(kv.at[pl.ds(0, 2 - j)], kv_sem))
        arrived(bq_pair, small_sem.at[0])
        for step in (1, 2, 3):
            pl.when(cp + step < 4)(lambda: arrived(seg.at[cp], small_sem.at[step]))


def write_out(y_in, k_in, v_in, y_out, k_out, v_out, sems):
    copies = [pltpu.make_async_copy(a, b, sems.at[i]) for i, (a, b) in enumerate(((y_in, y_out), (k_in, k_out), (v_in, v_out)))]
    for copy in copies:
        copy.start()
    for copy in copies:
        copy.wait()


def solution(mesh):
    def local_block(hidden, seg_ids, w_q, b_q, w_kv, b_kv, w_o, b_o, ln_gain, ln_bias):
        tok, d_model = hidden.shape
        width = w_q.shape[1]
        heads = width // HEAD_DIM
        tile = tok // 4
        hbm = pl.BlockSpec(memory_space=pltpu.HBM)
        vmem = pl.BlockSpec(memory_space=pltpu.VMEM)
        dma = pltpu.SemaphoreType.DMA
        far = lambda a: pltpu.with_memory_space_constraint(a, pltpu.HBM)
        outs = pl.pallas_call(
            kernel,
            out_shape=(jax.ShapeDtypeStruct((tok, d_model), BF16), jax.ShapeDtypeStruct((tok, HEAD_DIM), BF16),
                       jax.ShapeDtypeStruct((tok, HEAD_DIM), BF16)),
            in_specs=[hbm] * 10,
            out_specs=(vmem, vmem, vmem),
            scratch_shapes=[
                pltpu.VMEM((tok, d_model), BF16),
                pltpu.VMEM((tok, d_model), BF16),
                pltpu.VMEM((d_model, 2 * HEAD_DIM), BF16),
                pltpu.VMEM((2, d_model, width), BF16),
                pltpu.VMEM((4 * width, d_model), BF16),
                pltpu.VMEM((width,), BF16),
                pltpu.VMEM((width,), BF16),
                pltpu.VMEM((2 * HEAD_DIM,), BF16),
                pltpu.VMEM((d_model,), BF16),
                pltpu.VMEM((d_model,), BF16),
                pltpu.VMEM((d_model,), BF16),
                pltpu.VMEM((4, 1, tok), jnp.int32),
                pltpu.VMEM((4, tile, tile), jnp.int32),
                pltpu.VMEM((4, 2, tok, HEAD_DIM), BF16),
                pltpu.VMEM((8, heads * tile, HEAD_DIM), BF16),
                pltpu.VMEM((4, tok, width), BF16),
                pltpu.VMEM((2, tok, d_model), BF16),
                pltpu.VMEM((tok, d_model), F32),
                pltpu.VMEM((4, heads * tile, HEAD_DIM), F32),
                pltpu.VMEM((4, heads * tile, HEAD_DIM), F32),
                pltpu.VMEM((4, heads * tile, HEAD_DIM), F32),
                dma((10,)), dma(()), dma(()), dma(()), dma((4,)), dma(()), dma((4,)), dma((4, 2)), dma((9,)), dma((4, 9)), dma((8,)),
            ],
            compiler_params=pltpu.CompilerParams(collective_id=0, has_side_effects=True, vmem_limit_bytes=48 * 2 ** 20),
            name='block',
        )(far(hidden), far(seg_ids.reshape(1, -1)), far(w_q), far(b_q), far(w_kv), far(b_kv), far(w_o), far(b_o), far(ln_gain), far(ln_bias))
        near = lambda a: pltpu.with_memory_space_constraint(a, pltpu.VMEM)
        return pl.pallas_call(
            write_out,
            out_shape=tuple(jax.ShapeDtypeStruct(a.shape, a.dtype) for a in outs),
            in_specs=[vmem] * 3,
            out_specs=(pl.BlockSpec(memory_space=pl.ANY),) * 3,
            scratch_shapes=[dma((3,))],
            name='write',
        )(*map(near, outs))

    row_spec = P(('dp', 'cp'), None)
    tok_spec = P(('dp', 'cp'))
    return jax.shard_map(local_block, mesh=mesh,
                         in_specs=(row_spec, tok_spec, P(None, 'tp'), P('tp'), P(None, None), P(None), P('tp', None), P(None), P(None), P(None)),
                         out_specs=(row_spec, row_spec, row_spec), check_vma=False)
```

```python
import functools
import jax
import jax.numpy as jnp
from jax import lax
from jax.experimental import pallas as pl
from jax.experimental.pallas import tpu as pltpu
from jax.sharding import PartitionSpec as P

HEAD_DIM = 128
LN_EPS = 1e-5
SCORE_SCALE = HEAD_DIM ** -0.5 * 1.4426950408889634
MESH = pl.DeviceIdType.MESH
BF16 = jnp.bfloat16
F32 = jnp.float32


def send(src, dst, sent, recv, to):
    pltpu.make_async_remote_copy(src_ref=src, dst_ref=dst, send_sem=sent, recv_sem=recv, device_id=to, device_id_type=MESH).start()


def scoped(fn):
    def run(*about):
        with jax.named_scope(fn.__name__ + '_'.join(str(a) for a in about if isinstance(a, (str, int)))):
            return fn(*about)
    return run


def arrived(dst, recv):
    pltpu.make_async_copy(dst, dst, recv).wait()


def kernel(hid_hbm, seg_hbm, wq_hbm, bq_hbm, wkv_hbm, bkv_hbm, wo_hbm, bo_hbm, gain_hbm, lnb_hbm,
           y_ref, k_ref, v_ref,
           hid, normed, wkv, wq, wo, bq_own, bq_pair, bkv_ref, bo_ref, gain_ref, lnb_ref, seg, segcol, kv, q_s, o_all, part, run_s, m_s, l_s, acc_s,
           load_sem, spread_sem, line_sem, kv_sem, small_sem, bq_recv, seg_recv, kv_recv, wq_recv, wo_recv, o_recv):
    tok, d_model = hid.shape
    width = wq.shape[2]
    heads = width // HEAD_DIM
    tile = tok // 4
    q_rows, o_rows = d_model // 8, width // 8
    dp, z, cp = lax.axis_index('dp'), lax.axis_index('tp'), lax.axis_index('cp')
    y, c = cp // 2, cp % 2
    pair = z + 1 - 2 * (z % 2)
    below, above = {'tp': z - 1}, {'tp': z + 1}
    to_x, to_y, to_core = {'dp': 1 - dp}, {'cp': cp + 2 - 4 * y}, {'cp': cp + 1 - 2 * c}
    pos = lambda px, py, pc: px * 4 + py * 2 + pc
    p_me, p_x, p_y, p_d = pos(dp, y, c), pos(1 - dp, y, c), pos(dp, 1 - y, c), pos(1 - dp, 1 - y, c)
    g_a = 1 + z % 2
    g_c = 3 - 3 * (z // 2)
    g_b = 6 - z - g_a - g_c

    loads = [pltpu.make_async_copy(hid_hbm, hid, load_sem.at[0]),
             pltpu.make_async_copy(wkv_hbm, wkv, load_sem.at[1]),
             pltpu.make_async_copy(wq_hbm, wq.at[0], load_sem.at[2]),
             pltpu.make_async_copy(bq_hbm, bq_own, load_sem.at[3]),
             pltpu.make_async_copy(seg_hbm, seg.at[cp], load_sem.at[4]),
             pltpu.make_async_copy(wo_hbm, wo.at[pl.ds(z * width, width), :], load_sem.at[5]),
             pltpu.make_async_copy(gain_hbm, gain_ref, load_sem.at[6]),
             pltpu.make_async_copy(lnb_hbm, lnb_ref, load_sem.at[7]),
             pltpu.make_async_copy(bkv_hbm, bkv_ref, load_sem.at[8]),
             pltpu.make_async_copy(bo_hbm, bo_ref, load_sem.at[9])]
    for i in (0, 6, 7, 8, 3, 4, 9):
        loads[i].start()

    barrier = pltpu.get_barrier_semaphore()
    for step in (1, 2, 3):
        pl.semaphore_signal(barrier, inc=1, device_id={'cp': (cp + step) % 4}, device_id_type=MESH)
    pl.semaphore_signal(barrier, inc=1, device_id=to_x, device_id_type=MESH)

    @pl.when(z > 0)
    def _():
        pl.semaphore_signal(barrier, inc=1, device_id={'tp': z - 1}, device_id_type=MESH)

    @pl.when(z < 3)
    def _():
        pl.semaphore_signal(barrier, inc=1, device_id={'tp': z + 1}, device_id_type=MESH)

    loads[1].start()
    with jax.named_scope('barr'):
        pl.semaphore_wait(barrier, 5 + (z + 1) // 2 - 2 * (z // 3))

    loads[2].start()
    def q_piece(p, h):
        half = q_rows // 2
        return wq.at[1, pl.ds(pl.multiple_of(p * q_rows + h * half, half), half), :]

    def o_piece(g, p, h):
        half = o_rows // 2
        return wo.at[pl.ds(pl.multiple_of(g * width + p * o_rows + h * half, half), half), :]

    def sem(g, kind, h):
        at = {'z': 0, 'x': 2, 'y': 4, 'd': 6, 'core': 8}[kind] + (0 if kind == 'core' else h)
        return wq_recv.at[at] if g is None else wo_recv.at[g, at]

    middle, edge = (z > 0) & (z < 3), (z == 0) | (z == 3)

    send(bq_hbm, bq_pair, small_sem.at[0], bq_recv, {'tp': pair})
    for h in (0, 1):
        half = q_rows // 2
        send(wq_hbm.at[pl.ds(pl.multiple_of(p_me * q_rows + h * half, half), half), :], q_piece(p_me, h), spread_sem, sem(None, 'z', h),
             {'tp': pair})
    for h in (0, 1):
        half = o_rows // 2
        for to, cond in ((below, z > 0), (above, z < 3)):
            @pl.when(cond)
            def _():
                send(wo_hbm.at[pl.ds(pl.multiple_of(p_me * o_rows + h * half, half), half), :], o_piece(z, p_me, h), line_sem,
                     sem(z, 'z', h), to)
    for step in (1, 2, 3):
        pl.when(cp + step < 4)(lambda: send(seg_hbm, seg.at[cp], small_sem.at[step], seg_recv.at[cp], {'cp': cp + step}))

    def pass_on(g, source, h, by_x):
        p = {'z': p_me, 's': p_me, 'x': p_x, 'y': p_y, 'd': p_d}[source]
        piece = q_piece(p, h) if g is None else o_piece(g, p, h)
        if source == 's':
            send(piece, piece, spread_sem, sem(g, 'x', h), to_x)
            send(piece, piece, spread_sem, sem(g, 'y', h), to_y)
            return
        arrived(piece, sem(g, source, h))
        if source == 'z' and g is not None:
            pl.when((g > z) & (z > 0))(lambda: send(piece, piece, line_sem, sem(g, 'z', h), below))
            pl.when((g < z) & (z < 3))(lambda: send(piece, piece, line_sem, sem(g, 'z', h), above))
        elif source == 'x':
            if not by_x:
                pl.when(c == 1)(lambda: send(piece, piece, spread_sem, sem(g, 'd', h), to_y))
        elif source == 'y':
            pl.when((c == 0) | by_x)(lambda: send(piece, piece, spread_sem, sem(g, 'd', h), to_x))
        send(piece, piece, spread_sem, sem(g, 'core', h), to_core)

    groups = {'q': None, 'a': g_a, 'b': g_b, 'c': g_c}

    @scoped
    def ev(name, sources, *halves):
        for h in halves or (0, 1):
            for source in sources:
                pass_on(groups[name], source, h, name == 'q')

    @scoped
    def whole(name):
        if name == 'q':
            arrived(wq.at[1, pl.ds(0, 4 * q_rows), :], sem(None, 'core', 0))
        else:
            arrived(wo.at[pl.ds(0, 4 * o_rows), :], sem(groups[name], 'core', 0))

    loads[5].start()

    with jax.named_scope('load_wait'):
        for i in (0, 6, 7):
            loads[i].wait()
    gain = gain_ref[...].astype(F32)
    lnb = lnb_ref[...].astype(F32)
    ln_rows = min(64, tok)

    def ln_step(i, carry):
        rows = pl.ds(pl.multiple_of(i * ln_rows, ln_rows), ln_rows)
        x = hid[rows, :].astype(F32)
        cen = x - jnp.mean(x, axis=-1, keepdims=True)
        var = jnp.mean(cen * cen, axis=-1, keepdims=True)
        normed[rows, :] = (cen * lax.rsqrt(var + LN_EPS) * gain + lnb).astype(BF16)
        return carry

    with jax.named_scope('ln'):
        lax.fori_loop(0, tok // ln_rows, ln_step, 0)

    loads[1].wait()
    loads[8].wait()
    kv_new = (jnp.dot(normed[...], wkv[...], preferred_element_type=F32) + bkv_ref[...].astype(F32)).astype(BF16)
    kv[cp, 0] = kv_new[:, :HEAD_DIM]
    kv[cp, 1] = kv_new[:, HEAD_DIM:]
    k_ref[...] = kv_new[:, :HEAD_DIM]
    v_ref[...] = kv_new[:, HEAD_DIM:]

    @scoped
    def project_q(which, bias):
        qf = jnp.dot(normed[...], wq[which], preferred_element_type=F32) + bias[...].astype(F32)
        for r in range(4):
            for h in range(heads):
                q_s[which * 4 + r, h * tile:(h + 1) * tile, :] = qf[r * tile:(r + 1) * tile, h * HEAD_DIM:(h + 1) * HEAD_DIM].astype(BF16)

    loads[2].wait()
    loads[3].wait()
    for i in (0, 1):
        pl.when(y == 0)(lambda: send(kv.at[cp, i], kv.at[cp, i], kv_sem, kv_recv.at[cp, i], to_y))
    for i in (0, 1):
        pl.when(c == 0)(lambda: send(kv.at[cp, i], kv.at[cp, i], kv_sem, kv_recv.at[cp, i], to_core))
    project_q(0, bq_own)
    loads[4].wait()
    for r in range(4):
        row = jnp.broadcast_to(seg[cp, :, r * tile:(r + 1) * tile], (tile, tile))
        segcol[r] = row.T

    g_1, g_2 = 2 - z // 2, 3 - 3 * (z // 2)
    tile_rows = lambda r: pl.ds(pl.multiple_of(r * tile, tile), tile)
    every = pl.ds(0, tok)

    def scores(q, k_blk, mask):
        keys = k_blk.shape[0]
        s = lax.dot_general(q, k_blk, (((1,), (1,)), ((), ())), preferred_element_type=F32) * SCORE_SCALE
        return jnp.where(mask[None], s.reshape(heads, tile, keys), -jnp.inf).reshape(heads * tile, keys)

    @scoped
    def attend_own(t, carry):
        r = t % 4
        k_pos = lax.broadcasted_iota(jnp.int32, (tile, tok), 1)
        q_pos = lax.broadcasted_iota(jnp.int32, (tile, tok), 0) + r * tile
        s = scores(q_s[t], kv[cp, 0], (seg[cp] == segcol[r][:, :1]) & (k_pos <= q_pos))
        m_new = jnp.max(s, axis=-1, keepdims=True)
        p = jnp.exp2(s - m_new)
        m_s[r] = jnp.broadcast_to(m_new, m_s.shape[1:])
        l_s[r] = jnp.broadcast_to(jnp.sum(p, axis=-1, keepdims=True), l_s.shape[1:])
        acc_s[r] = jnp.dot(p.astype(BF16), kv[cp, 1], preferred_element_type=F32)
        return carry

    def attend_block(t, j):
        r = t % 4
        s = scores(q_s[t], kv[j, 0], seg[j] == segcol[r][:, :1])
        m_prev = m_s[r]
        m_new = jnp.maximum(m_prev, jnp.max(s, axis=-1, keepdims=True))
        p = jnp.exp2(s - m_new[:, :1])
        alpha = jnp.exp2(m_prev - m_new)
        m_s[r] = m_new
        l_s[r] = l_s[r] * alpha + jnp.sum(p, axis=-1, keepdims=True)
        acc_s[r] = acc_s[r] * alpha + jnp.dot(p.astype(BF16), kv[j, 1], preferred_element_type=F32)

    def attend_end(t, g):
        r = t % 4
        for h in range(heads):
            at = slice(h * tile, (h + 1) * tile)
            o_all[g, tile_rows(r), h * HEAD_DIM:(h + 1) * HEAD_DIM] = (acc_s[r, at, :] / l_s[r, at, :]).astype(BF16)

    def send_heads(t, g):
        o_tile = o_all.at[g, tile_rows(t % 4), :]
        pl.when(middle)(lambda: send(o_tile, o_tile, line_sem, o_recv.at[t], {'tp': 3 - z}))

    @scoped
    def heads_event(u):
        o_tile = o_all.at[g_1 if u < 4 else g_2, tile_rows(u % 4), :]
        arrived(o_tile, o_recv.at[u])
        for to, cond in ((0, z == 1), (3, z == 2)):
            pl.when(cond)(lambda: send(o_tile, o_tile, line_sem, o_recv.at[u], {'tp': to}))

    def heads_here(*tiles):
        on(middle, *((heads_event, u) for u in tiles))

    def on(cond, *todo):
        @pl.when(cond)
        def _():
            for what, *about in todo:
                what(*about)

    n_col = min(512, d_model)

    def project(g, rows, use):
        def cols(n, carry):
            at = pl.ds(pl.multiple_of(n * n_col, n_col), n_col)
            use(rows, at, jnp.dot(o_all[g, rows, :], wo[pl.ds(pl.multiple_of(g * width, width), width), at],
                                  preferred_element_type=F32).astype(BF16))
            return carry

        lax.fori_loop(0, d_model // n_col, cols, 0)

    @scoped
    def project_o(g):
        def keep(rows, at, fresh):
            part[g % 2, rows, at] = fresh

        project(g, every, keep)

    @scoped
    def project_third(g):
        def add(rows, at, fresh):
            pair_sum = part[(3 - g) % 2, rows, at].astype(F32) + fresh.astype(F32)
            run_s[rows, at] = hid[rows, at].astype(F32) + bo_ref[at].astype(F32) + pair_sum

        project(g, every, add)

    @scoped
    def project_last(g, rows):
        def add(rows, at, fresh):
            y_ref[rows, at] = (run_s[rows, at] + (part[(3 - g) % 2, rows, at].astype(F32) + fresh.astype(F32))).astype(BF16)

        project(g, rows, add)

    @scoped
    def kv_pass(i):
        @pl.when(y == 1)
        def _():
            arrived(kv.at[c, i], kv_recv.at[c, i])
            send(kv.at[c, i], kv.at[c, i], kv_sem, kv_recv.at[c, i], to_core)

    def own_block(t, carry):
        attend_own(t, carry)
        on(t == 0, (ev, 'q', 'zs', 0))
        on(t == 3, (kv_pass, 0))
        return carry

    lax.fori_loop(0, 4, own_block, 0)

    @pl.when(c == 1)
    def _():
        arrived(seg.at[cp - 1], seg_recv.at[cp - 1])
        for i in (0, 1):
            arrived(kv.at[cp - 1, i], kv_recv.at[cp - 1, i])

    def first_block(t, carry):
        pl.when(c == 1)(lambda: attend_block(t, cp - 1))
        on(t == 0, (ev, 'q', 'zs', 1))
        on(t == 1, (kv_pass, 1))
        on((t == 2) & middle, (ev, 'a', 'z', 0))
        on((t == 3) & middle, (ev, 'a', 'z', 1))
        on(t == 3, (ev, 'q', 'x', 0))
        on((t == 3) & middle, (ev, 'a', 's', 0))
        return carry

    lax.fori_loop(0, 4, first_block, 0)
    pl.when(y == 1)(lambda: arrived(seg.at[c], seg_recv.at[c]))

    def second_block(t, carry):
        pl.when(y == 1)(lambda: attend_block(t, c))
        on(t == 1, (ev, 'q', 'y', 0))
        on((t == 2) & middle, (ev, 'b', 'z', 0))
        on((t == 2) & edge, (ev, 'a', 'zs', 0))
        on(t == 3, (ev, 'q', 'x', 1))
        return carry

    lax.fori_loop(0, 4, second_block, 0)

    @pl.when(y == 1)
    def _():
        arrived(seg.at[1 - c], seg_recv.at[1 - c])
        for i in (0, 1):
            arrived(kv.at[1 - c, i], kv_recv.at[1 - c, i])

    def third_block(t, carry):
        pl.when(y == 1)(lambda: attend_block(t, 1 - c))
        attend_end(t, z)
        send_heads(t, z)
        on((t == 0) & middle, (ev, 'b', 'z', 1))
        on(t == 1, (ev, 'q', 'y', 1))
        on((t == 1) & middle, (ev, 'a', 's', 1))
        on((t == 2) & middle, (ev, 'b', 's', 0))
        on((t == 2) & edge, (ev, 'a', 'zs', 1))
        return carry

    lax.fori_loop(0, 4, third_block, 0)
    on(edge, (ev, 'b', 'zs', 0))
    on(middle, (ev, 'b', 's', 1), (ev, 'c', 'z', 0))
    ev('q', 'd', 0)
    loads[5].wait()
    project_o(z)
    ev('a', 'xy', 0)
    on(edge, (ev, 'b', 'zs', 1))
    ev('q', 'd', 1)
    whole('q')
    arrived(bq_pair, bq_recv)
    project_q(1, bq_pair)
    on(middle, (ev, 'c', 'z', 1), (ev, 'c', 's', 0))
    ev('a', 'xy', 1)
    heads_here(0)
    on(edge, (ev, 'c', 'zs', 0))

    def pair_heads(t, carry):
        attend_own(t, carry)
        on((t == 4) & middle, (ev, 'c', 's', 1), (heads_event, 1))
        on(t == 5, (ev, 'b', 'xy', 0))
        on(t == 6, (ev, 'b', 'xy', 1))
        on((t == 6) & middle, (heads_event, 4))
        on((t == 7) & middle, (heads_event, 5))

        def block(j, inner):
            attend_block(t, j)
            return inner

        lax.fori_loop(0, cp, block, 0)
        attend_end(t, pair)
        send_heads(t, pair)
        on((t == 4) & edge, (ev, 'c', 'zs', 1))
        on((t == 4) & middle, (heads_event, 2))
        on(t == 4, (ev, 'a', 'd', 0))
        on((t == 5) & middle, (heads_event, 3))
        on(t == 5, (ev, 'a', 'd', 1))
        on(t == 6, (ev, 'c', 'xy', 0))
        on(t == 7, (ev, 'c', 'xy', 1))
        return carry

    lax.fori_loop(4, 8, pair_heads, 0)
    heads_here(6)
    ev('b', 'd')
    heads_here(7)
    whole('a')
    whole('b')
    ev('c', 'd', 0)
    project_o(pair)
    ev('c', 'd', 1)
    on(edge, *((heads_event, u) for u in range(4)))
    loads[9].wait()
    project_third(g_1)
    whole('c')

    pl.when(middle)(lambda: project_last(g_2, every))

    def last(r, carry):
        arrived(o_all.at[g_2, tile_rows(r), :], o_recv.at[4 + r])
        project_last(g_2, tile_rows(r))
        return carry

    @pl.when(edge)
    def _():
        lax.fori_loop(0, 4, last, 0)

    with jax.named_scope('drain'):
        unit = o_rows // 2

        def sent(count, sems):
            arrived(wo.at[pl.ds(0, count * unit), :], sems)

        sent(58, spread_sem)
        pl.when(edge)(lambda: sent(2, line_sem))
        pl.when(middle)(lambda: sent(26, line_sem))
        for j in (0, 1):
            pl.when(c == j)(lambda: arrived(kv.at[pl.ds(0, 2 - j)], kv_sem))
        arrived(bq_pair, small_sem.at[0])
        for step in (1, 2, 3):
            pl.when(cp + step < 4)(lambda: arrived(seg.at[cp], small_sem.at[step]))


def write_out(y_in, k_in, v_in, y_out, k_out, v_out, sems):
    copies = [pltpu.make_async_copy(a, b, sems.at[i]) for i, (a, b) in enumerate(((y_in, y_out), (k_in, k_out), (v_in, v_out)))]
    for copy in copies:
        copy.start()
    for copy in copies:
        copy.wait()


def solution(mesh):
    def local_block(hidden, seg_ids, w_q, b_q, w_kv, b_kv, w_o, b_o, ln_gain, ln_bias):
        tok, d_model = hidden.shape
        width = w_q.shape[1]
        heads = width // HEAD_DIM
        tile = tok // 4
        hbm = pl.BlockSpec(memory_space=pltpu.HBM)
        vmem = pl.BlockSpec(memory_space=pltpu.VMEM)
        dma = pltpu.SemaphoreType.DMA
        far = lambda a: pltpu.with_memory_space_constraint(a, pltpu.HBM)
        outs = pl.pallas_call(
            kernel,
            out_shape=(jax.ShapeDtypeStruct((tok, d_model), BF16), jax.ShapeDtypeStruct((tok, HEAD_DIM), BF16),
                       jax.ShapeDtypeStruct((tok, HEAD_DIM), BF16)),
            in_specs=[hbm] * 10,
            out_specs=(vmem, vmem, vmem),
            scratch_shapes=[
                pltpu.VMEM((tok, d_model), BF16),
                pltpu.VMEM((tok, d_model), BF16),
                pltpu.VMEM((d_model, 2 * HEAD_DIM), BF16),
                pltpu.VMEM((2, d_model, width), BF16),
                pltpu.VMEM((4 * width, d_model), BF16),
                pltpu.VMEM((width,), BF16),
                pltpu.VMEM((width,), BF16),
                pltpu.VMEM((2 * HEAD_DIM,), BF16),
                pltpu.VMEM((d_model,), BF16),
                pltpu.VMEM((d_model,), BF16),
                pltpu.VMEM((d_model,), BF16),
                pltpu.VMEM((4, 1, tok), jnp.int32),
                pltpu.VMEM((4, tile, tile), jnp.int32),
                pltpu.VMEM((4, 2, tok, HEAD_DIM), BF16),
                pltpu.VMEM((8, heads * tile, HEAD_DIM), BF16),
                pltpu.VMEM((4, tok, width), BF16),
                pltpu.VMEM((2, tok, d_model), BF16),
                pltpu.VMEM((tok, d_model), F32),
                pltpu.VMEM((4, heads * tile, HEAD_DIM), F32),
                pltpu.VMEM((4, heads * tile, HEAD_DIM), F32),
                pltpu.VMEM((4, heads * tile, HEAD_DIM), F32),
                dma((10,)), dma(()), dma(()), dma(()), dma((4,)), dma(()), dma((4,)), dma((4, 2)), dma((9,)), dma((4, 9)), dma((8,)),
            ],
            compiler_params=pltpu.CompilerParams(collective_id=0, has_side_effects=True, vmem_limit_bytes=48 * 2 ** 20),
            name='block',
        )(far(hidden), far(seg_ids.reshape(1, -1)), far(w_q), far(b_q), far(w_kv), far(b_kv), far(w_o), far(b_o), far(ln_gain), far(ln_bias))
        near = lambda a: pltpu.with_memory_space_constraint(a, pltpu.VMEM)
        return pl.pallas_call(
            write_out,
            out_shape=tuple(jax.ShapeDtypeStruct(a.shape, a.dtype) for a in outs),
            in_specs=[vmem] * 3,
            out_specs=(pl.BlockSpec(memory_space=pl.ANY),) * 3,
            scratch_shapes=[dma((3,))],
            name='write',
        )(*map(near, outs))

    row_spec = P(('dp', 'cp'), None)
    tok_spec = P(('dp', 'cp'))
    return jax.shard_map(local_block, mesh=mesh,
                         in_specs=(row_spec, tok_spec, P(None, 'tp'), P('tp'), P(None, None), P(None), P('tp', None), P(None), P(None), P(None)),
                         out_specs=(row_spec, row_spec, row_spec), check_vma=False)
```

```python
import functools
import jax
import jax.numpy as jnp
from jax import lax
from jax.experimental import pallas as pl
from jax.experimental.pallas import tpu as pltpu
from jax.sharding import PartitionSpec as P

HEAD_DIM = 128
LN_EPS = 1e-5
SCORE_SCALE = HEAD_DIM ** -0.5 * 1.4426950408889634
MESH = pl.DeviceIdType.MESH
BF16 = jnp.bfloat16
F32 = jnp.float32


def send(src, dst, sent, recv, to):
    pltpu.make_async_remote_copy(src_ref=src, dst_ref=dst, send_sem=sent, recv_sem=recv, device_id=to, device_id_type=MESH).start()


def scoped(fn):
    def run(*about):
        with jax.named_scope(fn.__name__ + '_'.join(str(a) for a in about if isinstance(a, (str, int)))):
            return fn(*about)
    return run


def arrived(dst, recv):
    pltpu.make_async_copy(dst, dst, recv).wait()


def kernel(hid_hbm, seg_hbm, wq_hbm, bq_hbm, wkv_hbm, bkv_hbm, wo_hbm, bo_hbm, gain_hbm, lnb_hbm,
           y_ref, k_ref, v_ref,
           hid, normed, wkv, wq, wo, bq_own, bq_pair, bkv_ref, bo_ref, gain_ref, lnb_ref, seg, segcol, kv, q_s, o_all, part, run_s, m_s, l_s, acc_s,
           load_sem, spread_sem, line_sem, kv_sem, small_sem, bq_recv, seg_recv, kv_recv, wq_recv, wo_recv, o_recv):
    tok, d_model = hid.shape
    width = wq.shape[2]
    heads = width // HEAD_DIM
    tile = tok // 4
    q_rows, o_rows = d_model // 8, width // 8
    dp, z, cp = lax.axis_index('dp'), lax.axis_index('tp'), lax.axis_index('cp')
    y, c = cp // 2, cp % 2
    pair = z + 1 - 2 * (z % 2)
    below, above = {'tp': z - 1}, {'tp': z + 1}
    to_x, to_y, to_core = {'dp': 1 - dp}, {'cp': cp + 2 - 4 * y}, {'cp': cp + 1 - 2 * c}
    pos = lambda px, py, pc: px * 4 + py * 2 + pc
    p_me, p_x, p_y, p_d = pos(dp, y, c), pos(1 - dp, y, c), pos(dp, 1 - y, c), pos(1 - dp, 1 - y, c)
    g_a = 1 + z % 2
    g_c = 3 - 3 * (z // 2)
    g_b = 6 - z - g_a - g_c

    loads = [pltpu.make_async_copy(hid_hbm, hid, load_sem.at[0]),
             pltpu.make_async_copy(wkv_hbm, wkv, load_sem.at[1]),
             pltpu.make_async_copy(wq_hbm, wq.at[0], load_sem.at[2]),
             pltpu.make_async_copy(bq_hbm, bq_own, load_sem.at[3]),
             pltpu.make_async_copy(seg_hbm, seg.at[cp], load_sem.at[4]),
             pltpu.make_async_copy(wo_hbm, wo.at[pl.ds(z * width, width), :], load_sem.at[5]),
             pltpu.make_async_copy(gain_hbm, gain_ref, load_sem.at[6]),
             pltpu.make_async_copy(lnb_hbm, lnb_ref, load_sem.at[7]),
             pltpu.make_async_copy(bkv_hbm, bkv_ref, load_sem.at[8]),
             pltpu.make_async_copy(bo_hbm, bo_ref, load_sem.at[9])]
    for i in (0, 6, 7, 8, 3, 4, 9):
        loads[i].start()

    barrier = pltpu.get_barrier_semaphore()
    for step in (1, 2, 3):
        pl.semaphore_signal(barrier, inc=1, device_id={'cp': (cp + step) % 4}, device_id_type=MESH)
    pl.semaphore_signal(barrier, inc=1, device_id=to_x, device_id_type=MESH)

    @pl.when(z > 0)
    def _():
        pl.semaphore_signal(barrier, inc=1, device_id={'tp': z - 1}, device_id_type=MESH)

    @pl.when(z < 3)
    def _():
        pl.semaphore_signal(barrier, inc=1, device_id={'tp': z + 1}, device_id_type=MESH)

    loads[1].start()
    with jax.named_scope('barr'):
        pl.semaphore_wait(barrier, 5 + (z + 1) // 2 - 2 * (z // 3))

    loads[2].start()
    def q_piece(p, h):
        half = q_rows // 2
        return wq.at[1, pl.ds(pl.multiple_of(p * q_rows + h * half, half), half), :]

    def o_piece(g, p, h):
        half = o_rows // 2
        return wo.at[pl.ds(pl.multiple_of(g * width + p * o_rows + h * half, half), half), :]

    def sem(g, kind, h):
        at = {'z': 0, 'x': 2, 'y': 4, 'd': 6, 'core': 8}[kind] + (0 if kind == 'core' else h)
        return wq_recv.at[at] if g is None else wo_recv.at[g, at]

    middle, edge = (z > 0) & (z < 3), (z == 0) | (z == 3)

    send(bq_hbm, bq_pair, small_sem.at[0], bq_recv, {'tp': pair})
    for h in (0, 1):
        half = q_rows // 2
        send(wq_hbm.at[pl.ds(pl.multiple_of(p_me * q_rows + h * half, half), half), :], q_piece(p_me, h), spread_sem, sem(None, 'z', h),
             {'tp': pair})
    for h in (0, 1):
        half = o_rows // 2
        for to, cond in ((below, z > 0), (above, z < 3)):
            @pl.when(cond)
            def _():
                send(wo_hbm.at[pl.ds(pl.multiple_of(p_me * o_rows + h * half, half), half), :], o_piece(z, p_me, h), line_sem,
                     sem(z, 'z', h), to)
    for step in (1, 2, 3):
        pl.when(cp + step < 4)(lambda: send(seg_hbm, seg.at[cp], small_sem.at[step], seg_recv.at[cp], {'cp': cp + step}))

    def pass_on(g, source, h, by_x):
        p = {'z': p_me, 's': p_me, 'x': p_x, 'y': p_y, 'd': p_d}[source]
        piece = q_piece(p, h) if g is None else o_piece(g, p, h)
        if source == 's':
            send(piece, piece, spread_sem, sem(g, 'x', h), to_x)
            send(piece, piece, spread_sem, sem(g, 'y', h), to_y)
            return
        arrived(piece, sem(g, source, h))
        if source == 'z' and g is not None:
            pl.when((g > z) & (z > 0))(lambda: send(piece, piece, line_sem, sem(g, 'z', h), below))
            pl.when((g < z) & (z < 3))(lambda: send(piece, piece, line_sem, sem(g, 'z', h), above))
        elif source == 'x':
            if not by_x:
                pl.when(c == 1)(lambda: send(piece, piece, spread_sem, sem(g, 'd', h), to_y))
        elif source == 'y':
            pl.when((c == 0) | by_x)(lambda: send(piece, piece, spread_sem, sem(g, 'd', h), to_x))
        send(piece, piece, spread_sem, sem(g, 'core', h), to_core)

    groups = {'q': None, 'a': g_a, 'b': g_b, 'c': g_c}

    @scoped
    def ev(name, sources, *halves):
        for h in halves or (0, 1):
            for source in sources:
                pass_on(groups[name], source, h, name == 'q')

    @scoped
    def whole(name):
        if name == 'q':
            arrived(wq.at[1, pl.ds(0, 4 * q_rows), :], sem(None, 'core', 0))
        else:
            arrived(wo.at[pl.ds(0, 4 * o_rows), :], sem(groups[name], 'core', 0))

    loads[5].start()

    with jax.named_scope('load_wait'):
        for i in (0, 6, 7):
            loads[i].wait()
    gain = gain_ref[...].astype(F32)
    lnb = lnb_ref[...].astype(F32)
    ln_rows = min(64, tok)

    def ln_step(i, carry):
        rows = pl.ds(pl.multiple_of(i * ln_rows, ln_rows), ln_rows)
        x = hid[rows, :].astype(F32)
        cen = x - jnp.mean(x, axis=-1, keepdims=True)
        var = jnp.mean(cen * cen, axis=-1, keepdims=True)
        normed[rows, :] = (cen * lax.rsqrt(var + LN_EPS) * gain + lnb).astype(BF16)
        return carry

    with jax.named_scope('ln'):
        lax.fori_loop(0, tok // ln_rows, ln_step, 0)

    loads[1].wait()
    loads[8].wait()
    kv_new = (jnp.dot(normed[...], wkv[...], preferred_element_type=F32) + bkv_ref[...].astype(F32)).astype(BF16)
    kv[cp, 0] = kv_new[:, :HEAD_DIM]
    kv[cp, 1] = kv_new[:, HEAD_DIM:]
    k_ref[...] = kv_new[:, :HEAD_DIM]
    v_ref[...] = kv_new[:, HEAD_DIM:]

    @scoped
    def project_q(which, bias):
        qf = jnp.dot(normed[...], wq[which], preferred_element_type=F32) + bias[...].astype(F32)
        for r in range(4):
            for h in range(heads):
                q_s[which * 4 + r, h * tile:(h + 1) * tile, :] = qf[r * tile:(r + 1) * tile, h * HEAD_DIM:(h + 1) * HEAD_DIM].astype(BF16)

    loads[2].wait()
    loads[3].wait()
    for i in (0, 1):
        pl.when(y == 0)(lambda: send(kv.at[cp, i], kv.at[cp, i], kv_sem, kv_recv.at[cp, i], to_y))
    for i in (0, 1):
        pl.when(c == 0)(lambda: send(kv.at[cp, i], kv.at[cp, i], kv_sem, kv_recv.at[cp, i], to_core))
    project_q(0, bq_own)
    loads[4].wait()
    for r in range(4):
        row = jnp.broadcast_to(seg[cp, :, r * tile:(r + 1) * tile], (tile, tile))
        segcol[r] = row.T

    g_1, g_2 = 2 - z // 2, 3 - 3 * (z // 2)
    tile_rows = lambda r: pl.ds(pl.multiple_of(r * tile, tile), tile)
    every = pl.ds(0, tok)

    def scores(q, k_blk, mask):
        keys = k_blk.shape[0]
        s = lax.dot_general(q, k_blk, (((1,), (1,)), ((), ())), preferred_element_type=F32) * SCORE_SCALE
        return jnp.where(mask[None], s.reshape(heads, tile, keys), -jnp.inf).reshape(heads * tile, keys)

    @scoped
    def attend_own(t, carry):
        r = t % 4

        def step(keys):
            k_pos = lax.broadcasted_iota(jnp.int32, (tile, keys), 1)
            q_pos = lax.broadcasted_iota(jnp.int32, (tile, keys), 0) + r * tile
            s = scores(q_s[t], kv[cp, 0, :keys, :], (seg[cp, :, :keys] == segcol[r][:, :1]) & (k_pos <= q_pos))
            m_new = jnp.max(s, axis=-1, keepdims=True)
            p = jnp.exp2(s - m_new)
            m_s[r] = jnp.broadcast_to(m_new, m_s.shape[1:])
            l_s[r] = jnp.broadcast_to(jnp.sum(p, axis=-1, keepdims=True), l_s.shape[1:])
            acc_s[r] = jnp.dot(p.astype(BF16), kv[cp, 1, :keys, :], preferred_element_type=F32)

        pl.when(r < 2)(lambda: step(tok // 2))
        pl.when(r >= 2)(lambda: step(tok))
        return carry

    def attend_block(t, j):
        r = t % 4
        s = scores(q_s[t], kv[j, 0], seg[j] == segcol[r][:, :1])
        m_prev = m_s[r]
        m_new = jnp.maximum(m_prev, jnp.max(s, axis=-1, keepdims=True))
        p = jnp.exp2(s - m_new[:, :1])
        alpha = jnp.exp2(m_prev - m_new)
        m_s[r] = m_new
        l_s[r] = l_s[r] * alpha + jnp.sum(p, axis=-1, keepdims=True)
        acc_s[r] = acc_s[r] * alpha + jnp.dot(p.astype(BF16), kv[j, 1], preferred_element_type=F32)

    def attend_end(t, g):
        r = t % 4
        for h in range(heads):
            at = slice(h * tile, (h + 1) * tile)
            o_all[g, tile_rows(r), h * HEAD_DIM:(h + 1) * HEAD_DIM] = (acc_s[r, at, :] / l_s[r, at, :]).astype(BF16)

    def send_heads(t, g):
        o_tile = o_all.at[g, tile_rows(t % 4), :]
        pl.when(middle)(lambda: send(o_tile, o_tile, line_sem, o_recv.at[t], {'tp': 3 - z}))

    @scoped
    def heads_event(u):
        o_tile = o_all.at[g_1 if u < 4 else g_2, tile_rows(u % 4), :]
        arrived(o_tile, o_recv.at[u])
        for to, cond in ((0, z == 1), (3, z == 2)):
            pl.when(cond)(lambda: send(o_tile, o_tile, line_sem, o_recv.at[u], {'tp': to}))

    def heads_here(*tiles):
        on(middle, *((heads_event, u) for u in tiles))

    def on(cond, *todo):
        @pl.when(cond)
        def _():
            for what, *about in todo:
                what(*about)

    n_col = min(512, d_model)

    def project(g, rows, use):
        def cols(n, carry):
            at = pl.ds(pl.multiple_of(n * n_col, n_col), n_col)
            use(rows, at, jnp.dot(o_all[g, rows, :], wo[pl.ds(pl.multiple_of(g * width, width), width), at],
                                  preferred_element_type=F32).astype(BF16))
            return carry

        lax.fori_loop(0, d_model // n_col, cols, 0)

    @scoped
    def project_o(g):
        def keep(rows, at, fresh):
            part[g % 2, rows, at] = fresh

        project(g, every, keep)

    @scoped
    def project_third(g):
        def add(rows, at, fresh):
            pair_sum = part[(3 - g) % 2, rows, at].astype(F32) + fresh.astype(F32)
            run_s[rows, at] = hid[rows, at].astype(F32) + bo_ref[at].astype(F32) + pair_sum

        project(g, every, add)

    @scoped
    def project_last(g, rows):
        def add(rows, at, fresh):
            y_ref[rows, at] = (run_s[rows, at] + (part[(3 - g) % 2, rows, at].astype(F32) + fresh.astype(F32))).astype(BF16)

        project(g, rows, add)

    @scoped
    def kv_pass(i):
        @pl.when(y == 1)
        def _():
            arrived(kv.at[c, i], kv_recv.at[c, i])
            send(kv.at[c, i], kv.at[c, i], kv_sem, kv_recv.at[c, i], to_core)

    def own_block(t, carry):
        attend_own(t, carry)
        on(t == 0, (ev, 'q', 'zs', 0))
        on(t == 3, (kv_pass, 0))
        return carry

    lax.fori_loop(0, 4, own_block, 0)

    @pl.when(c == 1)
    def _():
        arrived(seg.at[cp - 1], seg_recv.at[cp - 1])
        for i in (0, 1):
            arrived(kv.at[cp - 1, i], kv_recv.at[cp - 1, i])

    def first_block(t, carry):
        pl.when(c == 1)(lambda: attend_block(t, cp - 1))
        on(t == 0, (ev, 'q', 'zs', 1))
        on(t == 1, (kv_pass, 1))
        on((t == 2) & middle, (ev, 'a', 'z', 0))
        on((t == 3) & middle, (ev, 'a', 'z', 1))
        on(t == 3, (ev, 'q', 'x', 0))
        on((t == 3) & middle, (ev, 'a', 's', 0))
        return carry

    lax.fori_loop(0, 4, first_block, 0)
    pl.when(y == 1)(lambda: arrived(seg.at[c], seg_recv.at[c]))

    def second_block(t, carry):
        pl.when(y == 1)(lambda: attend_block(t, c))
        on(t == 1, (ev, 'q', 'y', 0))
        on((t == 2) & middle, (ev, 'b', 'z', 0))
        on((t == 2) & edge, (ev, 'a', 'zs', 0))
        on(t == 3, (ev, 'q', 'x', 1))
        return carry

    lax.fori_loop(0, 4, second_block, 0)

    @pl.when(y == 1)
    def _():
        arrived(seg.at[1 - c], seg_recv.at[1 - c])
        for i in (0, 1):
            arrived(kv.at[1 - c, i], kv_recv.at[1 - c, i])

    def third_block(t, carry):
        pl.when(y == 1)(lambda: attend_block(t, 1 - c))
        attend_end(t, z)
        send_heads(t, z)
        on((t == 0) & middle, (ev, 'b', 'z', 1))
        on(t == 1, (ev, 'q', 'y', 1))
        on((t == 1) & middle, (ev, 'a', 's', 1))
        on((t == 2) & middle, (ev, 'b', 's', 0))
        on((t == 2) & edge, (ev, 'a', 'zs', 1))
        return carry

    lax.fori_loop(0, 4, third_block, 0)
    on(edge, (ev, 'b', 'zs', 0))
    on(middle, (ev, 'b', 's', 1), (ev, 'c', 'z', 0))
    ev('q', 'd', 0)
    loads[5].wait()
    project_o(z)
    ev('a', 'xy', 0)
    on(edge, (ev, 'b', 'zs', 1))
    ev('q', 'd', 1)
    whole('q')
    arrived(bq_pair, bq_recv)
    project_q(1, bq_pair)
    on(middle, (ev, 'c', 'z', 1), (ev, 'c', 's', 0))
    ev('a', 'xy', 1)
    heads_here(0)
    on(edge, (ev, 'c', 'zs', 0))

    def pair_heads(t, carry):
        attend_own(t, carry)
        on((t == 4) & middle, (ev, 'c', 's', 1), (heads_event, 1))
        on((t == 5) & (y == 1), (ev, 'b', 'xy', 0))
        on((t == 6) & (y == 1), (ev, 'b', 'xy', 1))
        on((t == 6) & (y == 1) & middle, (heads_event, 4))
        on((t == 7) & (y == 1) & middle, (heads_event, 5))

        def block(j, inner):
            attend_block(t, j)
            return inner

        lax.fori_loop(0, cp, block, 0)
        attend_end(t, pair)
        send_heads(t, pair)
        on((t == 4) & edge, (ev, 'c', 'zs', 1))
        on((t == 4) & (y == 1) & middle, (heads_event, 2))
        on((t == 4) & (y == 1), (ev, 'a', 'd', 0))
        on((t == 5) & (y == 1) & middle, (heads_event, 3))
        on((t == 6) & (y == 1), (ev, 'a', 'd', 1), (ev, 'c', 'xy', 0))
        on((t == 7) & (y == 1), (ev, 'c', 'xy', 1))
        return carry

    lax.fori_loop(4, 8, pair_heads, 0)

    @pl.when(y == 0)
    def _():
        heads_here(2, 3)
        ev('b', 'xy', 0)
        ev('a', 'd', 0)
        heads_here(4)
        ev('b', 'xy', 1)
        heads_here(5)
        ev('a', 'd', 1)
        ev('c', 'xy', 0)
        ev('c', 'xy', 1)

    heads_here(6)
    ev('b', 'd')
    heads_here(7)
    whole('a')
    whole('b')
    ev('c', 'd', 0)
    project_o(pair)
    ev('c', 'd', 1)
    on(edge, *((heads_event, u) for u in range(4)))
    loads[9].wait()
    project_third(g_1)
    whole('c')

    pl.when(middle)(lambda: project_last(g_2, every))

    def last(r, carry):
        arrived(o_all.at[g_2, tile_rows(r), :], o_recv.at[4 + r])
        project_last(g_2, tile_rows(r))
        return carry

    @pl.when(edge)
    def _():
        lax.fori_loop(0, 4, last, 0)

    with jax.named_scope('drain'):
        unit = o_rows // 2

        def sent(count, sems):
            arrived(wo.at[pl.ds(0, count * unit), :], sems)

        sent(58, spread_sem)
        pl.when(edge)(lambda: sent(2, line_sem))
        pl.when(middle)(lambda: sent(26, line_sem))
        for j in (0, 1):
            pl.when(c == j)(lambda: arrived(kv.at[pl.ds(0, 2 - j)], kv_sem))
        arrived(bq_pair, small_sem.at[0])
        for step in (1, 2, 3):
            pl.when(cp + step < 4)(lambda: arrived(seg.at[cp], small_sem.at[step]))


def write_out(y_in, k_in, v_in, y_out, k_out, v_out, sems):
    copies = [pltpu.make_async_copy(a, b, sems.at[i]) for i, (a, b) in enumerate(((y_in, y_out), (k_in, k_out), (v_in, v_out)))]
    for copy in copies:
        copy.start()
    for copy in copies:
        copy.wait()


def solution(mesh):
    def local_block(hidden, seg_ids, w_q, b_q, w_kv, b_kv, w_o, b_o, ln_gain, ln_bias):
        tok, d_model = hidden.shape
        width = w_q.shape[1]
        heads = width // HEAD_DIM
        tile = tok // 4
        hbm = pl.BlockSpec(memory_space=pltpu.HBM)
        vmem = pl.BlockSpec(memory_space=pltpu.VMEM)
        dma = pltpu.SemaphoreType.DMA
        far = lambda a: pltpu.with_memory_space_constraint(a, pltpu.HBM)
        outs = pl.pallas_call(
            kernel,
            out_shape=(jax.ShapeDtypeStruct((tok, d_model), BF16), jax.ShapeDtypeStruct((tok, HEAD_DIM), BF16),
                       jax.ShapeDtypeStruct((tok, HEAD_DIM), BF16)),
            in_specs=[hbm] * 10,
            out_specs=(vmem, vmem, vmem),
            scratch_shapes=[
                pltpu.VMEM((tok, d_model), BF16),
                pltpu.VMEM((tok, d_model), BF16),
                pltpu.VMEM((d_model, 2 * HEAD_DIM), BF16),
                pltpu.VMEM((2, d_model, width), BF16),
                pltpu.VMEM((4 * width, d_model), BF16),
                pltpu.VMEM((width,), BF16),
                pltpu.VMEM((width,), BF16),
                pltpu.VMEM((2 * HEAD_DIM,), BF16),
                pltpu.VMEM((d_model,), BF16),
                pltpu.VMEM((d_model,), BF16),
                pltpu.VMEM((d_model,), BF16),
                pltpu.VMEM((4, 1, tok), jnp.int32),
                pltpu.VMEM((4, tile, tile), jnp.int32),
                pltpu.VMEM((4, 2, tok, HEAD_DIM), BF16),
                pltpu.VMEM((8, heads * tile, HEAD_DIM), BF16),
                pltpu.VMEM((4, tok, width), BF16),
                pltpu.VMEM((2, tok, d_model), BF16),
                pltpu.VMEM((tok, d_model), F32),
                pltpu.VMEM((4, heads * tile, HEAD_DIM), F32),
                pltpu.VMEM((4, heads * tile, HEAD_DIM), F32),
                pltpu.VMEM((4, heads * tile, HEAD_DIM), F32),
                dma((10,)), dma(()), dma(()), dma(()), dma((4,)), dma(()), dma((4,)), dma((4, 2)), dma((9,)), dma((4, 9)), dma((8,)),
            ],
            compiler_params=pltpu.CompilerParams(collective_id=0, has_side_effects=True, vmem_limit_bytes=48 * 2 ** 20),
            name='block',
        )(far(hidden), far(seg_ids.reshape(1, -1)), far(w_q), far(b_q), far(w_kv), far(b_kv), far(w_o), far(b_o), far(ln_gain), far(ln_bias))
        near = lambda a: pltpu.with_memory_space_constraint(a, pltpu.VMEM)
        return pl.pallas_call(
            write_out,
            out_shape=tuple(jax.ShapeDtypeStruct(a.shape, a.dtype) for a in outs),
            in_specs=[vmem] * 3,
            out_specs=(pl.BlockSpec(memory_space=pl.ANY),) * 3,
            scratch_shapes=[dma((3,))],
            name='write',
        )(*map(near, outs))

    row_spec = P(('dp', 'cp'), None)
    tok_spec = P(('dp', 'cp'))
    return jax.shard_map(local_block, mesh=mesh,
                         in_specs=(row_spec, tok_spec, P(None, 'tp'), P('tp'), P(None, None), P(None), P('tp', None), P(None), P(None), P(None)),
                         out_specs=(row_spec, row_spec, row_spec), check_vma=False)
```

```python
import functools
import jax
import jax.numpy as jnp
from jax import lax
from jax.experimental import pallas as pl
from jax.experimental.pallas import tpu as pltpu
from jax.sharding import PartitionSpec as P

HEAD_DIM = 128
LN_EPS = 1e-5
SCORE_SCALE = HEAD_DIM ** -0.5 * 1.4426950408889634
MESH = pl.DeviceIdType.MESH
BF16 = jnp.bfloat16
F32 = jnp.float32


def send(src, dst, sent, recv, to):
    pltpu.make_async_remote_copy(src_ref=src, dst_ref=dst, send_sem=sent, recv_sem=recv, device_id=to, device_id_type=MESH).start()


def scoped(fn):
    def run(*about):
        with jax.named_scope(fn.__name__ + '_'.join(str(a) for a in about if isinstance(a, (str, int)))):
            return fn(*about)
    return run


def arrived(dst, recv):
    pltpu.make_async_copy(dst, dst, recv).wait()


def kernel(hid_hbm, seg_hbm, wq_hbm, bq_hbm, wkv_hbm, bkv_hbm, wo_hbm, bo_hbm, gain_hbm, lnb_hbm,
           y_ref, k_ref, v_ref,
           hid, normed, wkv, wq, wo, bq_own, bq_pair, bkv_ref, bo_ref, gain_ref, lnb_ref, seg, segcol, kv, q_s, o_all, part, run_s, m_s, l_s, acc_s,
           load_sem, spread_sem, line_sem, kv_sem, small_sem, bq_recv, seg_recv, kv_recv, wq_recv, wo_recv, o_recv):
    tok, d_model = hid.shape
    width = wq.shape[2]
    heads = width // HEAD_DIM
    tile = tok // 4
    q_rows, o_rows = d_model // 8, width // 8
    dp, z, cp = lax.axis_index('dp'), lax.axis_index('tp'), lax.axis_index('cp')
    y, c = cp // 2, cp % 2
    pair = z + 1 - 2 * (z % 2)
    below, above = {'tp': z - 1}, {'tp': z + 1}
    to_x, to_y, to_core = {'dp': 1 - dp}, {'cp': cp + 2 - 4 * y}, {'cp': cp + 1 - 2 * c}
    pos = lambda px, py, pc: px * 4 + py * 2 + pc
    p_me, p_x, p_y, p_d = pos(dp, y, c), pos(1 - dp, y, c), pos(dp, 1 - y, c), pos(1 - dp, 1 - y, c)
    g_a = 1 + z % 2
    g_c = 3 - 3 * (z // 2)
    g_b = 6 - z - g_a - g_c

    loads = [pltpu.make_async_copy(hid_hbm, hid, load_sem.at[0]),
             pltpu.make_async_copy(wkv_hbm, wkv, load_sem.at[1]),
             pltpu.make_async_copy(wq_hbm, wq.at[0], load_sem.at[2]),
             pltpu.make_async_copy(bq_hbm, bq_own, load_sem.at[3]),
             pltpu.make_async_copy(seg_hbm, seg.at[cp], load_sem.at[4]),
             pltpu.make_async_copy(wo_hbm, wo.at[pl.ds(z * width, width), :], load_sem.at[5]),
             pltpu.make_async_copy(gain_hbm, gain_ref, load_sem.at[6]),
             pltpu.make_async_copy(lnb_hbm, lnb_ref, load_sem.at[7]),
             pltpu.make_async_copy(bkv_hbm, bkv_ref, load_sem.at[8]),
             pltpu.make_async_copy(bo_hbm, bo_ref, load_sem.at[9])]
    for i in (0, 6, 7, 8, 3, 4, 9):
        loads[i].start()

    barrier = pltpu.get_barrier_semaphore()
    for step in (1, 2, 3):
        pl.semaphore_signal(barrier, inc=1, device_id={'cp': (cp + step) % 4}, device_id_type=MESH)
    pl.semaphore_signal(barrier, inc=1, device_id=to_x, device_id_type=MESH)

    @pl.when(z > 0)
    def _():
        pl.semaphore_signal(barrier, inc=1, device_id={'tp': z - 1}, device_id_type=MESH)

    @pl.when(z < 3)
    def _():
        pl.semaphore_signal(barrier, inc=1, device_id={'tp': z + 1}, device_id_type=MESH)

    loads[1].start()
    with jax.named_scope('barr'):
        pl.semaphore_wait(barrier, 5 + (z + 1) // 2 - 2 * (z // 3))

    loads[2].start()
    def q_piece(p, h):
        half = q_rows // 2
        return wq.at[1, pl.ds(pl.multiple_of(p * q_rows + h * half, half), half), :]

    def o_piece(g, p, h):
        half = o_rows // 2
        return wo.at[pl.ds(pl.multiple_of(g * width + p * o_rows + h * half, half), half), :]

    def sem(g, kind, h):
        at = {'z': 0, 'x': 2, 'y': 4, 'd': 6, 'core': 8}[kind] + (0 if kind == 'core' else h)
        return wq_recv.at[at] if g is None else wo_recv.at[g, at]

    middle, edge = (z > 0) & (z < 3), (z == 0) | (z == 3)

    send(bq_hbm, bq_pair, small_sem.at[0], bq_recv, {'tp': pair})
    for h in (0, 1):
        half = q_rows // 2
        send(wq_hbm.at[pl.ds(pl.multiple_of(p_me * q_rows + h * half, half), half), :], q_piece(p_me, h), spread_sem, sem(None, 'z', h),
             {'tp': pair})
    for h in (0, 1):
        half = o_rows // 2
        for to, cond in ((below, z > 0), (above, z < 3)):
            @pl.when(cond)
            def _():
                send(wo_hbm.at[pl.ds(pl.multiple_of(p_me * o_rows + h * half, half), half), :], o_piece(z, p_me, h), line_sem,
                     sem(z, 'z', h), to)
    for step in (1, 2, 3):
        pl.when(cp + step < 4)(lambda: send(seg_hbm, seg.at[cp], small_sem.at[step], seg_recv.at[cp], {'cp': cp + step}))

    def pass_on(g, source, h, by_x):
        p = {'z': p_me, 's': p_me, 'x': p_x, 'y': p_y, 'd': p_d}[source]
        piece = q_piece(p, h) if g is None else o_piece(g, p, h)
        if source == 's':
            send(piece, piece, spread_sem, sem(g, 'x', h), to_x)
            send(piece, piece, spread_sem, sem(g, 'y', h), to_y)
            return
        arrived(piece, sem(g, source, h))
        if source == 'z' and g is not None:
            pl.when((g > z) & (z > 0))(lambda: send(piece, piece, line_sem, sem(g, 'z', h), below))
            pl.when((g < z) & (z < 3))(lambda: send(piece, piece, line_sem, sem(g, 'z', h), above))
        elif source == 'x':
            if not by_x:
                pl.when(c == 1)(lambda: send(piece, piece, spread_sem, sem(g, 'd', h), to_y))
        elif source == 'y':
            pl.when((c == 0) | by_x)(lambda: send(piece, piece, spread_sem, sem(g, 'd', h), to_x))
        send(piece, piece, spread_sem, sem(g, 'core', h), to_core)

    groups = {'q': None, 'a': g_a, 'b': g_b, 'c': g_c}

    @scoped
    def ev(name, sources, *halves):
        for h in halves or (0, 1):
            for source in sources:
                pass_on(groups[name], source, h, name == 'q')

    @scoped
    def whole(name):
        if name == 'q':
            arrived(wq.at[1, pl.ds(0, 4 * q_rows), :], sem(None, 'core', 0))
        else:
            arrived(wo.at[pl.ds(0, 4 * o_rows), :], sem(groups[name], 'core', 0))

    loads[5].start()

    with jax.named_scope('load_wait'):
        for i in (0, 6, 7):
            loads[i].wait()
    gain = gain_ref[...].astype(F32)
    lnb = lnb_ref[...].astype(F32)
    ln_rows = min(64, tok)

    def ln_step(i, carry):
        rows = pl.ds(pl.multiple_of(i * ln_rows, ln_rows), ln_rows)
        x = hid[rows, :].astype(F32)
        cen = x - jnp.mean(x, axis=-1, keepdims=True)
        var = jnp.mean(cen * cen, axis=-1, keepdims=True)
        normed[rows, :] = (cen * lax.rsqrt(var + LN_EPS) * gain + lnb).astype(BF16)
        return carry

    with jax.named_scope('ln'):
        lax.fori_loop(0, tok // ln_rows, ln_step, 0)

    loads[1].wait()
    loads[8].wait()
    kv_new = (jnp.dot(normed[...], wkv[...], preferred_element_type=F32) + bkv_ref[...].astype(F32)).astype(BF16)
    kv[cp, 0] = kv_new[:, :HEAD_DIM]
    kv[cp, 1] = kv_new[:, HEAD_DIM:]
    k_ref[...] = kv_new[:, :HEAD_DIM]
    v_ref[...] = kv_new[:, HEAD_DIM:]

    @scoped
    def project_q(which, bias):
        qf = jnp.dot(normed[...], wq[which], preferred_element_type=F32) + bias[...].astype(F32)
        for r in range(4):
            for h in range(heads):
                q_s[which * 4 + r, h * tile:(h + 1) * tile, :] = qf[r * tile:(r + 1) * tile, h * HEAD_DIM:(h + 1) * HEAD_DIM].astype(BF16)

    loads[2].wait()
    loads[3].wait()
    for i in (0, 1):
        pl.when(y == 0)(lambda: send(kv.at[cp, i], kv.at[cp, i], kv_sem, kv_recv.at[cp, i], to_y))
    for i in (0, 1):
        pl.when(c == 0)(lambda: send(kv.at[cp, i], kv.at[cp, i], kv_sem, kv_recv.at[cp, i], to_core))
    project_q(0, bq_own)
    loads[4].wait()
    for r in range(4):
        row = jnp.broadcast_to(seg[cp, :, r * tile:(r + 1) * tile], (tile, tile))
        segcol[r] = row.T

    g_1, g_2 = 2 - z // 2, 3 - 3 * (z // 2)
    tile_rows = lambda r: pl.ds(pl.multiple_of(r * tile, tile), tile)
    every = pl.ds(0, tok)

    def scores(q, k_blk, mask):
        keys = k_blk.shape[0]
        s = lax.dot_general(q, k_blk, (((1,), (1,)), ((), ())), preferred_element_type=F32) * SCORE_SCALE
        return jnp.where(mask[None], s.reshape(heads, tile, keys), -jnp.inf).reshape(heads * tile, keys)

    @scoped
    def attend_own(t, carry):
        r = t % 4

        def step(keys):
            k_pos = lax.broadcasted_iota(jnp.int32, (tile, keys), 1)
            q_pos = lax.broadcasted_iota(jnp.int32, (tile, keys), 0) + r * tile
            s = scores(q_s[t], kv[cp, 0, :keys, :], (seg[cp, :, :keys] == segcol[r][:, :1]) & (k_pos <= q_pos))
            m_new = jnp.max(s, axis=-1, keepdims=True)
            p = jnp.exp2(s - m_new)
            m_s[r] = jnp.broadcast_to(m_new, m_s.shape[1:])
            l_s[r] = jnp.broadcast_to(jnp.sum(p, axis=-1, keepdims=True), l_s.shape[1:])
            acc_s[r] = jnp.dot(p.astype(BF16), kv[cp, 1, :keys, :], preferred_element_type=F32)

        pl.when(r < 2)(lambda: step(tok // 2))
        pl.when(r >= 2)(lambda: step(tok))
        return carry

    def attend_block(t, j):
        r = t % 4
        s = scores(q_s[t], kv[j, 0], seg[j] == segcol[r][:, :1])
        m_prev = m_s[r]
        m_new = jnp.maximum(m_prev, jnp.max(s, axis=-1, keepdims=True))
        p = jnp.exp2(s - m_new[:, :1])
        alpha = jnp.exp2(m_prev - m_new)
        m_s[r] = m_new
        l_s[r] = l_s[r] * alpha + jnp.sum(p, axis=-1, keepdims=True)
        acc_s[r] = acc_s[r] * alpha + jnp.dot(p.astype(BF16), kv[j, 1], preferred_element_type=F32)

    def attend_end(t, g):
        r = t % 4
        for h in range(heads):
            at = slice(h * tile, (h + 1) * tile)
            o_all[g, tile_rows(r), h * HEAD_DIM:(h + 1) * HEAD_DIM] = (acc_s[r, at, :] / l_s[r, at, :]).astype(BF16)

    def send_heads(t, g):
        o_tile = o_all.at[g, tile_rows(t % 4), :]
        pl.when(middle)(lambda: send(o_tile, o_tile, line_sem, o_recv.at[t], {'tp': 3 - z}))

    @scoped
    def heads_event(u):
        o_tile = o_all.at[g_1 if u < 4 else g_2, tile_rows(u % 4), :]
        arrived(o_tile, o_recv.at[u])
        for to, cond in ((0, z == 1), (3, z == 2)):
            pl.when(cond)(lambda: send(o_tile, o_tile, line_sem, o_recv.at[u], {'tp': to}))

    def heads_here(*tiles):
        on(middle, *((heads_event, u) for u in tiles))

    def on(cond, *todo):
        @pl.when(cond)
        def _():
            for what, *about in todo:
                what(*about)

    n_col = min(512, d_model)

    def project(g, rows, use):
        def cols(n, carry):
            at = pl.ds(pl.multiple_of(n * n_col, n_col), n_col)
            use(rows, at, jnp.dot(o_all[g, rows, :], wo[pl.ds(pl.multiple_of(g * width, width), width), at],
                                  preferred_element_type=F32).astype(BF16))
            return carry

        lax.fori_loop(0, d_model // n_col, cols, 0)

    @scoped
    def project_o(g):
        def keep(rows, at, fresh):
            part[g % 2, rows, at] = fresh

        project(g, every, keep)

    @scoped
    def project_third(g):
        def add(rows, at, fresh):
            pair_sum = part[(3 - g) % 2, rows, at].astype(F32) + fresh.astype(F32)
            run_s[rows, at] = hid[rows, at].astype(F32) + bo_ref[at].astype(F32) + pair_sum

        project(g, every, add)

    @scoped
    def project_last(g, rows):
        def add(rows, at, fresh):
            y_ref[rows, at] = (run_s[rows, at] + (part[(3 - g) % 2, rows, at].astype(F32) + fresh.astype(F32))).astype(BF16)

        project(g, rows, add)

    @scoped
    def kv_pass(i):
        @pl.when(y == 1)
        def _():
            arrived(kv.at[c, i], kv_recv.at[c, i])
            send(kv.at[c, i], kv.at[c, i], kv_sem, kv_recv.at[c, i], to_core)

    def own_block(t, carry):
        attend_own(t, carry)
        on(t == 0, (ev, 'q', 'zs', 0))
        on(t == 3, (kv_pass, 0))
        return carry

    lax.fori_loop(0, 4, own_block, 0)

    @pl.when(c == 1)
    def _():
        arrived(seg.at[cp - 1], seg_recv.at[cp - 1])
        for i in (0, 1):
            arrived(kv.at[cp - 1, i], kv_recv.at[cp - 1, i])

    def first_block(t, carry):
        pl.when(c == 1)(lambda: attend_block(t, cp - 1))
        on(t == 0, (ev, 'q', 'zs', 1))
        on(t == 1, (kv_pass, 1))
        on((t == 2) & middle, (ev, 'a', 'z', 0))
        on((t == 3) & middle, (ev, 'a', 'z', 1))
        on(t == 3, (ev, 'q', 'x', 0))
        on((t == 3) & middle, (ev, 'a', 's', 0))
        return carry

    lax.fori_loop(0, 4, first_block, 0)
    pl.when(y == 1)(lambda: arrived(seg.at[c], seg_recv.at[c]))

    def second_block(t, carry):
        pl.when(y == 1)(lambda: attend_block(t, c))
        on(t == 1, (ev, 'q', 'y', 0))
        on((t == 2) & middle, (ev, 'b', 'z', 0))
        on((t == 2) & edge, (ev, 'a', 'zs', 0))
        on(t == 3, (ev, 'q', 'x', 1))
        return carry

    lax.fori_loop(0, 4, second_block, 0)

    @pl.when(y == 1)
    def _():
        arrived(seg.at[1 - c], seg_recv.at[1 - c])
        for i in (0, 1):
            arrived(kv.at[1 - c, i], kv_recv.at[1 - c, i])

    def third_block(t, carry):
        pl.when(y == 1)(lambda: attend_block(t, 1 - c))
        attend_end(t, z)
        on((t == 0) & middle, (ev, 'b', 'z', 1))
        send_heads(t, z)
        on(t == 1, (ev, 'q', 'y', 1))
        on((t == 1) & middle, (ev, 'a', 's', 1))
        on((t == 2) & middle, (ev, 'b', 's', 0))
        on((t == 2) & edge, (ev, 'a', 'zs', 1))
        return carry

    lax.fori_loop(0, 4, third_block, 0)
    on(edge, (ev, 'b', 'zs', 0))
    on(middle, (ev, 'b', 's', 1), (ev, 'c', 'z', 0))
    ev('q', 'd', 0)
    loads[5].wait()
    project_o(z)
    ev('a', 'xy', 0)
    on(edge, (ev, 'b', 'zs', 1))
    ev('q', 'd', 1)
    on(middle, (ev, 'c', 'z', 1))
    whole('q')
    arrived(bq_pair, bq_recv)
    project_q(1, bq_pair)
    on(middle, (ev, 'c', 's', 0))
    ev('a', 'xy', 1)
    heads_here(0)
    on(edge, (ev, 'c', 'zs', 0))

    def pair_heads(t, carry):
        attend_own(t, carry)
        on((t == 4) & middle, (ev, 'c', 's', 1), (heads_event, 1))
        on((t == 5) & (y == 1), (ev, 'b', 'xy', 0))
        on((t == 6) & (y == 1), (ev, 'b', 'xy', 1))
        on((t == 6) & (y == 1) & middle, (heads_event, 4))
        on((t == 7) & (y == 1) & middle, (heads_event, 5))

        def block(j, inner):
            attend_block(t, j)
            return inner

        lax.fori_loop(0, cp, block, 0)
        attend_end(t, pair)
        send_heads(t, pair)
        on((t == 4) & edge, (ev, 'c', 'zs', 1))
        on((t == 4) & (y == 1) & middle, (heads_event, 2))
        on((t == 4) & (y == 1), (ev, 'a', 'd', 0))
        on((t == 5) & (y == 1) & middle, (heads_event, 3))
        on((t == 6) & (y == 1), (ev, 'a', 'd', 1), (ev, 'c', 'xy', 0))
        on((t == 7) & (y == 1), (ev, 'c', 'xy', 1))
        return carry

    lax.fori_loop(4, 8, pair_heads, 0)

    @pl.when(y == 0)
    def _():
        heads_here(2, 3)
        ev('b', 'xy', 0)
        ev('a', 'd', 0)
        heads_here(4)
        ev('b', 'xy', 1)
        heads_here(5)
        ev('a', 'd', 1)
        ev('c', 'xy', 0)
        ev('c', 'xy', 1)

    heads_here(6)
    ev('b', 'd')
    heads_here(7)
    whole('a')
    whole('b')
    ev('c', 'd', 0)
    project_o(pair)
    ev('c', 'd', 1)
    on(edge, *((heads_event, u) for u in range(4)))
    loads[9].wait()
    project_third(g_1)
    whole('c')

    pl.when(middle)(lambda: project_last(g_2, every))

    def last(r, carry):
        arrived(o_all.at[g_2, tile_rows(r), :], o_recv.at[4 + r])
        project_last(g_2, tile_rows(r))
        return carry

    @pl.when(edge)
    def _():
        lax.fori_loop(0, 4, last, 0)

    with jax.named_scope('drain'):
        unit = o_rows // 2

        def sent(count, sems):
            arrived(wo.at[pl.ds(0, count * unit), :], sems)

        sent(58, spread_sem)
        pl.when(edge)(lambda: sent(2, line_sem))
        pl.when(middle)(lambda: sent(26, line_sem))
        for j in (0, 1):
            pl.when(c == j)(lambda: arrived(kv.at[pl.ds(0, 2 - j)], kv_sem))
        arrived(bq_pair, small_sem.at[0])
        for step in (1, 2, 3):
            pl.when(cp + step < 4)(lambda: arrived(seg.at[cp], small_sem.at[step]))


def write_out(y_in, k_in, v_in, y_out, k_out, v_out, sems):
    copies = [pltpu.make_async_copy(a, b, sems.at[i]) for i, (a, b) in enumerate(((y_in, y_out), (k_in, k_out), (v_in, v_out)))]
    for copy in copies:
        copy.start()
    for copy in copies:
        copy.wait()


def solution(mesh):
    def local_block(hidden, seg_ids, w_q, b_q, w_kv, b_kv, w_o, b_o, ln_gain, ln_bias):
        tok, d_model = hidden.shape
        width = w_q.shape[1]
        heads = width // HEAD_DIM
        tile = tok // 4
        hbm = pl.BlockSpec(memory_space=pltpu.HBM)
        vmem = pl.BlockSpec(memory_space=pltpu.VMEM)
        dma = pltpu.SemaphoreType.DMA
        far = lambda a: pltpu.with_memory_space_constraint(a, pltpu.HBM)
        outs = pl.pallas_call(
            kernel,
            out_shape=(jax.ShapeDtypeStruct((tok, d_model), BF16), jax.ShapeDtypeStruct((tok, HEAD_DIM), BF16),
                       jax.ShapeDtypeStruct((tok, HEAD_DIM), BF16)),
            in_specs=[hbm] * 10,
            out_specs=(vmem, vmem, vmem),
            scratch_shapes=[
                pltpu.VMEM((tok, d_model), BF16),
                pltpu.VMEM((tok, d_model), BF16),
                pltpu.VMEM((d_model, 2 * HEAD_DIM), BF16),
                pltpu.VMEM((2, d_model, width), BF16),
                pltpu.VMEM((4 * width, d_model), BF16),
                pltpu.VMEM((width,), BF16),
                pltpu.VMEM((width,), BF16),
                pltpu.VMEM((2 * HEAD_DIM,), BF16),
                pltpu.VMEM((d_model,), BF16),
                pltpu.VMEM((d_model,), BF16),
                pltpu.VMEM((d_model,), BF16),
                pltpu.VMEM((4, 1, tok), jnp.int32),
                pltpu.VMEM((4, tile, tile), jnp.int32),
                pltpu.VMEM((4, 2, tok, HEAD_DIM), BF16),
                pltpu.VMEM((8, heads * tile, HEAD_DIM), BF16),
                pltpu.VMEM((4, tok, width), BF16),
                pltpu.VMEM((2, tok, d_model), BF16),
                pltpu.VMEM((tok, d_model), F32),
                pltpu.VMEM((4, heads * tile, HEAD_DIM), F32),
                pltpu.VMEM((4, heads * tile, HEAD_DIM), F32),
                pltpu.VMEM((4, heads * tile, HEAD_DIM), F32),
                dma((10,)), dma(()), dma(()), dma(()), dma((4,)), dma(()), dma((4,)), dma((4, 2)), dma((9,)), dma((4, 9)), dma((8,)),
            ],
            compiler_params=pltpu.CompilerParams(collective_id=0, has_side_effects=True, vmem_limit_bytes=48 * 2 ** 20),
            name='block',
        )(far(hidden), far(seg_ids.reshape(1, -1)), far(w_q), far(b_q), far(w_kv), far(b_kv), far(w_o), far(b_o), far(ln_gain), far(ln_bias))
        near = lambda a: pltpu.with_memory_space_constraint(a, pltpu.VMEM)
        return pl.pallas_call(
            write_out,
            out_shape=tuple(jax.ShapeDtypeStruct(a.shape, a.dtype) for a in outs),
            in_specs=[vmem] * 3,
            out_specs=(pl.BlockSpec(memory_space=pl.ANY),) * 3,
            scratch_shapes=[dma((3,))],
            name='write',
        )(*map(near, outs))

    row_spec = P(('dp', 'cp'), None)
    tok_spec = P(('dp', 'cp'))
    return jax.shard_map(local_block, mesh=mesh,
                         in_specs=(row_spec, tok_spec, P(None, 'tp'), P('tp'), P(None, None), P(None), P('tp', None), P(None), P(None), P(None)),
                         out_specs=(row_spec, row_spec, row_spec), check_vma=False)
```

```python
import functools
import jax
import jax.numpy as jnp
from jax import lax
from jax.experimental import pallas as pl
from jax.experimental.pallas import tpu as pltpu
from jax.sharding import PartitionSpec as P

HEAD_DIM = 128
LN_EPS = 1e-5
SCORE_SCALE = HEAD_DIM ** -0.5 * 1.4426950408889634
MESH = pl.DeviceIdType.MESH
BF16 = jnp.bfloat16
F32 = jnp.float32


def send(src, dst, sent, recv, to):
    pltpu.make_async_remote_copy(src_ref=src, dst_ref=dst, send_sem=sent, recv_sem=recv, device_id=to, device_id_type=MESH).start()


def scoped(fn):
    def run(*about):
        with jax.named_scope(fn.__name__ + '_'.join(str(a) for a in about if isinstance(a, (str, int)))):
            return fn(*about)
    return run


def arrived(dst, recv):
    pltpu.make_async_copy(dst, dst, recv).wait()


def kernel(hid_hbm, seg_hbm, wq_hbm, bq_hbm, wkv_hbm, bkv_hbm, wo_hbm, bo_hbm, gain_hbm, lnb_hbm,
           y_ref, k_ref, v_ref,
           hid, normed, wkv, wq, wo, bq_own, bq_pair, bkv_ref, bo_ref, gain_ref, lnb_ref, seg, segcol, kv, q_s, o_all, part, run_s, m_s, l_s, acc_s,
           load_sem, spread_sem, line_sem, kv_sem, small_sem, bq_recv, seg_recv, kv_recv, wq_recv, wo_recv, o_recv):
    tok, d_model = hid.shape
    width = wq.shape[2]
    heads = width // HEAD_DIM
    tile = tok // 4
    q_rows, o_rows = d_model // 8, width // 8
    dp, z, cp = lax.axis_index('dp'), lax.axis_index('tp'), lax.axis_index('cp')
    y, c = cp // 2, cp % 2
    pair = z + 1 - 2 * (z % 2)
    below, above = {'tp': z - 1}, {'tp': z + 1}
    to_x, to_y, to_core = {'dp': 1 - dp}, {'cp': cp + 2 - 4 * y}, {'cp': cp + 1 - 2 * c}
    pos = lambda px, py, pc: px * 4 + py * 2 + pc
    p_me, p_x, p_y, p_d = pos(dp, y, c), pos(1 - dp, y, c), pos(dp, 1 - y, c), pos(1 - dp, 1 - y, c)
    g_a = 1 + z % 2
    g_c = 3 - 3 * (z // 2)
    g_b = 6 - z - g_a - g_c

    loads = [pltpu.make_async_copy(hid_hbm, hid, load_sem.at[0]),
             pltpu.make_async_copy(wkv_hbm, wkv, load_sem.at[1]),
             pltpu.make_async_copy(wq_hbm, wq.at[0], load_sem.at[2]),
             pltpu.make_async_copy(bq_hbm, bq_own, load_sem.at[3]),
             pltpu.make_async_copy(seg_hbm, seg.at[cp], load_sem.at[4]),
             pltpu.make_async_copy(wo_hbm, wo.at[pl.ds(z * width, width), :], load_sem.at[5]),
             pltpu.make_async_copy(gain_hbm, gain_ref, load_sem.at[6]),
             pltpu.make_async_copy(lnb_hbm, lnb_ref, load_sem.at[7]),
             pltpu.make_async_copy(bkv_hbm, bkv_ref, load_sem.at[8]),
             pltpu.make_async_copy(bo_hbm, bo_ref, load_sem.at[9])]
    for i in (0, 6, 7, 8, 3, 4, 9):
        loads[i].start()

    barrier = pltpu.get_barrier_semaphore()
    for step in (1, 2, 3):
        pl.semaphore_signal(barrier, inc=1, device_id={'cp': (cp + step) % 4}, device_id_type=MESH)
    pl.semaphore_signal(barrier, inc=1, device_id=to_x, device_id_type=MESH)

    @pl.when(z > 0)
    def _():
        pl.semaphore_signal(barrier, inc=1, device_id={'tp': z - 1}, device_id_type=MESH)

    @pl.when(z < 3)
    def _():
        pl.semaphore_signal(barrier, inc=1, device_id={'tp': z + 1}, device_id_type=MESH)

    loads[1].start()
    with jax.named_scope('barr'):
        pl.semaphore_wait(barrier, 5 + (z + 1) // 2 - 2 * (z // 3))

    loads[2].start()
    def q_piece(p, h):
        half = q_rows // 2
        return wq.at[1, pl.ds(pl.multiple_of(p * q_rows + h * half, half), half), :]

    def o_piece(g, p, h):
        half = o_rows // 2
        return wo.at[pl.ds(pl.multiple_of(g * width + p * o_rows + h * half, half), half), :]

    def sem(g, kind, h):
        at = {'z': 0, 'x': 2, 'y': 4, 'd': 6, 'core': 8}[kind] + (0 if kind == 'core' else h)
        return wq_recv.at[at] if g is None else wo_recv.at[g, at]

    middle, edge = (z > 0) & (z < 3), (z == 0) | (z == 3)

    send(bq_hbm, bq_pair, small_sem.at[0], bq_recv, {'tp': pair})
    for h in (0, 1):
        half = q_rows // 2
        send(wq_hbm.at[pl.ds(pl.multiple_of(p_me * q_rows + h * half, half), half), :], q_piece(p_me, h), spread_sem, sem(None, 'z', h),
             {'tp': pair})
    for h in (0, 1):
        half = o_rows // 2
        for to, cond in ((below, z > 0), (above, z < 3)):
            @pl.when(cond)
            def _():
                send(wo_hbm.at[pl.ds(pl.multiple_of(p_me * o_rows + h * half, half), half), :], o_piece(z, p_me, h), line_sem,
                     sem(z, 'z', h), to)
    for step in (1, 2, 3):
        pl.when(cp + step < 4)(lambda: send(seg_hbm, seg.at[cp], small_sem.at[step], seg_recv.at[cp], {'cp': cp + step}))

    def pass_on(g, source, h, by_x):
        p = {'z': p_me, 's': p_me, 'x': p_x, 'y': p_y, 'd': p_d}[source]
        piece = q_piece(p, h) if g is None else o_piece(g, p, h)
        if source == 's':
            send(piece, piece, spread_sem, sem(g, 'x', h), to_x)
            send(piece, piece, spread_sem, sem(g, 'y', h), to_y)
            return
        arrived(piece, sem(g, source, h))
        if source == 'z' and g is not None:
            pl.when((g > z) & (z > 0))(lambda: send(piece, piece, line_sem, sem(g, 'z', h), below))
            pl.when((g < z) & (z < 3))(lambda: send(piece, piece, line_sem, sem(g, 'z', h), above))
        elif source == 'x':
            if not by_x:
                pl.when(c == 1)(lambda: send(piece, piece, spread_sem, sem(g, 'd', h), to_y))
        elif source == 'y':
            pl.when((c == 0) | by_x)(lambda: send(piece, piece, spread_sem, sem(g, 'd', h), to_x))
        send(piece, piece, spread_sem, sem(g, 'core', h), to_core)

    groups = {'q': None, 'a': g_a, 'b': g_b, 'c': g_c}

    @scoped
    def ev(name, sources, *halves):
        for h in halves or (0, 1):
            for source in sources:
                pass_on(groups[name], source, h, name == 'q')

    @scoped
    def whole(name):
        if name == 'q':
            arrived(wq.at[1, pl.ds(0, 4 * q_rows), :], sem(None, 'core', 0))
        else:
            arrived(wo.at[pl.ds(0, 4 * o_rows), :], sem(groups[name], 'core', 0))

    loads[5].start()

    with jax.named_scope('load_wait'):
        for i in (0, 6, 7):
            loads[i].wait()
    gain = gain_ref[...].astype(F32)
    lnb = lnb_ref[...].astype(F32)
    ln_rows = min(64, tok)

    def ln_step(i, carry):
        rows = pl.ds(pl.multiple_of(i * ln_rows, ln_rows), ln_rows)
        x = hid[rows, :].astype(F32)
        cen = x - jnp.mean(x, axis=-1, keepdims=True)
        var = jnp.mean(cen * cen, axis=-1, keepdims=True)
        normed[rows, :] = (cen * lax.rsqrt(var + LN_EPS) * gain + lnb).astype(BF16)
        return carry

    with jax.named_scope('ln'):
        lax.fori_loop(0, tok // ln_rows, ln_step, 0)

    loads[1].wait()
    loads[8].wait()
    kv_new = (jnp.dot(normed[...], wkv[...], preferred_element_type=F32) + bkv_ref[...].astype(F32)).astype(BF16)
    kv[cp, 0] = kv_new[:, :HEAD_DIM]
    kv[cp, 1] = kv_new[:, HEAD_DIM:]
    k_ref[...] = kv_new[:, :HEAD_DIM]
    v_ref[...] = kv_new[:, HEAD_DIM:]

    @scoped
    def project_q(which, bias):
        qf = jnp.dot(normed[...], wq[which], preferred_element_type=F32) + bias[...].astype(F32)
        for r in range(4):
            for h in range(heads):
                q_s[which * 4 + r, h * tile:(h + 1) * tile, :] = qf[r * tile:(r + 1) * tile, h * HEAD_DIM:(h + 1) * HEAD_DIM].astype(BF16)

    loads[2].wait()
    loads[3].wait()
    for i in (0, 1):
        pl.when(y == 0)(lambda: send(kv.at[cp, i], kv.at[cp, i], kv_sem, kv_recv.at[cp, i], to_y))
    for i in (0, 1):
        pl.when(c == 0)(lambda: send(kv.at[cp, i], kv.at[cp, i], kv_sem, kv_recv.at[cp, i], to_core))
    project_q(0, bq_own)
    loads[4].wait()
    for r in range(4):
        row = jnp.broadcast_to(seg[cp, :, r * tile:(r + 1) * tile], (tile, tile))
        segcol[r] = row.T

    g_1, g_2 = 2 - z // 2, 3 - 3 * (z // 2)
    tile_rows = lambda r: pl.ds(pl.multiple_of(r * tile, tile), tile)
    every = pl.ds(0, tok)

    def scores(q, k_blk, mask):
        keys = k_blk.shape[0]
        s = lax.dot_general(q, k_blk, (((1,), (1,)), ((), ())), preferred_element_type=F32) * SCORE_SCALE
        return jnp.where(mask[None], s.reshape(heads, tile, keys), -jnp.inf).reshape(heads * tile, keys)

    @scoped
    def attend_own(t, carry):
        r = t % 4

        def step(keys):
            k_pos = lax.broadcasted_iota(jnp.int32, (tile, keys), 1)
            q_pos = lax.broadcasted_iota(jnp.int32, (tile, keys), 0) + r * tile
            s = scores(q_s[t], kv[cp, 0, :keys, :], (seg[cp, :, :keys] == segcol[r][:, :1]) & (k_pos <= q_pos))
            m_new = jnp.max(s, axis=-1, keepdims=True)
            p = jnp.exp2(s - m_new)
            m_s[r] = jnp.broadcast_to(m_new, m_s.shape[1:])
            l_s[r] = jnp.broadcast_to(jnp.sum(p, axis=-1, keepdims=True), l_s.shape[1:])
            acc_s[r] = jnp.dot(p.astype(BF16), kv[cp, 1, :keys, :], preferred_element_type=F32)

        pl.when(r < 2)(lambda: step(tok // 2))
        pl.when(r >= 2)(lambda: step(tok))
        return carry

    def attend_block(t, j):
        r = t % 4
        s = scores(q_s[t], kv[j, 0], seg[j] == segcol[r][:, :1])
        m_prev = m_s[r]
        m_new = jnp.maximum(m_prev, jnp.max(s, axis=-1, keepdims=True))
        p = jnp.exp2(s - m_new[:, :1])
        alpha = jnp.exp2(m_prev - m_new)
        m_s[r] = m_new
        l_s[r] = l_s[r] * alpha + jnp.sum(p, axis=-1, keepdims=True)
        acc_s[r] = acc_s[r] * alpha + jnp.dot(p.astype(BF16), kv[j, 1], preferred_element_type=F32)

    def attend_end(t, g):
        r = t % 4
        for h in range(heads):
            at = slice(h * tile, (h + 1) * tile)
            o_all[g, tile_rows(r), h * HEAD_DIM:(h + 1) * HEAD_DIM] = (acc_s[r, at, :] / l_s[r, at, :]).astype(BF16)

    def send_heads(t, g):
        o_tile = o_all.at[g, tile_rows(t % 4), :]
        pl.when(middle)(lambda: send(o_tile, o_tile, line_sem, o_recv.at[t], {'tp': 3 - z}))

    @scoped
    def heads_event(u):
        o_tile = o_all.at[g_1 if u < 4 else g_2, tile_rows(u % 4), :]
        arrived(o_tile, o_recv.at[u])
        for to, cond in ((0, z == 1), (3, z == 2)):
            pl.when(cond)(lambda: send(o_tile, o_tile, line_sem, o_recv.at[u], {'tp': to}))

    def heads_here(*tiles):
        on(middle, *((heads_event, u) for u in tiles))

    def on(cond, *todo):
        @pl.when(cond)
        def _():
            for what, *about in todo:
                what(*about)

    n_col = min(512, d_model)

    def project(g, rows, use):
        def cols(n, carry):
            at = pl.ds(pl.multiple_of(n * n_col, n_col), n_col)
            use(rows, at, jnp.dot(o_all[g, rows, :], wo[pl.ds(pl.multiple_of(g * width, width), width), at],
                                  preferred_element_type=F32).astype(BF16))
            return carry

        lax.fori_loop(0, d_model // n_col, cols, 0)

    @scoped
    def project_o(g):
        def keep(rows, at, fresh):
            part[g % 2, rows, at] = fresh

        project(g, every, keep)

    @scoped
    def project_third(g):
        def add(rows, at, fresh):
            pair_sum = part[(3 - g) % 2, rows, at].astype(F32) + fresh.astype(F32)
            run_s[rows, at] = hid[rows, at].astype(F32) + bo_ref[at].astype(F32) + pair_sum

        project(g, every, add)

    @scoped
    def project_last(g, rows):
        def add(rows, at, fresh):
            y_ref[rows, at] = (run_s[rows, at] + (part[(3 - g) % 2, rows, at].astype(F32) + fresh.astype(F32))).astype(BF16)

        project(g, rows, add)

    @scoped
    def kv_pass(i):
        @pl.when(y == 1)
        def _():
            arrived(kv.at[c, i], kv_recv.at[c, i])
            send(kv.at[c, i], kv.at[c, i], kv_sem, kv_recv.at[c, i], to_core)

    def own_block(t, carry):
        attend_own(t, carry)
        on(t == 0, (ev, 'q', 'zs', 0))
        on(t == 3, (kv_pass, 0))
        return carry

    lax.fori_loop(0, 4, own_block, 0)

    @pl.when(c == 1)
    def _():
        arrived(seg.at[cp - 1], seg_recv.at[cp - 1])
        for i in (0, 1):
            arrived(kv.at[cp - 1, i], kv_recv.at[cp - 1, i])

    def first_block(t, carry):
        pl.when(c == 1)(lambda: attend_block(t, cp - 1))
        on(t == 0, (ev, 'q', 'zs', 1))
        on(t == 1, (kv_pass, 1))
        on((t == 2) & middle, (ev, 'a', 'z', 0))
        on((t == 3) & middle, (ev, 'a', 'z', 1))
        on(t == 3, (ev, 'q', 'x', 0))
        on((t == 3) & middle, (ev, 'a', 's', 0))
        return carry

    lax.fori_loop(0, 4, first_block, 0)
    pl.when(y == 1)(lambda: arrived(seg.at[c], seg_recv.at[c]))

    def second_block(t, carry):
        pl.when(y == 1)(lambda: attend_block(t, c))
        on(t == 1, (ev, 'q', 'y', 0))
        on((t == 2) & middle, (ev, 'b', 'z', 0))
        on((t == 2) & edge, (ev, 'a', 'zs', 0))
        on(t == 3, (ev, 'q', 'x', 1))
        return carry

    lax.fori_loop(0, 4, second_block, 0)

    @pl.when(y == 1)
    def _():
        arrived(seg.at[1 - c], seg_recv.at[1 - c])
        for i in (0, 1):
            arrived(kv.at[1 - c, i], kv_recv.at[1 - c, i])

    def third_block(t, carry):
        pl.when(y == 1)(lambda: attend_block(t, 1 - c))
        attend_end(t, z)
        on((t == 0) & middle, (ev, 'b', 'z', 1))
        send_heads(t, z)
        on(t == 1, (ev, 'q', 'y', 1))
        on((t == 1) & middle, (ev, 'a', 's', 1))
        on((t == 2) & middle, (ev, 'b', 's', 0))
        on((t == 2) & edge, (ev, 'a', 'zs', 1))
        return carry

    lax.fori_loop(0, 4, third_block, 0)
    on(edge, (ev, 'b', 'zs', 0))
    on(middle, (ev, 'b', 's', 1), (ev, 'c', 'z', 0))
    ev('q', 'd', 0)
    loads[5].wait()
    project_o(z)
    ev('a', 'xy', 0)
    on(edge, (ev, 'b', 'zs', 1))
    ev('q', 'd', 1)
    on(middle, (ev, 'c', 'z', 1))
    whole('q')
    arrived(bq_pair, bq_recv)
    project_q(1, bq_pair)
    on(middle, (ev, 'c', 's', 0))
    ev('a', 'xy', 1)
    heads_here(0)
    on(edge, (ev, 'c', 'zs', 0))

    def pair_heads(t, carry):
        attend_own(t, carry)
        on((t == 4) & middle, (ev, 'c', 's', 1), (heads_event, 1))
        on((t == 5) & (y == 1), (ev, 'b', 'xy', 0))
        on((t == 6) & (y == 1), (ev, 'b', 'xy', 1))
        on((t == 6) & (y == 1) & middle, (heads_event, 4))
        on((t == 7) & (y == 1) & middle, (heads_event, 5))

        def block(j, inner):
            attend_block(t, j)
            return inner

        lax.fori_loop(0, cp, block, 0)
        attend_end(t, pair)
        send_heads(t, pair)
        on((t == 4) & edge, (ev, 'c', 'zs', 1))
        on((t == 4) & (y == 1) & middle, (heads_event, 2))
        on((t == 4) & (y == 1), (ev, 'a', 'd', 0))
        on((t == 5) & (y == 1) & middle, (heads_event, 3))
        on((t == 6) & (y == 1), (ev, 'a', 'd', 1), (ev, 'c', 'xy', 0))
        on((t == 7) & (y == 1), (ev, 'c', 'xy', 1))
        return carry

    lax.fori_loop(4, 8, pair_heads, 0)

    @pl.when(y == 0)
    def _():
        heads_here(2, 3)
        ev('b', 'xy', 0)
        ev('a', 'd', 0)
        heads_here(4)
        ev('b', 'xy', 1)
        heads_here(5)
        ev('a', 'd', 1)
        ev('c', 'xy', 0)
        ev('c', 'xy', 1)

    heads_here(6)
    ev('b', 'd')
    whole('a')
    loads[9].wait()
    on(edge, (project_o, pair))
    on(middle, (project_third, g_1))
    heads_here(7)
    whole('b')
    ev('c', 'd', 0)
    on(edge, *((heads_event, u) for u in range(4)))
    on(edge, (project_third, g_1))
    on(middle, (project_o, pair))
    ev('c', 'd', 1)
    whole('c')

    pl.when(middle)(lambda: project_last(g_2, every))

    def last(i, carry):
        for r in (2 * i, 2 * i + 1):
            arrived(o_all.at[g_2, tile_rows(r), :], o_recv.at[4 + r])
        project_last(g_2, pl.ds(pl.multiple_of(2 * i * tile, 2 * tile), 2 * tile))
        return carry

    @pl.when(edge)
    def _():
        lax.fori_loop(0, 2, last, 0)

    with jax.named_scope('drain'):
        unit = o_rows // 2

        def sent(count, sems):
            arrived(wo.at[pl.ds(0, count * unit), :], sems)

        sent(58, spread_sem)
        pl.when(edge)(lambda: sent(2, line_sem))
        pl.when(middle)(lambda: sent(26, line_sem))
        for j in (0, 1):
            pl.when(c == j)(lambda: arrived(kv.at[pl.ds(0, 2 - j)], kv_sem))
        arrived(bq_pair, small_sem.at[0])
        for step in (1, 2, 3):
            pl.when(cp + step < 4)(lambda: arrived(seg.at[cp], small_sem.at[step]))


def write_out(y_in, k_in, v_in, y_out, k_out, v_out, sems):
    copies = [pltpu.make_async_copy(a, b, sems.at[i]) for i, (a, b) in enumerate(((y_in, y_out), (k_in, k_out), (v_in, v_out)))]
    for copy in copies:
        copy.start()
    for copy in copies:
        copy.wait()


def solution(mesh):
    def local_block(hidden, seg_ids, w_q, b_q, w_kv, b_kv, w_o, b_o, ln_gain, ln_bias):
        tok, d_model = hidden.shape
        width = w_q.shape[1]
        heads = width // HEAD_DIM
        tile = tok // 4
        hbm = pl.BlockSpec(memory_space=pltpu.HBM)
        vmem = pl.BlockSpec(memory_space=pltpu.VMEM)
        dma = pltpu.SemaphoreType.DMA
        far = lambda a: pltpu.with_memory_space_constraint(a, pltpu.HBM)
        outs = pl.pallas_call(
            kernel,
            out_shape=(jax.ShapeDtypeStruct((tok, d_model), BF16), jax.ShapeDtypeStruct((tok, HEAD_DIM), BF16),
                       jax.ShapeDtypeStruct((tok, HEAD_DIM), BF16)),
            in_specs=[hbm] * 10,
            out_specs=(vmem, vmem, vmem),
            scratch_shapes=[
                pltpu.VMEM((tok, d_model), BF16),
                pltpu.VMEM((tok, d_model), BF16),
                pltpu.VMEM((d_model, 2 * HEAD_DIM), BF16),
                pltpu.VMEM((2, d_model, width), BF16),
                pltpu.VMEM((4 * width, d_model), BF16),
                pltpu.VMEM((width,), BF16),
                pltpu.VMEM((width,), BF16),
                pltpu.VMEM((2 * HEAD_DIM,), BF16),
                pltpu.VMEM((d_model,), BF16),
                pltpu.VMEM((d_model,), BF16),
                pltpu.VMEM((d_model,), BF16),
                pltpu.VMEM((4, 1, tok), jnp.int32),
                pltpu.VMEM((4, tile, tile), jnp.int32),
                pltpu.VMEM((4, 2, tok, HEAD_DIM), BF16),
                pltpu.VMEM((8, heads * tile, HEAD_DIM), BF16),
                pltpu.VMEM((4, tok, width), BF16),
                pltpu.VMEM((2, tok, d_model), BF16),
                pltpu.VMEM((tok, d_model), F32),
                pltpu.VMEM((4, heads * tile, HEAD_DIM), F32),
                pltpu.VMEM((4, heads * tile, HEAD_DIM), F32),
                pltpu.VMEM((4, heads * tile, HEAD_DIM), F32),
                dma((10,)), dma(()), dma(()), dma(()), dma((4,)), dma(()), dma((4,)), dma((4, 2)), dma((9,)), dma((4, 9)), dma((8,)),
            ],
            compiler_params=pltpu.CompilerParams(collective_id=0, has_side_effects=True, vmem_limit_bytes=48 * 2 ** 20),
            name='block',
        )(far(hidden), far(seg_ids.reshape(1, -1)), far(w_q), far(b_q), far(w_kv), far(b_kv), far(w_o), far(b_o), far(ln_gain), far(ln_bias))
        near = lambda a: pltpu.with_memory_space_constraint(a, pltpu.VMEM)
        return pl.pallas_call(
            write_out,
            out_shape=tuple(jax.ShapeDtypeStruct(a.shape, a.dtype) for a in outs),
            in_specs=[vmem] * 3,
            out_specs=(pl.BlockSpec(memory_space=pl.ANY),) * 3,
            scratch_shapes=[dma((3,))],
            name='write',
        )(*map(near, outs))

    row_spec = P(('dp', 'cp'), None)
    tok_spec = P(('dp', 'cp'))
    return jax.shard_map(local_block, mesh=mesh,
                         in_specs=(row_spec, tok_spec, P(None, 'tp'), P('tp'), P(None, None), P(None), P('tp', None), P(None), P(None), P(None)),
                         out_specs=(row_spec, row_spec, row_spec), check_vma=False)
```

```python
import functools
import jax
import jax.numpy as jnp
from jax import lax
from jax.experimental import pallas as pl
from jax.experimental.pallas import tpu as pltpu
from jax.sharding import PartitionSpec as P

HEAD_DIM = 128
LN_EPS = 1e-5
SCORE_SCALE = HEAD_DIM ** -0.5 * 1.4426950408889634
MESH = pl.DeviceIdType.MESH
BF16 = jnp.bfloat16
F32 = jnp.float32


def send(src, dst, sent, recv, to):
    pltpu.make_async_remote_copy(src_ref=src, dst_ref=dst, send_sem=sent, recv_sem=recv, device_id=to, device_id_type=MESH).start()


def scoped(fn):
    def run(*about):
        with jax.named_scope(fn.__name__ + '_'.join(str(a) for a in about if isinstance(a, (str, int)))):
            return fn(*about)
    return run


def arrived(dst, recv):
    pltpu.make_async_copy(dst, dst, recv).wait()


def kernel(hid_hbm, seg_hbm, wq_hbm, bq_hbm, wkv_hbm, bkv_hbm, wo_hbm, bo_hbm, gain_hbm, lnb_hbm,
           y_ref, k_ref, v_ref,
           hid, normed, wkv, wq, wo, bq_own, bq_pair, bkv_ref, bo_ref, gain_ref, lnb_ref, seg, segcol, kv, q_s, o_all, part, run_s, m_s, l_s, acc_s,
           load_sem, spread_sem, line_sem, kv_sem, small_sem, bq_recv, seg_recv, kv_recv, wq_recv, wo_recv, o_recv):
    tok, d_model = hid.shape
    width = wq.shape[2]
    heads = width // HEAD_DIM
    tile = tok // 4
    q_rows, o_rows = d_model // 8, width // 8
    dp, z, cp = lax.axis_index('dp'), lax.axis_index('tp'), lax.axis_index('cp')
    y, c = cp // 2, cp % 2
    pair = z + 1 - 2 * (z % 2)
    below, above = {'tp': z - 1}, {'tp': z + 1}
    to_x, to_y, to_core = {'dp': 1 - dp}, {'cp': cp + 2 - 4 * y}, {'cp': cp + 1 - 2 * c}
    pos = lambda px, py, pc: px * 4 + py * 2 + pc
    p_me, p_x, p_y, p_d = pos(dp, y, c), pos(1 - dp, y, c), pos(dp, 1 - y, c), pos(1 - dp, 1 - y, c)
    g_a = 1 + z % 2
    g_c = 3 - 3 * (z // 2)
    g_b = 6 - z - g_a - g_c

    loads = [pltpu.make_async_copy(hid_hbm, hid, load_sem.at[0]),
             pltpu.make_async_copy(wkv_hbm, wkv, load_sem.at[1]),
             pltpu.make_async_copy(wq_hbm, wq.at[0], load_sem.at[2]),
             pltpu.make_async_copy(bq_hbm, bq_own, load_sem.at[3]),
             pltpu.make_async_copy(seg_hbm, seg.at[cp], load_sem.at[4]),
             pltpu.make_async_copy(wo_hbm, wo.at[pl.ds(z * width, width), :], load_sem.at[5]),
             pltpu.make_async_copy(gain_hbm, gain_ref, load_sem.at[6]),
             pltpu.make_async_copy(lnb_hbm, lnb_ref, load_sem.at[7]),
             pltpu.make_async_copy(bkv_hbm, bkv_ref, load_sem.at[8]),
             pltpu.make_async_copy(bo_hbm, bo_ref, load_sem.at[9])]
    for i in (0, 6, 7, 8, 3, 4, 9):
        loads[i].start()

    barrier = pltpu.get_barrier_semaphore()
    for step in (1, 2, 3):
        pl.semaphore_signal(barrier, inc=1, device_id={'cp': (cp + step) % 4}, device_id_type=MESH)
    pl.semaphore_signal(barrier, inc=1, device_id=to_x, device_id_type=MESH)

    @pl.when(z > 0)
    def _():
        pl.semaphore_signal(barrier, inc=1, device_id={'tp': z - 1}, device_id_type=MESH)

    @pl.when(z < 3)
    def _():
        pl.semaphore_signal(barrier, inc=1, device_id={'tp': z + 1}, device_id_type=MESH)

    loads[1].start()
    with jax.named_scope('barr'):
        pl.semaphore_wait(barrier, 5 + (z + 1) // 2 - 2 * (z // 3))

    loads[2].start()
    def q_piece(p, h):
        half = q_rows // 2
        return wq.at[1, pl.ds(pl.multiple_of(p * q_rows + h * half, half), half), :]

    def o_piece(g, p, h):
        half = o_rows // 2
        return wo.at[pl.ds(pl.multiple_of(g * width + p * o_rows + h * half, half), half), :]

    def sem(g, kind, h):
        at = {'z': 0, 'x': 2, 'y': 4, 'd': 6, 'core': 8}[kind] + (0 if kind == 'core' else h)
        return wq_recv.at[at] if g is None else wo_recv.at[g, at]

    middle, edge = (z > 0) & (z < 3), (z == 0) | (z == 3)

    send(bq_hbm, bq_pair, small_sem.at[0], bq_recv, {'tp': pair})
    for h in (0, 1):
        half = q_rows // 2
        send(wq_hbm.at[pl.ds(pl.multiple_of(p_me * q_rows + h * half, half), half), :], q_piece(p_me, h), spread_sem, sem(None, 'z', h),
             {'tp': pair})
    for h in (0, 1):
        half = o_rows // 2
        for to, cond in ((below, z > 0), (above, z < 3)):
            @pl.when(cond)
            def _():
                send(wo_hbm.at[pl.ds(pl.multiple_of(p_me * o_rows + h * half, half), half), :], o_piece(z, p_me, h), line_sem,
                     sem(z, 'z', h), to)
    for step in (1, 2, 3):
        pl.when(cp + step < 4)(lambda: send(seg_hbm, seg.at[cp], small_sem.at[step], seg_recv.at[cp], {'cp': cp + step}))

    def pass_on(g, source, h, by_x):
        p = {'z': p_me, 's': p_me, 'x': p_x, 'y': p_y, 'd': p_d}[source]
        piece = q_piece(p, h) if g is None else o_piece(g, p, h)
        if source == 's':
            send(piece, piece, spread_sem, sem(g, 'x', h), to_x)
            send(piece, piece, spread_sem, sem(g, 'y', h), to_y)
            return
        arrived(piece, sem(g, source, h))
        if source == 'z' and g is not None:
            pl.when((g > z) & (z > 0))(lambda: send(piece, piece, line_sem, sem(g, 'z', h), below))
            pl.when((g < z) & (z < 3))(lambda: send(piece, piece, line_sem, sem(g, 'z', h), above))
        elif source == 'x':
            if not by_x:
                pl.when(c == 1)(lambda: send(piece, piece, spread_sem, sem(g, 'd', h), to_y))
        elif source == 'y':
            pl.when((c == 0) | by_x)(lambda: send(piece, piece, spread_sem, sem(g, 'd', h), to_x))
        send(piece, piece, spread_sem, sem(g, 'core', h), to_core)

    groups = {'q': None, 'a': g_a, 'b': g_b, 'c': g_c}

    @scoped
    def ev(name, sources, *halves):
        for h in halves or (0, 1):
            for source in sources:
                pass_on(groups[name], source, h, name == 'q')

    @scoped
    def whole(name):
        if name == 'q':
            arrived(wq.at[1, pl.ds(0, 4 * q_rows), :], sem(None, 'core', 0))
        else:
            arrived(wo.at[pl.ds(0, 4 * o_rows), :], sem(groups[name], 'core', 0))

    loads[5].start()

    with jax.named_scope('load_wait'):
        for i in (0, 6, 7):
            loads[i].wait()
    gain = gain_ref[...].astype(F32)
    lnb = lnb_ref[...].astype(F32)
    ln_rows = min(64, tok)

    def ln_step(i, carry):
        rows = pl.ds(pl.multiple_of(i * ln_rows, ln_rows), ln_rows)
        x = hid[rows, :].astype(F32)
        cen = x - jnp.mean(x, axis=-1, keepdims=True)
        var = jnp.mean(cen * cen, axis=-1, keepdims=True)
        normed[rows, :] = (cen * lax.rsqrt(var + LN_EPS) * gain + lnb).astype(BF16)
        return carry

    with jax.named_scope('ln'):
        lax.fori_loop(0, tok // ln_rows, ln_step, 0)

    loads[1].wait()
    loads[8].wait()
    kv_new = (jnp.dot(normed[...], wkv[...], preferred_element_type=F32) + bkv_ref[...].astype(F32)).astype(BF16)
    kv[cp, 0] = kv_new[:, :HEAD_DIM]
    kv[cp, 1] = kv_new[:, HEAD_DIM:]
    k_ref[...] = kv_new[:, :HEAD_DIM]
    v_ref[...] = kv_new[:, HEAD_DIM:]

    @scoped
    def project_q(which, bias):
        qf = jnp.dot(normed[...], wq[which], preferred_element_type=F32) + bias[...].astype(F32)
        for r in range(4):
            for h in range(heads):
                q_s[which * 4 + r, h * tile:(h + 1) * tile, :] = qf[r * tile:(r + 1) * tile, h * HEAD_DIM:(h + 1) * HEAD_DIM].astype(BF16)

    loads[2].wait()
    loads[3].wait()
    for i in (0, 1):
        pl.when(y == 0)(lambda: send(kv.at[cp, i], kv.at[cp, i], kv_sem, kv_recv.at[cp, i], to_y))
    for i in (0, 1):
        pl.when(c == 0)(lambda: send(kv.at[cp, i], kv.at[cp, i], kv_sem, kv_recv.at[cp, i], to_core))
    project_q(0, bq_own)
    loads[4].wait()
    for r in range(4):
        row = jnp.broadcast_to(seg[cp, :, r * tile:(r + 1) * tile], (tile, tile))
        segcol[r] = row.T

    g_1, g_2 = 2 - z // 2, 3 - 3 * (z // 2)
    tile_rows = lambda r: pl.ds(pl.multiple_of(r * tile, tile), tile)
    every = pl.ds(0, tok)

    def scores(q, k_blk, mask):
        keys = k_blk.shape[0]
        s = lax.dot_general(q, k_blk, (((1,), (1,)), ((), ())), preferred_element_type=F32) * SCORE_SCALE
        return jnp.where(mask[None], s.reshape(heads, tile, keys), -jnp.inf).reshape(heads * tile, keys)

    @scoped
    def attend_own(t, carry):
        r = t % 4

        def step(keys):
            k_pos = lax.broadcasted_iota(jnp.int32, (tile, keys), 1)
            q_pos = lax.broadcasted_iota(jnp.int32, (tile, keys), 0) + r * tile
            s = scores(q_s[t], kv[cp, 0, :keys, :], (seg[cp, :, :keys] == segcol[r][:, :1]) & (k_pos <= q_pos))
            m_new = jnp.max(s, axis=-1, keepdims=True)
            p = jnp.exp2(s - m_new)
            m_s[r] = jnp.broadcast_to(m_new, m_s.shape[1:])
            l_s[r] = jnp.broadcast_to(jnp.sum(p, axis=-1, keepdims=True), l_s.shape[1:])
            acc_s[r] = jnp.dot(p.astype(BF16), kv[cp, 1, :keys, :], preferred_element_type=F32)

        pl.when(r < 2)(lambda: step(tok // 2))
        pl.when(r >= 2)(lambda: step(tok))
        return carry

    def attend_block(t, j):
        r = t % 4
        s = scores(q_s[t], kv[j, 0], seg[j] == segcol[r][:, :1])
        m_prev = m_s[r]
        m_new = jnp.maximum(m_prev, jnp.max(s, axis=-1, keepdims=True))
        p = jnp.exp2(s - m_new[:, :1])
        alpha = jnp.exp2(m_prev - m_new)
        m_s[r] = m_new
        l_s[r] = l_s[r] * alpha + jnp.sum(p, axis=-1, keepdims=True)
        acc_s[r] = acc_s[r] * alpha + jnp.dot(p.astype(BF16), kv[j, 1], preferred_element_type=F32)

    def attend_end(t, g):
        r = t % 4
        for h in range(heads):
            at = slice(h * tile, (h + 1) * tile)
            o_all[g, tile_rows(r), h * HEAD_DIM:(h + 1) * HEAD_DIM] = (acc_s[r, at, :] / l_s[r, at, :]).astype(BF16)

    def send_heads(t, g):
        o_tile = o_all.at[g, tile_rows(t % 4), :]
        pl.when(middle)(lambda: send(o_tile, o_tile, line_sem, o_recv.at[t], {'tp': 3 - z}))

    @scoped
    def heads_event(u):
        o_tile = o_all.at[g_1 if u < 4 else g_2, tile_rows(u % 4), :]
        arrived(o_tile, o_recv.at[u])
        for to, cond in ((0, z == 1), (3, z == 2)):
            pl.when(cond)(lambda: send(o_tile, o_tile, line_sem, o_recv.at[u], {'tp': to}))

    def heads_here(*tiles):
        on(middle, *((heads_event, u) for u in tiles))

    def on(cond, *todo):
        @pl.when(cond)
        def _():
            for what, *about in todo:
                what(*about)

    n_col = min(512, d_model)

    def project(g, rows, use):
        def cols(n, carry):
            at = pl.ds(pl.multiple_of(n * n_col, n_col), n_col)
            use(rows, at, jnp.dot(o_all[g, rows, :], wo[pl.ds(pl.multiple_of(g * width, width), width), at],
                                  preferred_element_type=F32).astype(BF16))
            return carry

        lax.fori_loop(0, d_model // n_col, cols, 0)

    @scoped
    def project_o(g):
        def keep(rows, at, fresh):
            part[g % 2, rows, at] = fresh

        project(g, every, keep)

    @scoped
    def project_third(g):
        def add(rows, at, fresh):
            pair_sum = part[(3 - g) % 2, rows, at].astype(F32) + fresh.astype(F32)
            run_s[rows, at] = hid[rows, at].astype(F32) + bo_ref[at].astype(F32) + pair_sum

        project(g, every, add)

    @scoped
    def project_last(g, rows):
        def add(rows, at, fresh):
            y_ref[rows, at] = (run_s[rows, at] + (part[(3 - g) % 2, rows, at].astype(F32) + fresh.astype(F32))).astype(BF16)

        project(g, rows, add)

    @scoped
    def kv_pass(i):
        @pl.when(y == 1)
        def _():
            arrived(kv.at[c, i], kv_recv.at[c, i])
            send(kv.at[c, i], kv.at[c, i], kv_sem, kv_recv.at[c, i], to_core)

    def own_block(t, carry):
        attend_own(t, carry)
        on(t == 0, (ev, 'q', 'zs', 0))
        on(t == 3, (kv_pass, 0))
        return carry

    lax.fori_loop(0, 4, own_block, 0)

    @pl.when(c == 1)
    def _():
        arrived(seg.at[cp - 1], seg_recv.at[cp - 1])
        for i in (0, 1):
            arrived(kv.at[cp - 1, i], kv_recv.at[cp - 1, i])

    def first_block(t, carry):
        pl.when(c == 1)(lambda: attend_block(t, cp - 1))
        on(t == 0, (ev, 'q', 'zs', 1))
        on(t == 1, (kv_pass, 1))
        on((t == 2) & middle, (ev, 'a', 'z', 0))
        on((t == 3) & middle, (ev, 'a', 'z', 1))
        on(t == 3, (ev, 'q', 'x', 0))
        on((t == 3) & middle, (ev, 'a', 's', 0))
        return carry

    lax.fori_loop(0, 4, first_block, 0)
    pl.when(y == 1)(lambda: arrived(seg.at[c], seg_recv.at[c]))

    def second_block(t, carry):
        pl.when(y == 1)(lambda: attend_block(t, c))
        on(t == 1, (ev, 'q', 'y', 0))
        on((t == 2) & middle, (ev, 'b', 'z', 0))
        on((t == 2) & edge, (ev, 'a', 'zs', 0))
        on(t == 3, (ev, 'q', 'x', 1))
        return carry

    lax.fori_loop(0, 4, second_block, 0)

    @pl.when(y == 1)
    def _():
        arrived(seg.at[1 - c], seg_recv.at[1 - c])
        for i in (0, 1):
            arrived(kv.at[1 - c, i], kv_recv.at[1 - c, i])

    def third_block(t, carry):
        pl.when(y == 1)(lambda: attend_block(t, 1 - c))
        attend_end(t, z)
        on((t == 0) & middle, (ev, 'b', 'z', 1))
        send_heads(t, z)
        on(t == 1, (ev, 'q', 'y', 1))
        on((t == 1) & middle, (ev, 'a', 's', 1))
        on((t == 2) & middle, (ev, 'b', 's', 0))
        on((t == 2) & edge, (ev, 'a', 'zs', 1))
        return carry

    lax.fori_loop(0, 4, third_block, 0)
    on(edge, (ev, 'b', 'zs', 0))
    on(middle, (ev, 'b', 's', 1), (ev, 'c', 'z', 0))
    ev('q', 'd', 0)
    loads[5].wait()
    project_o(z)
    ev('a', 'xy', 0)
    on(edge, (ev, 'b', 'zs', 1))
    ev('q', 'd', 1)
    on(middle, (ev, 'c', 'z', 1))
    whole('q')
    arrived(bq_pair, bq_recv)
    project_q(1, bq_pair)
    on(middle, (ev, 'c', 's', 0))
    ev('a', 'xy', 1)
    heads_here(0)
    on(edge, (ev, 'c', 'zs', 0))

    def pair_heads(t, carry):
        attend_own(t, carry)
        on((t == 4) & middle, (ev, 'c', 's', 1), (heads_event, 1))
        on((t == 5) & (y == 1), (ev, 'b', 'xy', 0))
        on((t == 6) & (y == 1), (ev, 'b', 'xy', 1))
        on((t == 6) & (y == 1) & middle, (heads_event, 4))
        on((t == 7) & (y == 1) & middle, (heads_event, 5))

        def block(j, inner):
            attend_block(t, j)
            return inner

        lax.fori_loop(0, cp, block, 0)
        attend_end(t, pair)
        send_heads(t, pair)
        on((t == 4) & edge, (ev, 'c', 'zs', 1))
        on((t == 4) & (y == 1) & middle, (heads_event, 2))
        on((t == 4) & (y == 1), (ev, 'a', 'd', 0))
        on((t == 5) & (y == 1) & middle, (heads_event, 3))
        on((t == 6) & (y == 1), (ev, 'a', 'd', 1), (ev, 'c', 'xy', 0))
        on((t == 7) & (y == 1), (ev, 'c', 'xy', 1))
        return carry

    lax.fori_loop(4, 8, pair_heads, 0)

    @pl.when(y == 0)
    def _():
        heads_here(2, 3)
        ev('b', 'xy', 0)
        ev('a', 'd', 0)
        heads_here(4)
        ev('b', 'xy', 1)
        heads_here(5)
        ev('a', 'd', 1)
        ev('c', 'xy', 0)
        ev('c', 'xy', 1)

    heads_here(6)
    ev('b', 'd')
    whole('a')
    loads[9].wait()
    on(edge, (project_o, pair))
    on(middle, (project_third, g_1))
    heads_here(7)
    whole('b')
    ev('c', 'd', 0)
    on(edge, *((heads_event, u) for u in range(4)))
    on(edge, (project_third, g_1))
    on(middle, (project_o, pair))
    ev('c', 'd', 1)
    whole('c')

    pl.when(middle)(lambda: project_last(g_2, every))

    def tile_event(r):
        arrived(o_all.at[g_2, tile_rows(r), :], o_recv.at[4 + r])

    def last(r, carry):
        tile_event(r)
        project_last(g_2, tile_rows(r))
        return carry

    @pl.when(edge)
    def _():
        tile_event(0)
        tile_event(1)
        project_last(g_2, pl.ds(0, 2 * tile))
        lax.fori_loop(2, 4, last, 0)

    with jax.named_scope('drain'):
        unit = o_rows // 2

        def sent(count, sems):
            arrived(wo.at[pl.ds(0, count * unit), :], sems)

        sent(58, spread_sem)
        pl.when(edge)(lambda: sent(2, line_sem))
        pl.when(middle)(lambda: sent(26, line_sem))
        for j in (0, 1):
            pl.when(c == j)(lambda: arrived(kv.at[pl.ds(0, 2 - j)], kv_sem))
        arrived(bq_pair, small_sem.at[0])
        for step in (1, 2, 3):
            pl.when(cp + step < 4)(lambda: arrived(seg.at[cp], small_sem.at[step]))


def write_out(y_in, k_in, v_in, y_out, k_out, v_out, sems):
    copies = [pltpu.make_async_copy(a, b, sems.at[i]) for i, (a, b) in enumerate(((y_in, y_out), (k_in, k_out), (v_in, v_out)))]
    for copy in copies:
        copy.start()
    for copy in copies:
        copy.wait()


def solution(mesh):
    def local_block(hidden, seg_ids, w_q, b_q, w_kv, b_kv, w_o, b_o, ln_gain, ln_bias):
        tok, d_model = hidden.shape
        width = w_q.shape[1]
        heads = width // HEAD_DIM
        tile = tok // 4
        hbm = pl.BlockSpec(memory_space=pltpu.HBM)
        vmem = pl.BlockSpec(memory_space=pltpu.VMEM)
        dma = pltpu.SemaphoreType.DMA
        far = lambda a: pltpu.with_memory_space_constraint(a, pltpu.HBM)
        outs = pl.pallas_call(
            kernel,
            out_shape=(jax.ShapeDtypeStruct((tok, d_model), BF16), jax.ShapeDtypeStruct((tok, HEAD_DIM), BF16),
                       jax.ShapeDtypeStruct((tok, HEAD_DIM), BF16)),
            in_specs=[hbm] * 10,
            out_specs=(vmem, vmem, vmem),
            scratch_shapes=[
                pltpu.VMEM((tok, d_model), BF16),
                pltpu.VMEM((tok, d_model), BF16),
                pltpu.VMEM((d_model, 2 * HEAD_DIM), BF16),
                pltpu.VMEM((2, d_model, width), BF16),
                pltpu.VMEM((4 * width, d_model), BF16),
                pltpu.VMEM((width,), BF16),
                pltpu.VMEM((width,), BF16),
                pltpu.VMEM((2 * HEAD_DIM,), BF16),
                pltpu.VMEM((d_model,), BF16),
                pltpu.VMEM((d_model,), BF16),
                pltpu.VMEM((d_model,), BF16),
                pltpu.VMEM((4, 1, tok), jnp.int32),
                pltpu.VMEM((4, tile, tile), jnp.int32),
                pltpu.VMEM((4, 2, tok, HEAD_DIM), BF16),
                pltpu.VMEM((8, heads * tile, HEAD_DIM), BF16),
                pltpu.VMEM((4, tok, width), BF16),
                pltpu.VMEM((2, tok, d_model), BF16),
                pltpu.VMEM((tok, d_model), F32),
                pltpu.VMEM((4, heads * tile, HEAD_DIM), F32),
                pltpu.VMEM((4, heads * tile, HEAD_DIM), F32),
                pltpu.VMEM((4, heads * tile, HEAD_DIM), F32),
                dma((10,)), dma(()), dma(()), dma(()), dma((4,)), dma(()), dma((4,)), dma((4, 2)), dma((9,)), dma((4, 9)), dma((8,)),
            ],
            compiler_params=pltpu.CompilerParams(collective_id=0, has_side_effects=True, vmem_limit_bytes=48 * 2 ** 20),
            name='block',
        )(far(hidden), far(seg_ids.reshape(1, -1)), far(w_q), far(b_q), far(w_kv), far(b_kv), far(w_o), far(b_o), far(ln_gain), far(ln_bias))
        near = lambda a: pltpu.with_memory_space_constraint(a, pltpu.VMEM)
        return pl.pallas_call(
            write_out,
            out_shape=tuple(jax.ShapeDtypeStruct(a.shape, a.dtype) for a in outs),
            in_specs=[vmem] * 3,
            out_specs=(pl.BlockSpec(memory_space=pl.ANY),) * 3,
            scratch_shapes=[dma((3,))],
            name='write',
        )(*map(near, outs))

    row_spec = P(('dp', 'cp'), None)
    tok_spec = P(('dp', 'cp'))
    return jax.shard_map(local_block, mesh=mesh,
                         in_specs=(row_spec, tok_spec, P(None, 'tp'), P('tp'), P(None, None), P(None), P('tp', None), P(None), P(None), P(None)),
                         out_specs=(row_spec, row_spec, row_spec), check_vma=False)
```

```python
import functools
import jax
import jax.numpy as jnp
from jax import lax
from jax.experimental import pallas as pl
from jax.experimental.pallas import tpu as pltpu
from jax.sharding import PartitionSpec as P

HEAD_DIM = 128
LN_EPS = 1e-5
SCORE_SCALE = HEAD_DIM ** -0.5 * 1.4426950408889634
MESH = pl.DeviceIdType.MESH
BF16 = jnp.bfloat16
F32 = jnp.float32


def send(src, dst, sent, recv, to):
    pltpu.make_async_remote_copy(src_ref=src, dst_ref=dst, send_sem=sent, recv_sem=recv, device_id=to, device_id_type=MESH).start()


def scoped(fn):
    def run(*about):
        with jax.named_scope(fn.__name__ + '_'.join(str(a) for a in about if isinstance(a, (str, int)))):
            return fn(*about)
    return run


def arrived(dst, recv):
    pltpu.make_async_copy(dst, dst, recv).wait()


def kernel(hid_hbm, seg_hbm, wq_hbm, bq_hbm, wkv_hbm, bkv_hbm, wo_hbm, bo_hbm, gain_hbm, lnb_hbm,
           y_ref, k_ref, v_ref,
           hid, normed, wkv, wq, wo, bq_own, bq_pair, bkv_ref, bo_ref, gain_ref, lnb_ref, seg, segcol, kv, q_s, o_all, part, run_s, m_s, l_s, acc_s,
           load_sem, spread_sem, line_sem, kv_sem, small_sem, bq_recv, seg_recv, kv_recv, wq_recv, wo_recv, o_recv):
    tok, d_model = hid.shape
    width = wq.shape[2]
    heads = width // HEAD_DIM
    tile = tok // 4
    q_rows, o_rows = d_model // 8, width // 8
    dp, z, cp = lax.axis_index('dp'), lax.axis_index('tp'), lax.axis_index('cp')
    y, c = cp // 2, cp % 2
    pair = z + 1 - 2 * (z % 2)
    below, above = {'tp': z - 1}, {'tp': z + 1}
    to_x, to_y, to_core = {'dp': 1 - dp}, {'cp': cp + 2 - 4 * y}, {'cp': cp + 1 - 2 * c}
    pos = lambda px, py, pc: px * 4 + py * 2 + pc
    p_me, p_x, p_y, p_d = pos(dp, y, c), pos(1 - dp, y, c), pos(dp, 1 - y, c), pos(1 - dp, 1 - y, c)
    g_a = 1 + z % 2
    g_c = 3 - 3 * (z // 2)
    g_b = 6 - z - g_a - g_c

    loads = [pltpu.make_async_copy(hid_hbm, hid, load_sem.at[0]),
             pltpu.make_async_copy(wkv_hbm, wkv, load_sem.at[1]),
             pltpu.make_async_copy(wq_hbm, wq.at[0], load_sem.at[2]),
             pltpu.make_async_copy(bq_hbm, bq_own, load_sem.at[3]),
             pltpu.make_async_copy(seg_hbm, seg.at[cp], load_sem.at[4]),
             pltpu.make_async_copy(wo_hbm, wo.at[pl.ds(z * width, width), :], load_sem.at[5]),
             pltpu.make_async_copy(gain_hbm, gain_ref, load_sem.at[6]),
             pltpu.make_async_copy(lnb_hbm, lnb_ref, load_sem.at[7]),
             pltpu.make_async_copy(bkv_hbm, bkv_ref, load_sem.at[8]),
             pltpu.make_async_copy(bo_hbm, bo_ref, load_sem.at[9])]
    for i in (0, 6, 7, 8, 3, 4, 9):
        loads[i].start()

    barrier = pltpu.get_barrier_semaphore()
    for step in (1, 2, 3):
        pl.semaphore_signal(barrier, inc=1, device_id={'cp': (cp + step) % 4}, device_id_type=MESH)
    pl.semaphore_signal(barrier, inc=1, device_id=to_x, device_id_type=MESH)

    @pl.when(z > 0)
    def _():
        pl.semaphore_signal(barrier, inc=1, device_id={'tp': z - 1}, device_id_type=MESH)

    @pl.when(z < 3)
    def _():
        pl.semaphore_signal(barrier, inc=1, device_id={'tp': z + 1}, device_id_type=MESH)

    loads[1].start()
    with jax.named_scope('barr'):
        pl.semaphore_wait(barrier, 5 + (z + 1) // 2 - 2 * (z // 3))

    loads[2].start()
    def q_piece(p, h):
        half = q_rows // 2
        return wq.at[1, pl.ds(pl.multiple_of(p * q_rows + h * half, half), half), :]

    def o_piece(g, p, h):
        half = o_rows // 2
        return wo.at[pl.ds(pl.multiple_of(g * width + p * o_rows + h * half, half), half), :]

    def sem(g, kind, h):
        at = {'z': 0, 'x': 2, 'y': 4, 'd': 6, 'core': 8}[kind] + (0 if kind == 'core' else h)
        return wq_recv.at[at] if g is None else wo_recv.at[g, at]

    middle, edge = (z > 0) & (z < 3), (z == 0) | (z == 3)

    send(bq_hbm, bq_pair, small_sem.at[0], bq_recv, {'tp': pair})
    for h in (0, 1):
        half = q_rows // 2
        send(wq_hbm.at[pl.ds(pl.multiple_of(p_me * q_rows + h * half, half), half), :], q_piece(p_me, h), spread_sem, sem(None, 'z', h),
             {'tp': pair})
    for h in (0, 1):
        half = o_rows // 2
        for to, cond in ((below, z > 0), (above, z < 3)):
            @pl.when(cond)
            def _():
                send(wo_hbm.at[pl.ds(pl.multiple_of(p_me * o_rows + h * half, half), half), :], o_piece(z, p_me, h), line_sem,
                     sem(z, 'z', h), to)
    for step in (1, 2, 3):
        pl.when(cp + step < 4)(lambda: send(seg_hbm, seg.at[cp], small_sem.at[step], seg_recv.at[cp], {'cp': cp + step}))

    def pass_on(g, source, h, by_x):
        p = {'z': p_me, 's': p_me, 'x': p_x, 'y': p_y, 'd': p_d}[source]
        piece = q_piece(p, h) if g is None else o_piece(g, p, h)
        if source == 's':
            send(piece, piece, spread_sem, sem(g, 'x', h), to_x)
            send(piece, piece, spread_sem, sem(g, 'y', h), to_y)
            return
        arrived(piece, sem(g, source, h))
        if source == 'z' and g is not None:
            pl.when((g > z) & (z > 0))(lambda: send(piece, piece, line_sem, sem(g, 'z', h), below))
            pl.when((g < z) & (z < 3))(lambda: send(piece, piece, line_sem, sem(g, 'z', h), above))
        elif source == 'x':
            if not by_x:
                pl.when(c == 1)(lambda: send(piece, piece, spread_sem, sem(g, 'd', h), to_y))
        elif source == 'y':
            pl.when((c == 0) | by_x)(lambda: send(piece, piece, spread_sem, sem(g, 'd', h), to_x))
        send(piece, piece, spread_sem, sem(g, 'core', h), to_core)

    groups = {'q': None, 'a': g_a, 'b': g_b, 'c': g_c}

    @scoped
    def ev(name, sources, *halves):
        for h in halves or (0, 1):
            for source in sources:
                pass_on(groups[name], source, h, name == 'q')

    @scoped
    def whole(name):
        if name == 'q':
            arrived(wq.at[1, pl.ds(0, 4 * q_rows), :], sem(None, 'core', 0))
        else:
            arrived(wo.at[pl.ds(0, 4 * o_rows), :], sem(groups[name], 'core', 0))

    loads[5].start()

    with jax.named_scope('load_wait'):
        for i in (0, 6, 7):
            loads[i].wait()
    gain = gain_ref[...].astype(F32)
    lnb = lnb_ref[...].astype(F32)
    ln_rows = min(64, tok)

    def ln_step(i, carry):
        rows = pl.ds(pl.multiple_of(i * ln_rows, ln_rows), ln_rows)
        x = hid[rows, :].astype(F32)
        cen = x - jnp.mean(x, axis=-1, keepdims=True)
        var = jnp.mean(cen * cen, axis=-1, keepdims=True)
        normed[rows, :] = (cen * lax.rsqrt(var + LN_EPS) * gain + lnb).astype(BF16)
        return carry

    with jax.named_scope('ln'):
        lax.fori_loop(0, tok // ln_rows, ln_step, 0)

    loads[1].wait()
    loads[8].wait()
    kv_new = (jnp.dot(normed[...], wkv[...], preferred_element_type=F32) + bkv_ref[...].astype(F32)).astype(BF16)
    kv[cp, 0] = kv_new[:, :HEAD_DIM]
    kv[cp, 1] = kv_new[:, HEAD_DIM:]
    k_ref[...] = kv_new[:, :HEAD_DIM]
    v_ref[...] = kv_new[:, HEAD_DIM:]

    @scoped
    def project_q(which, bias):
        qf = jnp.dot(normed[...], wq[which], preferred_element_type=F32) + bias[...].astype(F32)
        for r in range(4):
            for h in range(heads):
                q_s[which * 4 + r, h * tile:(h + 1) * tile, :] = qf[r * tile:(r + 1) * tile, h * HEAD_DIM:(h + 1) * HEAD_DIM].astype(BF16)

    loads[2].wait()
    loads[3].wait()
    for i in (0, 1):
        pl.when(y == 0)(lambda: send(kv.at[cp, i], kv.at[cp, i], kv_sem, kv_recv.at[cp, i], to_y))
    for i in (0, 1):
        pl.when(c == 0)(lambda: send(kv.at[cp, i], kv.at[cp, i], kv_sem, kv_recv.at[cp, i], to_core))
    project_q(0, bq_own)
    loads[4].wait()
    for r in range(4):
        row = jnp.broadcast_to(seg[cp, :, r * tile:(r + 1) * tile], (tile, tile))
        segcol[r] = row.T

    g_1, g_2 = 2 - z // 2, 3 - 3 * (z // 2)
    tile_rows = lambda r: pl.ds(pl.multiple_of(r * tile, tile), tile)
    every = pl.ds(0, tok)

    def scores(q, k_blk, mask):
        keys = k_blk.shape[0]
        s = lax.dot_general(q, k_blk, (((1,), (1,)), ((), ())), preferred_element_type=F32) * SCORE_SCALE
        return jnp.where(mask[None], s.reshape(heads, tile, keys), -jnp.inf).reshape(heads * tile, keys)

    @scoped
    def attend_own(t, carry):
        r = t % 4

        def step(keys):
            k_pos = lax.broadcasted_iota(jnp.int32, (tile, keys), 1)
            q_pos = lax.broadcasted_iota(jnp.int32, (tile, keys), 0) + r * tile
            s = scores(q_s[t], kv[cp, 0, :keys, :], (seg[cp, :, :keys] == segcol[r][:, :1]) & (k_pos <= q_pos))
            m_new = jnp.max(s, axis=-1, keepdims=True)
            p = jnp.exp2(s - m_new)
            m_s[r] = jnp.broadcast_to(m_new, m_s.shape[1:])
            l_s[r] = jnp.broadcast_to(jnp.sum(p, axis=-1, keepdims=True), l_s.shape[1:])
            acc_s[r] = jnp.dot(p.astype(BF16), kv[cp, 1, :keys, :], preferred_element_type=F32)

        pl.when(r < 2)(lambda: step(tok // 2))
        pl.when(r >= 2)(lambda: step(tok))
        return carry

    def attend_block(t, j):
        r = t % 4
        s = scores(q_s[t], kv[j, 0], seg[j] == segcol[r][:, :1])
        m_prev = m_s[r]
        m_new = jnp.maximum(m_prev, jnp.max(s, axis=-1, keepdims=True))
        p = jnp.exp2(s - m_new[:, :1])
        alpha = jnp.exp2(m_prev - m_new)
        m_s[r] = m_new
        l_s[r] = l_s[r] * alpha + jnp.sum(p, axis=-1, keepdims=True)
        acc_s[r] = acc_s[r] * alpha + jnp.dot(p.astype(BF16), kv[j, 1], preferred_element_type=F32)

    def attend_end(t, g):
        r = t % 4
        for h in range(heads):
            at = slice(h * tile, (h + 1) * tile)
            o_all[g, tile_rows(r), h * HEAD_DIM:(h + 1) * HEAD_DIM] = (acc_s[r, at, :] / l_s[r, at, :]).astype(BF16)

    def send_heads(t, g):
        o_tile = o_all.at[g, tile_rows(t % 4), :]
        pl.when(middle)(lambda: send(o_tile, o_tile, line_sem, o_recv.at[t], {'tp': 3 - z}))

    @scoped
    def heads_event(u):
        o_tile = o_all.at[g_1 if u < 4 else g_2, tile_rows(u % 4), :]
        arrived(o_tile, o_recv.at[u])
        for to, cond in ((0, z == 1), (3, z == 2)):
            pl.when(cond)(lambda: send(o_tile, o_tile, line_sem, o_recv.at[u], {'tp': to}))

    def heads_here(*tiles):
        on(middle, *((heads_event, u) for u in tiles))

    def on(cond, *todo):
        @pl.when(cond)
        def _():
            for what, *about in todo:
                what(*about)

    n_col = min(512, d_model)

    def project(g, rows, use):
        def cols(n, carry):
            at = pl.ds(pl.multiple_of(n * n_col, n_col), n_col)
            use(rows, at, jnp.dot(o_all[g, rows, :], wo[pl.ds(pl.multiple_of(g * width, width), width), at],
                                  preferred_element_type=F32).astype(BF16))
            return carry

        lax.fori_loop(0, d_model // n_col, cols, 0)

    @scoped
    def project_o(g):
        def keep(rows, at, fresh):
            part[g % 2, rows, at] = fresh

        project(g, every, keep)

    @scoped
    def project_third(g):
        def add(rows, at, fresh):
            pair_sum = part[(3 - g) % 2, rows, at].astype(F32) + fresh.astype(F32)
            run_s[rows, at] = hid[rows, at].astype(F32) + bo_ref[at].astype(F32) + pair_sum

        project(g, every, add)

    @scoped
    def project_last(g, rows):
        def add(rows, at, fresh):
            y_ref[rows, at] = (run_s[rows, at] + (part[(3 - g) % 2, rows, at].astype(F32) + fresh.astype(F32))).astype(BF16)

        project(g, rows, add)

    @scoped
    def kv_pass(i):
        @pl.when(y == 1)
        def _():
            arrived(kv.at[c, i], kv_recv.at[c, i])
            send(kv.at[c, i], kv.at[c, i], kv_sem, kv_recv.at[c, i], to_core)

    def own_block(t, carry):
        attend_own(t, carry)
        on(t == 0, (ev, 'q', 'zs', 0))
        on(t == 3, (kv_pass, 0))
        return carry

    lax.fori_loop(0, 4, own_block, 0)

    @pl.when(c == 1)
    def _():
        arrived(seg.at[cp - 1], seg_recv.at[cp - 1])
        for i in (0, 1):
            arrived(kv.at[cp - 1, i], kv_recv.at[cp - 1, i])

    def first_block(t, carry):
        pl.when(c == 1)(lambda: attend_block(t, cp - 1))
        on(t == 0, (ev, 'q', 'zs', 1))
        on(t == 1, (kv_pass, 1))
        on((t == 2) & middle, (ev, 'a', 'z', 0))
        on((t == 3) & middle, (ev, 'a', 'z', 1))
        on(t == 3, (ev, 'q', 'x', 0))
        on((t == 3) & middle, (ev, 'a', 's', 0))
        return carry

    lax.fori_loop(0, 4, first_block, 0)
    pl.when(y == 1)(lambda: arrived(seg.at[c], seg_recv.at[c]))

    def second_block(t, carry):
        pl.when(y == 1)(lambda: attend_block(t, c))
        on(t == 1, (ev, 'q', 'y', 0))
        on((t == 2) & middle, (ev, 'b', 'z', 0))
        on((t == 2) & edge, (ev, 'a', 'zs', 0))
        on(t == 3, (ev, 'q', 'x', 1))
        return carry

    lax.fori_loop(0, 4, second_block, 0)

    @pl.when(y == 1)
    def _():
        arrived(seg.at[1 - c], seg_recv.at[1 - c])
        for i in (0, 1):
            arrived(kv.at[1 - c, i], kv_recv.at[1 - c, i])

    def third_block(t, carry):
        pl.when(y == 1)(lambda: attend_block(t, 1 - c))
        attend_end(t, z)
        on((t == 0) & middle, (ev, 'b', 'z', 1))
        send_heads(t, z)
        on(t == 1, (ev, 'q', 'y', 1))
        on((t == 1) & middle, (ev, 'a', 's', 1))
        on((t == 2) & middle, (ev, 'b', 's', 0))
        on((t == 2) & edge, (ev, 'a', 'zs', 1))
        return carry

    lax.fori_loop(0, 4, third_block, 0)
    on(edge, (ev, 'b', 'zs', 0))
    on(middle, (ev, 'b', 's', 1), (ev, 'c', 'z', 0))
    ev('q', 'd', 0)
    loads[5].wait()
    project_o(z)
    ev('a', 'xy', 0)
    on(edge, (ev, 'b', 'zs', 1))
    ev('q', 'd', 1)
    on(middle, (ev, 'c', 'z', 1))
    whole('q')
    arrived(bq_pair, bq_recv)
    project_q(1, bq_pair)
    on(middle, (ev, 'c', 's', 0))
    ev('a', 'xy', 1)
    heads_here(0)
    on(edge, (ev, 'c', 'zs', 0))

    def pair_heads(t, carry):
        attend_own(t, carry)
        on((t == 4) & middle, (ev, 'c', 's', 1), (heads_event, 1))
        on((t == 5) & (y == 1), (ev, 'b', 'xy', 0))
        on((t == 6) & (y == 1), (ev, 'b', 'xy', 1))
        on((t == 6) & (y == 1) & middle, (heads_event, 4))
        on((t == 7) & (y == 1) & middle, (heads_event, 5))

        def block(j, inner):
            attend_block(t, j)
            return inner

        lax.fori_loop(0, cp, block, 0)
        attend_end(t, pair)
        send_heads(t, pair)
        on((t == 4) & edge, (ev, 'c', 'zs', 1))
        on((t == 4) & (y == 1) & middle, (heads_event, 2))
        on((t == 4) & (y == 1), (ev, 'a', 'd', 0))
        on((t == 5) & (y == 1) & middle, (heads_event, 3))
        on((t == 6) & (y == 1), (ev, 'a', 'd', 1), (ev, 'c', 'xy', 0))
        on((t == 7) & (y == 1), (ev, 'c', 'xy', 1))
        return carry

    lax.fori_loop(4, 8, pair_heads, 0)

    @pl.when(y == 0)
    def _():
        heads_here(2, 3)
        ev('b', 'xy', 0)
        ev('a', 'd', 0)
        heads_here(4)
        ev('b', 'xy', 1)
        heads_here(5)
        ev('a', 'd', 1)
        ev('c', 'xy', 0)
        ev('c', 'xy', 1)

    ev('b', 'd')
    whole('a')
    loads[9].wait()
    on(edge, (project_o, pair))
    heads_here(6)
    on(middle, (project_third, g_1))
    heads_here(7)
    whole('b')
    ev('c', 'd', 0)
    on(edge, *((heads_event, u) for u in range(4)))
    on(middle, (ev, 'c', 'd', 1))
    on(edge, (project_third, g_1))
    on(middle, (project_o, pair))
    on(edge, (ev, 'c', 'd', 1))
    whole('c')

    pl.when(middle)(lambda: project_last(g_2, every))

    def tile_event(r):
        arrived(o_all.at[g_2, tile_rows(r), :], o_recv.at[4 + r])

    def last(r, carry):
        tile_event(r)
        project_last(g_2, tile_rows(r))
        return carry

    @pl.when(edge)
    def _():
        tile_event(0)
        tile_event(1)
        project_last(g_2, pl.ds(0, 2 * tile))
        lax.fori_loop(2, 4, last, 0)

    with jax.named_scope('drain'):
        unit = o_rows // 2

        def sent(count, sems):
            arrived(wo.at[pl.ds(0, count * unit), :], sems)

        sent(58, spread_sem)
        pl.when(edge)(lambda: sent(2, line_sem))
        pl.when(middle)(lambda: sent(26, line_sem))
        for j in (0, 1):
            pl.when(c == j)(lambda: arrived(kv.at[pl.ds(0, 2 - j)], kv_sem))
        arrived(bq_pair, small_sem.at[0])
        for step in (1, 2, 3):
            pl.when(cp + step < 4)(lambda: arrived(seg.at[cp], small_sem.at[step]))


def write_out(y_in, k_in, v_in, y_out, k_out, v_out, sems):
    copies = [pltpu.make_async_copy(a, b, sems.at[i]) for i, (a, b) in enumerate(((y_in, y_out), (k_in, k_out), (v_in, v_out)))]
    for copy in copies:
        copy.start()
    for copy in copies:
        copy.wait()


def solution(mesh):
    def local_block(hidden, seg_ids, w_q, b_q, w_kv, b_kv, w_o, b_o, ln_gain, ln_bias):
        tok, d_model = hidden.shape
        width = w_q.shape[1]
        heads = width // HEAD_DIM
        tile = tok // 4
        hbm = pl.BlockSpec(memory_space=pltpu.HBM)
        vmem = pl.BlockSpec(memory_space=pltpu.VMEM)
        dma = pltpu.SemaphoreType.DMA
        far = lambda a: pltpu.with_memory_space_constraint(a, pltpu.HBM)
        outs = pl.pallas_call(
            kernel,
            out_shape=(jax.ShapeDtypeStruct((tok, d_model), BF16), jax.ShapeDtypeStruct((tok, HEAD_DIM), BF16),
                       jax.ShapeDtypeStruct((tok, HEAD_DIM), BF16)),
            in_specs=[hbm] * 10,
            out_specs=(vmem, vmem, vmem),
            scratch_shapes=[
                pltpu.VMEM((tok, d_model), BF16),
                pltpu.VMEM((tok, d_model), BF16),
                pltpu.VMEM((d_model, 2 * HEAD_DIM), BF16),
                pltpu.VMEM((2, d_model, width), BF16),
                pltpu.VMEM((4 * width, d_model), BF16),
                pltpu.VMEM((width,), BF16),
                pltpu.VMEM((width,), BF16),
                pltpu.VMEM((2 * HEAD_DIM,), BF16),
                pltpu.VMEM((d_model,), BF16),
                pltpu.VMEM((d_model,), BF16),
                pltpu.VMEM((d_model,), BF16),
                pltpu.VMEM((4, 1, tok), jnp.int32),
                pltpu.VMEM((4, tile, tile), jnp.int32),
                pltpu.VMEM((4, 2, tok, HEAD_DIM), BF16),
                pltpu.VMEM((8, heads * tile, HEAD_DIM), BF16),
                pltpu.VMEM((4, tok, width), BF16),
                pltpu.VMEM((2, tok, d_model), BF16),
                pltpu.VMEM((tok, d_model), F32),
                pltpu.VMEM((4, heads * tile, HEAD_DIM), F32),
                pltpu.VMEM((4, heads * tile, HEAD_DIM), F32),
                pltpu.VMEM((4, heads * tile, HEAD_DIM), F32),
                dma((10,)), dma(()), dma(()), dma(()), dma((4,)), dma(()), dma((4,)), dma((4, 2)), dma((9,)), dma((4, 9)), dma((8,)),
            ],
            compiler_params=pltpu.CompilerParams(collective_id=0, has_side_effects=True, vmem_limit_bytes=48 * 2 ** 20),
            name='block',
        )(far(hidden), far(seg_ids.reshape(1, -1)), far(w_q), far(b_q), far(w_kv), far(b_kv), far(w_o), far(b_o), far(ln_gain), far(ln_bias))
        near = lambda a: pltpu.with_memory_space_constraint(a, pltpu.VMEM)
        return pl.pallas_call(
            write_out,
            out_shape=tuple(jax.ShapeDtypeStruct(a.shape, a.dtype) for a in outs),
            in_specs=[vmem] * 3,
            out_specs=(pl.BlockSpec(memory_space=pl.ANY),) * 3,
            scratch_shapes=[dma((3,))],
            name='write',
        )(*map(near, outs))

    row_spec = P(('dp', 'cp'), None)
    tok_spec = P(('dp', 'cp'))
    return jax.shard_map(local_block, mesh=mesh,
                         in_specs=(row_spec, tok_spec, P(None, 'tp'), P('tp'), P(None, None), P(None), P('tp', None), P(None), P(None), P(None)),
                         out_specs=(row_spec, row_spec, row_spec), check_vma=False)
```
